32 devices in a mesh: gx: 4 (over y, core), gy: 8 (over z, x).
Axes of the slice: x: 2, y: 2, z: 4, core: 2. Of those that a mesh axis runs over, the one named last changes fastest.
Arguments:
- q_now: float32 [5, 64, 128, 256], P(None, 'gx', 'gy'), may hold values from -6 to 6
- q_prev: float32 [5, 64, 128, 256], P(None, 'gx', 'gy'), may hold values from -6 to 6
- jacobian: float32 [64, 128, 256], P('gx', 'gy'), may hold values from 0.5 to 2
- flux_split: float32 [3, 2, 5, 5], replicated, may hold values from -2 to 2
- donor_base: int32 [32768], P(('gx', 'gy')), may hold values from 0 to 57374
- donor_frac: float32 [3, 32768], P(None, ('gx', 'gy')), may hold values from 0 to 1
- fringe_dest: int32 [32768, 1], P(('gx', 'gy')), may hold values from 0 to 31; in each aligned block of 1024 rows (0 to 1023, 1024 to 2047, ...) at most 64 rows name the same one
- receptor_cell: int32 [32768], P(('gx', 'gy')), may hold values from 0 to 65535
- fringe_count: int32 [32], P(('gx', 'gy')), may hold values from 1 to 1024, 24576 in all
Outputs:
- q_next: float32 [5, 64, 128, 256], P(None, 'gx', 'gy')
The draws below stay inside these ranges and needn't reach their ends.
Inputs may be any that keep to these rules, and one draw needn't show every extreme that they name: `fringe_dest`: among the 1024 rows of one block, at most 64 name the same destination block; some block sends exactly 64 to one destination. A block's live rows are its first fringe_count rows; the counts sum to 24576 and some block has 1024. `receptor_cell`: several rows may share a receptor cell.
All inputs are finite; a program needn't handle non-finite values.
Results may differ from the reference program's by a relative error of at most 0.0003.
Values sent between devices are 32-bit elements; how exact they have to be, the bound alone decides.
No kernel may reach another device: no remote copies, remote signals or barrier semaphores. Data moves between devices by JAX's collectives and lax.ppermute only.
A program may use at most 192 MiB of HBM per device.

```python
import math
import jax
import jax.numpy as jnp
import numpy as np
from jax import lax

VARS = 5
CX = 16
CY = 16
CZ = 256
F_DEV = 1024
SUBITERS = 2
CELLS = 65536
CAP = 64
ROWS = 32768
NX = 64
NY = 128
N_GX = 4
N_GY = 8
DEVICES = 32


def place_ends(entries, stream_key, smallest, high):
    index_at = [jax.random.randint(jax.random.fold_in(stream_key, axis), (), 0, length) for axis, length in enumerate(entries.shape)]
    widest = entries.shape.index(max(entries.shape))
    beside = index_at[:widest] + [(index_at[widest] + 1) % entries.shape[widest]] + index_at[widest + 1:]
    return entries.at[tuple(index_at)].set(smallest).at[tuple(beside)].set(high)


def level_of(rng, shape, cuts, low, high):
    level = 1.0
    for dim, blocks in cuts:
        draws = jax.random.uniform(jax.random.fold_in(jax.random.fold_in(rng, 6), dim), (blocks,), jnp.float32, low / len(cuts), high / len(cuts))
        level = level * jnp.repeat(jnp.exp(draws), shape[dim] // blocks).reshape((-1,) + (1,) * (len(shape) - 1 - dim))
    return level


def length_profile(amount, total, bound, lean):
    weights = [(1 << 20) // math.isqrt(grade ** lean) + 1 for grade in range(2, amount + 1)]
    rest, holding = total - bound - (amount - 1), [1] * (amount - 1)
    while rest > 0:
        movable = [i for i in range(amount - 1) if holding[i] < bound]
        pool, remaining = sum([weights[i] for i in movable]), rest
        for i in movable:
            extra = min(bound - holding[i], max(1, remaining * weights[i] // pool), rest)
            holding[i] = holding[i] + extra
            rest = rest - extra
    return np.array([bound] + holding)


def uneven(stream_key, count, total, reach, slope):
    if count == 2:
        one = jax.random.randint(stream_key, (), max(1, total - reach), min(reach, total - 1) + 1)
        return jnp.stack([one, total - one])
    lengths = jnp.asarray(length_profile(count, total, reach, slope), jnp.int32)
    twos = (count - 1) // 2
    donor, sink = lengths[1:1 + 2 * twos:2], lengths[2:2 + 2 * twos:2]
    margin = jnp.minimum(donor - 1, reach - sink)
    passed = jax.random.randint(jax.random.fold_in(stream_key, 1), (twos,), 0, 1 << 20) % (margin + 1)
    lengths = lengths.at[1:1 + 2 * twos:2].set(donor - passed).at[2:2 + 2 * twos:2].set(sink + passed)
    return lengths[jax.random.permutation(jax.random.fold_in(stream_key, 2), count)]


def shared_out(key, own, number, rows, count, top, most, lean):
    order = jax.random.permutation(key, count)
    heavy_load, usual = portions_of(count, rows * top, most, lean, True), portions_of(count, rows * top, most, lean, False)
    places = jnp.arange(count)

    def named(sizes, offset_by):
        used = int((sizes > 0).sum())
        fixed = max(1, used // 4)
        passed = fixed + (places - fixed + offset_by * (used - fixed)) % max(1, count - fixed)
        return jnp.zeros((count,), jnp.int32).at[order[jnp.where(places < fixed, places, passed)]].set(jnp.asarray(sizes, jnp.int32))

    sizes = jnp.where(number % 4 == 0, named(heavy_load, number // 4), named(usual, number - number // 4 - 1))
    mixed = jax.random.permutation(jax.random.fold_in(own, 3), count)
    source_of, receiver = mixed[0:count // 2 * 2:2], mixed[1:count // 2 * 2:2]
    room = jnp.minimum(sizes[source_of] - 1, most - sizes[receiver]) // 2
    room = jnp.where((source_of == order[0]) | (receiver == order[0]) | (sizes[receiver] == 0), 0, jnp.maximum(room, 0))
    passed = jax.random.randint(jax.random.fold_in(own, 4), (count // 2,), 0, 1 << 20) % (room + 1)
    sizes = sizes.at[source_of].add(-passed).at[receiver].add(passed)
    members = jnp.searchsorted(jnp.cumsum(sizes), jnp.arange(rows * top), side="right").astype(jnp.int32)
    table = members.reshape(top, rows).T
    table = table[jax.random.permutation(jax.random.fold_in(own, 1), rows)]
    offset_by = jax.random.randint(jax.random.fold_in(own, 2), (rows, 1), 0, top)
    return jnp.take_along_axis(table, (jnp.arange(top)[None, :] + offset_by) % top, axis=1)


def portions_of(amount, total, limit, skew, full):
    loads = [(1 << 20) // math.isqrt(rank ** skew) + 1 for rank in range(1, amount + 1)]
    largest = limit if full else min(limit, max(-(-total // amount), total * loads[0] // sum(loads)))
    least = 1 if total - largest >= amount - 1 else 0
    counts, rest = [largest] + [least] * (amount - 1), total - largest - least * (amount - 1)
    while rest > 0:
        free = [i for i in range(1, amount) if counts[i] < largest] or [i for i in range(1, amount) if counts[i] < limit]
        whole, budget = sum([loads[i] for i in free]), rest
        for i in free:
            extra = min(limit - counts[i], max(1, budget * loads[i] // whole), rest)
            counts[i] = counts[i] + extra
            rest = rest - extra
    return np.array(counts)


def gaussian(rng, dims, deviation, limit, split=(), held_as=jnp.bfloat16):
    entries = deviation * jax.random.normal(rng, dims, jnp.float32)
    if split:
        entries = entries * level_of(rng, dims, split, -0.22, 0.18)
    return jnp.clip(entries, -limit, limit).astype(held_as)


def setup_inputs(seed: int = 0) -> dict:
    seeds = jax.random.split(jax.random.key(seed), 10)
    q_now = gaussian(seeds[0], (VARS, NX, NY, CZ), 1.0, 6.0, ((1, 4), (2, 8)), jnp.float32)
    q_prev = gaussian(seeds[1], (VARS, NX, NY, CZ), 1.0, 6.0, ((1, 4), (2, 8)), jnp.float32)
    jacobian = jnp.clip(jnp.exp(math.log(2.0) - 1.3862944 * jax.random.uniform(seeds[2], (NX, NY, CZ), jnp.float32) ** level_of(seeds[2], (NX, NY, CZ), ((0, 4), (1, 8)), -0.2, 0.2)), 0.5, 2.0)
    flux_split = gaussian(seeds[3], (3, 2, VARS, VARS), 10 ** -0.5, 2.0, (), jnp.float32)
    donor_base = place_ends(jax.random.randint(seeds[4], (ROWS,), 0, (CX - 1) * (CY - 1) * (CZ - 1)), jax.random.fold_in(seeds[4], 1), 0, ((CX - 1) * (CY - 1) * (CZ - 1)) - 1).astype(jnp.int32)
    donor_frac = jnp.clip(1.0 * jax.random.uniform(seeds[5], (3, ROWS), jnp.float32) ** level_of(seeds[5], (3, ROWS), ((1, 32),), -0.2, 0.2), 0.0, 1.0)
    fringe_dest_keys = jax.random.split(jax.random.fold_in(seeds[6], 1), ROWS // F_DEV)
    fringe_dest_turns = jax.random.permutation(jax.random.fold_in(seeds[6], 3), ROWS // F_DEV)
    fringe_dest = jax.vmap(lambda own, number: shared_out(jax.random.fold_in(seeds[6], 2), own, number, F_DEV, DEVICES, 1, CAP, 2))(fringe_dest_keys, fringe_dest_turns).reshape((ROWS, 1))
    receptor_cell = place_ends(jax.random.randint(seeds[7], (ROWS,), 0, CELLS), jax.random.fold_in(seeds[7], 1), 0, CELLS - 1).astype(jnp.int32)
    fringe_count = uneven(seeds[8], DEVICES, DEVICES * F_DEV * 3 // 4, F_DEV, 2).astype(jnp.int32)
    return {"q_now": q_now, "q_prev": q_prev, "jacobian": jacobian, "flux_split": flux_split, "donor_base": donor_base, "donor_frac": donor_frac, "fringe_dest": fringe_dest, "receptor_cell": receptor_cell, "fringe_count": fringe_count}


step_tau = 0.2
step_phys = 0.5
penalty = 2.0


def mixing(matrix, field):
    return jnp.einsum("ab,bxyz->axyz", matrix, field, precision=lax.Precision.HIGHEST)


def residual_padded(padded, flux_split):
    centre = padded[:, 1:-1, 1:-1, 1:-1]
    behind = [padded[:, :-2, 1:-1, 1:-1], padded[:, 1:-1, :-2, 1:-1], padded[:, 1:-1, 1:-1, :-2]]
    ahead = [padded[:, 2:, 1:-1, 1:-1], padded[:, 1:-1, 2:, 1:-1], padded[:, 1:-1, 1:-1, 2:]]
    total = jnp.zeros(centre.shape, jnp.float32)
    for direction in range(3):
        total = total + mixing(flux_split[direction, 0], centre - behind[direction])
        total = total + mixing(flux_split[direction, 1], ahead[direction] - centre)
    return total


def to_blocks(field):
    shaped = field.reshape(VARS, N_GX, CX, N_GY, CY, CZ).transpose(1, 3, 0, 2, 4, 5)
    return shaped.reshape(DEVICES, VARS, CELLS)


def from_blocks(blocks):
    shaped = blocks.reshape(N_GX, N_GY, VARS, CX, CY, CZ).transpose(2, 0, 3, 1, 4, 5)
    return shaped.reshape(VARS, NX, NY, CZ)


def reference(q_now, q_prev, jacobian, flux_split, donor_base, donor_frac, fringe_dest, receptor_cell, fringe_count):
    row_ids = jnp.arange(ROWS, dtype=jnp.int32)
    sender = row_ids // F_DEV
    live = ((row_ids % F_DEV) < fringe_count[sender]).astype(jnp.float32)
    dest = fringe_dest[:, 0]
    base_z = donor_base % (CZ - 1)
    base_y = (donor_base // (CZ - 1)) % (CY - 1)
    base_x = donor_base // ((CZ - 1) * (CY - 1))
    corners = []
    for i in range(2):
        for j in range(2):
            for k in range(2):
                index = ((base_x + i) * CY + base_y + j) * CZ + base_z + k
                weight = (donor_frac[0] if i else 1.0 - donor_frac[0])
                weight = weight * (donor_frac[1] if j else 1.0 - donor_frac[1])
                weight = weight * (donor_frac[2] if k else 1.0 - donor_frac[2])
                corners.append((index.astype(jnp.int32), weight))
    hits = jnp.zeros((DEVICES, CELLS), jnp.float32).at[dest, receptor_cell].add(live)
    hits = hits.reshape(N_GX, N_GY, CX, CY, CZ).transpose(0, 2, 1, 3, 4).reshape(NX, NY, CZ)
    state = q_now
    lagged = q_prev
    for step in range(SUBITERS):
        blocks = to_blocks(lagged)
        values = jnp.zeros((ROWS, VARS), jnp.float32)
        for index, weight in corners:
            values = values + weight[:, None] * blocks[sender, :, index]
        values = values * live[:, None]
        landed = jnp.zeros((DEVICES, VARS, CELLS), jnp.float32).at[dest, :, receptor_cell].add(values)
        target = from_blocks(landed)
        lagged = state
        padded = jnp.pad(state, ((0, 0), (1, 1), (1, 1), (1, 1)))
        flux = residual_padded(padded, flux_split)
        physical = (3.0 * state - 4.0 * q_now + q_prev) / (2.0 * step_phys)
        coupling = penalty * (hits[None] * state - target)
        state = state - step_tau * jacobian[None] * (flux + physical + coupling)
    return state
```

```python
import functools

import jax
import jax.numpy as jnp
from jax import lax
from jax.experimental import pallas as pl
from jax.experimental.pallas import tpu as pltpu
from jax.sharding import PartitionSpec as P

step_tau = 0.2
step_phys = 0.5
penalty = 2.0

AXES = ("gx", "gy")
LANES = 256
CHANNELS = 16
MIB = 1 << 20


def iota(shape, dim):
    return lax.broadcasted_iota(jnp.int32, shape, dim)


def dot(a, b, dims):
    return lax.dot_general(a, b, (dims, ((), ())), preferred_element_type=jnp.float32)


def halves(x):
    high = x.astype(jnp.bfloat16)
    return high, (x - high.astype(jnp.float32)).astype(jnp.bfloat16)


def ranks(dest, devices):
    rows = dest.shape[1]
    blocks = rows // LANES
    hot = (iota((devices, rows), 0) == dest).astype(jnp.float32)
    stacked = jnp.concatenate([hot[:, b * LANES : (b + 1) * LANES] for b in range(blocks)], axis=0)
    before = (iota((LANES, LANES), 0) < iota((LANES, LANES), 1)).astype(jnp.float32)
    local = dot(stacked.astype(jnp.bfloat16), before.astype(jnp.bfloat16), ((1,), (0,)))
    carried = jnp.zeros((devices, 1), jnp.float32)
    pieces = []
    for b in range(blocks):
        part = local[b * devices : (b + 1) * devices]
        own = hot[:, b * LANES : (b + 1) * LANES]
        pieces.append(jnp.sum((part + carried) * own, axis=0, keepdims=True))
        carried = carried + jnp.sum(own, axis=1, keepdims=True)
    return jnp.concatenate(pieces, axis=1)


def donor_kernel(count, q_prev, q_now, base, frac, dest, cell, out, planes, lhs, spread, corner, place, values, sems, *, size, devices, capacity):
    nvars, size_x, size_y, size_z = size
    columns = size_x * size_y
    rows = base.shape[1]
    copies = []
    for k, ref in enumerate((q_prev, q_now)):
        copies.append(pltpu.make_async_copy(ref, planes.at[k], sems.at[k]))
        copies[-1].start()
    start = base[...].astype(jnp.float32)
    in_y = jnp.floor((start + 0.5) * (1.0 / (size_z - 1)))
    base_z = start - in_y * (size_z - 1)
    base_x = jnp.floor((in_y + 0.5) * (1.0 / (size_y - 1)))
    base_y = in_y - base_x * (size_y - 1)
    frac_x, frac_y, frac_z = frac[0:1, :], frac[1:2, :], frac[2:3, :]

    def weights(first, part, shape):
        at = iota(shape, 0).astype(jnp.float32) - first
        return jnp.where(at == 0.0, 1.0 - part, jnp.where(at == 1.0, part, 0.0))

    along_z = weights(base_z, frac_z, (size_z, rows))
    high, low = halves(along_z)
    spread[0:size_z, :] = high
    spread[size_z : 2 * size_z, :] = low
    spread[2 * size_z : 3 * size_z, :] = high
    along_x = weights(base_x, frac_x, (size_x, rows))
    along_y = weights(base_y, frac_y, (size_y, rows))
    for x in range(size_x):
        corner[x * size_y : (x + 1) * size_y, :] = along_x[x : x + 1, :] * along_y
    alive = iota((1, rows), 1) < count[0]
    slot = ranks(dest[...], devices)
    where_to = jnp.where(alive, dest[...].astype(jnp.float32) * capacity + slot, -1.0)
    place[...] = jnp.transpose(jnp.broadcast_to(where_to, (8, rows)))
    landing = cell[...].astype(jnp.float32)
    land_xy = jnp.floor((landing + 0.5) * (1.0 / size_z))
    values[...] = jnp.zeros(values.shape, jnp.float32)
    values[2 * nvars : 2 * nvars + 1, :] = land_xy + 1.0
    values[2 * nvars + 1 : 2 * nvars + 2, :] = landing - land_xy * size_z
    for k in range(2):
        copies[k].wait()
        for v in range(nvars):
            at = pl.ds((k * nvars + v) * columns, columns)
            high, low = halves(planes[k, v])
            lhs[at, 0:size_z] = high
            lhs[at, size_z : 2 * size_z] = high
            lhs[at, 2 * size_z : 3 * size_z] = low
    for n in range(rows // LANES):
        lanes = slice(n * LANES, (n + 1) * LANES)
        for k in range(2):
            part = dot(lhs[k * nvars * columns : (k + 1) * nvars * columns, :], spread[:, lanes], ((1,), (0,)))
            for v in range(nvars):
                picked = part[v * columns : (v + 1) * columns] * corner[:, lanes]
                values[k * nvars + v : k * nvars + v + 1, lanes] = jnp.sum(picked, axis=0, keepdims=True)
    first = values[...]
    high, rest = first.astype(jnp.bfloat16), None
    rest = first - high.astype(jnp.float32)
    middle = rest.astype(jnp.bfloat16)
    last = (rest - middle.astype(jnp.float32)).astype(jnp.bfloat16)
    three = jnp.concatenate([high, middle, last], axis=0)
    column = jnp.broadcast_to(place[:, 0:1], (rows, LANES))
    for n in range(devices * capacity // LANES):
        chosen = (column == (iota((rows, LANES), 1) + n * LANES).astype(jnp.float32)).astype(jnp.float32).astype(jnp.bfloat16)
        moved = dot(three, chosen, ((1,), (0,)))
        moved = moved[0:CHANNELS] + moved[CHANNELS : 2 * CHANNELS] + moved[2 * CHANNELS : 3 * CHANNELS]
        for d in range(LANES // capacity):
            piece = moved[:, d * capacity : (d + 1) * capacity]
            to = n * (LANES // capacity) + d
            out[to] = jnp.concatenate([piece[0:8], piece[8:16]], axis=1)


def flux_of(coef, centre, neighbours):
    nvars = len(centre)
    total = [None] * nvars
    for d, (behind, ahead) in enumerate(neighbours):
        for side in range(2):
            moved = [c - b for c, b in zip(centre, behind)] if side == 0 else [f - c for c, f in zip(centre, ahead)]
            for a in range(nvars):
                for b in range(nvars):
                    term = coef[((d * 2 + side) * nvars + a) * nvars + b] * moved[b]
                    total[a] = term if total[a] is None else total[a] + term
    return total


def neighbours_at(x, state, x_low, x_high, y_low, y_high, size):
    nvars, size_x, size_y, size_z = size
    rows_at = iota((size_y, size_z), 0)
    z_at = iota((size_y, size_z), 1)
    centre = [state[v, x] for v in range(nvars)]
    back_x = [jnp.where(x == 0, x_low[v], state[v, jnp.maximum(x - 1, 0)]) for v in range(nvars)]
    fore_x = [jnp.where(x == size_x - 1, x_high[v], state[v, jnp.minimum(x + 1, size_x - 1)]) for v in range(nvars)]
    back_y = [jnp.where(rows_at == 0, y_low[v, pl.ds(x, 1), :], pltpu.roll(centre[v], 1, 0)) for v in range(nvars)]
    fore_y = [jnp.where(rows_at == size_y - 1, y_high[v, pl.ds(x, 1), :], pltpu.roll(centre[v], size_y - 1, 0)) for v in range(nvars)]
    back_z = [jnp.where(z_at == 0, 0.0, pltpu.roll(centre[v], 1, 1)) for v in range(nvars)]
    fore_z = [jnp.where(z_at == size_z - 1, 0.0, pltpu.roll(centre[v], size_z - 1, 1)) for v in range(nvars)]
    return centre, [(back_x, fore_x), (back_y, fore_y), (back_z, fore_z)]


def first_kernel(coef, q_now, q_prev, jac, got, x_low, x_high, y_low, y_high, state, target, hits, face_xl, face_xh, face_yl, face_yh, rows, grid, *, size, devices, capacity):
    nvars, size_x, size_y, size_z = size
    columns = size_x * size_y
    for d in range(devices):
        piece = got[d]
        lanes = slice(d * capacity, (d + 1) * capacity)
        rows[0:8, lanes] = piece[:, 0:capacity]
        rows[8:16, lanes] = piece[:, capacity : 2 * capacity]
    grid[...] = jnp.zeros(grid.shape, jnp.float32)
    place_xy = (iota((columns, LANES), 0) + 1).astype(jnp.float32)
    place_z = iota((size_z, LANES), 0).astype(jnp.float32)

    def chunk(n, carry):
        block = rows[:, pl.ds(pl.multiple_of(n * LANES, LANES), LANES)]
        hot_xy = (place_xy == block[2 * nvars : 2 * nvars + 1]).astype(jnp.float32).astype(jnp.bfloat16)
        hot_z = (place_z == block[2 * nvars + 1 : 2 * nvars + 2]).astype(jnp.float32).astype(jnp.bfloat16)
        high, low = halves(block[0 : 2 * nvars])
        pieces = []
        for c in range(2 * nvars):
            pieces += [hot_xy * high[c : c + 1], hot_xy * low[c : c + 1]]
        pieces.append(hot_xy)
        landed = dot(jnp.concatenate(pieces, axis=0), hot_z, ((1,), (1,)))
        for c in range(2 * nvars):
            at = 2 * c * columns
            grid[c] = grid[c] + (landed[at : at + columns] + landed[at + columns : at + 2 * columns])
        grid[2 * nvars] = grid[2 * nvars] + landed[4 * nvars * columns :]
        return carry

    lax.fori_loop(0, devices * capacity // LANES, chunk, 0)
    target[...] = grid[nvars : 2 * nvars]
    hits[...] = grid[2 * nvars]

    def plane(x, carry):
        at = pl.ds(pl.multiple_of(x * size_y, size_y), size_y)
        centre, around = neighbours_at(x, q_now, x_low, x_high, y_low, y_high, size)
        flux = flux_of(coef, centre, around)
        landed = grid[2 * nvars, at, :]
        scale = step_tau * jac[x]
        for v in range(nvars):
            physical = (3.0 * centre[v] - 4.0 * centre[v] + q_prev[v, x]) / (2.0 * step_phys)
            coupling = penalty * (landed * centre[v] - grid[v, at, :])
            new = centre[v] - scale * (flux[v] + physical + coupling)
            state[v, x] = new
            face_yl[v, pl.ds(x, 1), :] = new[0:1]
            face_yh[v, pl.ds(x, 1), :] = new[size_y - 1 : size_y]
        return carry

    lax.fori_loop(0, size_x, plane, 0)
    face_xl[...] = state[:, 0]
    face_xh[...] = state[:, size_x - 1]


def second_kernel(coef, state, q_now, q_prev, jac, target, hits, x_low, x_high, y_low, y_high, out, *, size):
    nvars, size_x, size_y, size_z = size

    def plane(x, carry):
        at = pl.ds(pl.multiple_of(x * size_y, size_y), size_y)
        centre, around = neighbours_at(x, state, x_low, x_high, y_low, y_high, size)
        flux = flux_of(coef, centre, around)
        landed = hits[at, :]
        scale = step_tau * jac[x]
        for v in range(nvars):
            physical = (3.0 * centre[v] - 4.0 * q_now[v, x] + q_prev[v, x]) / (2.0 * step_phys)
            coupling = penalty * (landed * centre[v] - target[v, at, :])
            out[v, x] = centre[v] - scale * (flux[v] + physical + coupling)
        return carry

    lax.fori_loop(0, size_x, plane, 0)


def swap_pairs(axis, odd):
    count = lax.axis_size(axis)
    pairs = []
    for i in range(odd, count - 1, 2):
        pairs += [(i, i + 1), (i + 1, i)]
    return pairs


def exchanged(low_face, high_face, axis):
    here = lax.axis_index(axis)
    even = here % 2 == 0
    inner = lax.ppermute(jnp.where(even, high_face, low_face), axis, swap_pairs(axis, 0))
    outer = lax.ppermute(jnp.where(even, low_face, high_face), axis, swap_pairs(axis, 1))
    return jnp.where(even, outer, inner), jnp.where(even, inner, outer)


def params(limit):
    return pltpu.CompilerParams(vmem_limit_bytes=limit * MIB)


def body(q_now, q_prev, jacobian, flux_split, donor_base, donor_frac, fringe_dest, receptor_cell, fringe_count):
    size = q_now.shape
    nvars, size_x, size_y, size_z = size
    columns = size_x * size_y
    devices = lax.axis_size("gx") * lax.axis_size("gy")
    rows = donor_base.shape[0]
    capacity = 2 * rows // devices
    slots = devices * capacity
    f32, bf16 = jnp.float32, jnp.bfloat16
    smem = pl.BlockSpec(memory_space=pltpu.SMEM)
    hbm = pl.BlockSpec(memory_space=pl.ANY)
    vmem = pl.BlockSpec(memory_space=pltpu.VMEM)
    coef = flux_split.reshape(-1)
    flat = (nvars, columns, size_z)
    sent = pl.pallas_call(
        functools.partial(donor_kernel, size=size, devices=devices, capacity=capacity),
        out_shape=jax.ShapeDtypeStruct((devices, 8, 2 * capacity), f32),
        in_specs=[smem, hbm, hbm, vmem, vmem, vmem, vmem],
        out_specs=vmem,
        scratch_shapes=[
            pltpu.VMEM((2, nvars, columns, size_z), f32),
            pltpu.VMEM((2 * nvars * columns, 3 * size_z), bf16),
            pltpu.VMEM((3 * size_z, rows), bf16),
            pltpu.VMEM((columns, rows), f32),
            pltpu.VMEM((rows, 8), f32),
            pltpu.VMEM((CHANNELS, rows), f32),
            pltpu.SemaphoreType.DMA((2,)),
        ],
        compiler_params=params(48),
        name="donor",
    )(
        fringe_count,
        q_prev.reshape(flat),
        q_now.reshape(flat),
        donor_base.reshape(1, rows),
        donor_frac,
        fringe_dest.reshape(1, rows),
        receptor_cell.reshape(1, rows),
    )
    got = lax.all_to_all(sent, AXES, split_axis=0, concat_axis=0, tiled=True)
    x_halo = exchanged(q_now[:, 0], q_now[:, size_x - 1], "gx")
    y_halo = exchanged(q_now[:, :, 0], q_now[:, :, size_y - 1], "gy")
    face_x = jax.ShapeDtypeStruct((nvars, size_y, size_z), f32)
    face_y = jax.ShapeDtypeStruct((nvars, size_x, size_z), f32)

    def edges(halo, axis):
        here, last = lax.axis_index(axis), lax.axis_size(axis) - 1
        return jnp.where(here == 0, 0.0, halo[0]), jnp.where(here == last, 0.0, halo[1])

    x_halo, y_halo = edges(x_halo, "gx"), edges(y_halo, "gy")
    state, target, hits, *faces = pl.pallas_call(
        functools.partial(first_kernel, size=size, devices=devices, capacity=capacity),
        out_shape=[
            jax.ShapeDtypeStruct(size, f32),
            jax.ShapeDtypeStruct(flat, f32),
            jax.ShapeDtypeStruct((columns, size_z), f32),
            face_x,
            face_x,
            face_y,
            face_y,
        ],
        in_specs=[smem] + [vmem] * 8,
        out_specs=[vmem] * 7,
        scratch_shapes=[pltpu.VMEM((CHANNELS, slots), f32), pltpu.VMEM((2 * nvars + 1, columns, size_z), f32)],
        compiler_params=params(48),
        name="first",
    )(coef, q_now, q_prev, jacobian, got, *x_halo, *y_halo)
    x_halo = edges(exchanged(faces[0], faces[1], "gx"), "gx")
    y_halo = edges(exchanged(faces[2], faces[3], "gy"), "gy")
    return pl.pallas_call(
        functools.partial(second_kernel, size=size),
        out_shape=jax.ShapeDtypeStruct(size, f32),
        in_specs=[smem] + [vmem] * 10,
        out_specs=vmem,
        compiler_params=params(48),
        name="second",
    )(coef, state, q_now, q_prev, jacobian, target, hits, *x_halo, *y_halo)


def solution(mesh):
    return jax.shard_map(
        body,
        mesh=mesh,
        in_specs=(
            P(None, "gx", "gy", None),
            P(None, "gx", "gy", None),
            P("gx", "gy", None),
            P(),
            P(("gx", "gy")),
            P(None, ("gx", "gy")),
            P(("gx", "gy"), None),
            P(("gx", "gy")),
            P(("gx", "gy")),
        ),
        out_specs=P(None, "gx", "gy", None),
        check_vma=False,
    )
```

```python
import functools

import jax
import jax.numpy as jnp
from jax import lax
from jax.experimental import pallas as pl
from jax.experimental.pallas import tpu as pltpu
from jax.sharding import PartitionSpec as P

step_tau = 0.2
step_phys = 0.5
penalty = 2.0

AXES = ("gx", "gy")
LANES = 256
CHANNELS = 16
MIB = 1 << 20


def iota(shape, dim):
    return lax.broadcasted_iota(jnp.int32, shape, dim)


def dot(a, b, dims):
    return lax.dot_general(a, b, (dims, ((), ())), preferred_element_type=jnp.float32)


def halves(x):
    high = x.astype(jnp.bfloat16)
    return high, (x - high.astype(jnp.float32)).astype(jnp.bfloat16)


def ranks(dest, devices):
    rows = dest.shape[1]
    blocks = rows // LANES
    hot = (iota((devices, rows), 0) == dest).astype(jnp.float32)
    stacked = jnp.concatenate([hot[:, b * LANES : (b + 1) * LANES] for b in range(blocks)], axis=0)
    before = (iota((LANES, LANES), 0) < iota((LANES, LANES), 1)).astype(jnp.float32)
    local = dot(stacked.astype(jnp.bfloat16), before.astype(jnp.bfloat16), ((1,), (0,)))
    carried = jnp.zeros((devices, 1), jnp.float32)
    pieces = []
    for b in range(blocks):
        part = local[b * devices : (b + 1) * devices]
        own = hot[:, b * LANES : (b + 1) * LANES]
        pieces.append(jnp.sum((part + carried) * own, axis=0, keepdims=True))
        carried = carried + jnp.sum(own, axis=1, keepdims=True)
    return jnp.concatenate(pieces, axis=1)


def donor_kernel(count, q_prev, q_now, base_in, frac_in, dest_in, cell_in, out, planes, lhs, spread, corner, place, values, base, frac, dest, cell, sems, *, size, devices, capacity):
    nvars, size_x, size_y, size_z = size
    columns = size_x * size_y
    rows = base.shape[1]
    small = [pltpu.make_async_copy(a, b, sems.at[2 + k]) for k, (a, b) in enumerate(((base_in, base), (frac_in, frac), (dest_in, dest), (cell_in, cell)))]
    copies = [pltpu.make_async_copy(ref, planes.at[k], sems.at[k]) for k, ref in enumerate((q_prev, q_now))]
    for copy in small + copies:
        copy.start()
    for copy in small:
        copy.wait()
    start = base[...].astype(jnp.float32)
    in_y = jnp.floor((start + 0.5) * (1.0 / (size_z - 1)))
    base_z = start - in_y * (size_z - 1)
    base_x = jnp.floor((in_y + 0.5) * (1.0 / (size_y - 1)))
    base_y = in_y - base_x * (size_y - 1)
    frac_x, frac_y, frac_z = frac[0:1, :], frac[1:2, :], frac[2:3, :]

    def weights(first, part, shape):
        at = iota(shape, 0).astype(jnp.float32) - first
        return jnp.where(at == 0.0, 1.0 - part, jnp.where(at == 1.0, part, 0.0))

    along_z = weights(base_z, frac_z, (size_z, rows))
    high, low = halves(along_z)
    spread[0:size_z, :] = high
    spread[size_z : 2 * size_z, :] = low
    spread[2 * size_z : 3 * size_z, :] = high
    along_x = weights(base_x, frac_x, (size_x, rows))
    along_y = weights(base_y, frac_y, (size_y, rows))
    for x in range(size_x):
        corner[x * size_y : (x + 1) * size_y, :] = along_x[x : x + 1, :] * along_y
    alive = iota((1, rows), 1) < count[0]
    slot = ranks(dest[...], devices)
    where_to = jnp.where(alive, dest[...].astype(jnp.float32) * capacity + slot, -1.0)
    place[...] = jnp.transpose(jnp.broadcast_to(where_to, (8, rows)))
    landing = cell[...].astype(jnp.float32)
    land_xy = jnp.floor((landing + 0.5) * (1.0 / size_z))
    values[...] = jnp.zeros(values.shape, jnp.float32)
    values[2 * nvars : 2 * nvars + 1, :] = land_xy + 1.0
    values[2 * nvars + 1 : 2 * nvars + 2, :] = landing - land_xy * size_z
    for k in range(2):
        copies[k].wait()
        for v in range(nvars):
            at = pl.ds((k * nvars + v) * columns, columns)
            high, low = halves(planes[k, v])
            lhs[at, 0:size_z] = high
            lhs[at, size_z : 2 * size_z] = high
            lhs[at, 2 * size_z : 3 * size_z] = low
    for n in range(rows // LANES):
        lanes = slice(n * LANES, (n + 1) * LANES)
        for k in range(2):
            part = dot(lhs[k * nvars * columns : (k + 1) * nvars * columns, :], spread[:, lanes], ((1,), (0,)))
            for v in range(nvars):
                picked = part[v * columns : (v + 1) * columns] * corner[:, lanes]
                values[k * nvars + v : k * nvars + v + 1, lanes] = jnp.sum(picked, axis=0, keepdims=True)
    first = values[...]
    high, rest = first.astype(jnp.bfloat16), None
    rest = first - high.astype(jnp.float32)
    middle = rest.astype(jnp.bfloat16)
    last = (rest - middle.astype(jnp.float32)).astype(jnp.bfloat16)
    three = jnp.concatenate([high, middle, last], axis=0)
    column = jnp.broadcast_to(place[:, 0:1], (rows, LANES))
    for n in range(devices * capacity // LANES):
        chosen = (column == (iota((rows, LANES), 1) + n * LANES).astype(jnp.float32)).astype(jnp.float32).astype(jnp.bfloat16)
        moved = dot(three, chosen, ((1,), (0,)))
        moved = moved[0:CHANNELS] + moved[CHANNELS : 2 * CHANNELS] + moved[2 * CHANNELS : 3 * CHANNELS]
        for d in range(LANES // capacity):
            piece = moved[:, d * capacity : (d + 1) * capacity]
            to = n * (LANES // capacity) + d
            out[to] = jnp.concatenate([piece[0:8], piece[8:16]], axis=1)


def mixing_weights(coef, high, low, size):
    nvars, size_x, size_y, size_z = size
    block = nvars * size_y
    width = 3 * block + CHANNELS
    row = iota((size_y, width), 0)
    offset = iota((size_y, width), 1) - row
    lane = iota((size_y, width), 1)

    def at(d, side, a, b):
        return coef[((d * 2 + side) * nvars + a) * nvars + b]

    for a in range(nvars):
        main = jnp.zeros((size_y, width), jnp.float32)
        back = main
        fore = main
        for b in range(nvars):
            first = b * size_y
            same = at(0, 0, a, b) - at(0, 1, a, b) + at(1, 0, a, b) - at(1, 1, a, b) + at(2, 0, a, b) - at(2, 1, a, b)
            main = jnp.where(offset == first, -at(0, 0, a, b), main)
            main = jnp.where(offset == block + first, same, main)
            main = jnp.where((offset == block + first - 1) & (row > 0), -at(1, 0, a, b), main)
            main = jnp.where((offset == block + first + 1) & (row < size_y - 1), at(1, 1, a, b), main)
            main = jnp.where(offset == 2 * block + first, at(0, 1, a, b), main)
            main = jnp.where((lane == 3 * block + b) & (row == 0), -at(1, 0, a, b), main)
            main = jnp.where((lane == 3 * block + nvars + b) & (row == size_y - 1), at(1, 1, a, b), main)
            back = jnp.where(offset == block + first, -at(2, 0, a, b), back)
            fore = jnp.where(offset == block + first, at(2, 1, a, b), fore)
        for k, part in enumerate((main, back, fore)):
            rows = slice(k * block + a * size_y, k * block + (a + 1) * size_y)
            high[rows, :], low[rows, :] = halves(part)


def fill_planes(state, x_low, x_high, y_low, y_high, planes, sides, size):
    nvars, size_x, size_y, size_z = size
    block = nvars * size_y
    for x in range(size_x + 2):
        for v in range(nvars):
            value = x_low[v] if x == 0 else x_high[v] if x == size_x + 1 else state[v, x - 1]
            rows = slice(x * block + v * size_y, x * block + (v + 1) * size_y)
            planes[0, rows, :], planes[1, rows, :] = halves(value)
    sides[...] = jnp.zeros(sides.shape, jnp.float32)
    for v in range(nvars):
        sides[:, v, :] = y_low[v]
        sides[:, nvars + v, :] = y_high[v]


def flux_at(x, weights, planes, sides, size):
    nvars, size_x, size_y, size_z = size
    block = nvars * size_y
    high, low = halves(sides[x])
    rows = slice(x * block, (x + 3) * block)
    around_high = jnp.concatenate([planes[0, rows, :], high], axis=0)
    around_low = jnp.concatenate([planes[1, rows, :], low], axis=0)
    both = jnp.concatenate([weights[0], weights[1]], axis=0)
    mixed = dot(both, around_high, ((1,), (0,)))
    mixed = mixed[0 : 3 * block] + mixed[3 * block :] + dot(weights[0], around_low, ((1,), (0,)))
    z_at = iota((block, size_z), 1)
    back = jnp.where(z_at == 0, 0.0, pltpu.roll(mixed[block : 2 * block], 1, 1))
    fore = jnp.where(z_at == size_z - 1, 0.0, pltpu.roll(mixed[2 * block :], size_z - 1, 1))
    flux = mixed[0:block] + back + fore
    return [flux[v * size_y : (v + 1) * size_y] for v in range(nvars)]


def first_kernel(coef, q_now, q_prev, jac, got, x_low, x_high, y_low, y_high, state, target, hits, face_xl, face_xh, face_yl, face_yh, weights, rows, hot_xy, hot_z, grid, planes, sides, *, size, devices, capacity):
    nvars, size_x, size_y, size_z = size
    columns = size_x * size_y
    slots = devices * capacity
    mixing_weights(coef, weights.at[0], weights.at[1], size)
    fill_planes(q_now, x_low, x_high, y_low, y_high, planes, sides, size)
    for d in range(devices):
        piece = got[d]
        lanes = slice(d * capacity, (d + 1) * capacity)
        rows[0:8, lanes] = piece[:, 0:capacity]
        rows[8:16, lanes] = piece[:, capacity : 2 * capacity]
    turned = jnp.transpose(rows[8:16, :])
    land_z = turned[:, 2 * nvars + 1 - 8 : 2 * nvars + 2 - 8]
    hot_z[...] = (iota((slots, size_z), 1).astype(jnp.float32) == land_z).astype(jnp.float32).astype(jnp.bfloat16)
    land_xy = rows[2 * nvars : 2 * nvars + 1, :]
    hot_xy[...] = ((iota((columns, slots), 0) + 1).astype(jnp.float32) == land_xy).astype(jnp.float32).astype(jnp.bfloat16)

    def pair(g, carry):
        pieces = []
        for c in range(2):
            for half in halves(rows[pl.ds(2 * g + c, 1), :]):
                pieces.append(hot_xy[...] * half)
        landed = dot(jnp.concatenate(pieces, axis=0), hot_z[...], ((1,), (0,)))
        for c in range(2):
            at = 2 * c * columns
            grid[2 * g + c] = landed[at : at + columns] + landed[at + columns : at + 2 * columns]
        return carry

    lax.fori_loop(0, nvars, pair, 0)
    hits[...] = dot(hot_xy[...], hot_z[...], ((1,), (0,)))
    target[...] = grid[nvars : 2 * nvars]
    for x in range(size_x):
        at = slice(x * size_y, (x + 1) * size_y)
        flux = flux_at(x, weights, planes, sides, size)
        landed = hits[at, :]
        scale = step_tau * jac[x]
        for v in range(nvars):
            centre = q_now[v, x]
            physical = (q_prev[v, x] - centre) / (2.0 * step_phys)
            coupling = penalty * (landed * centre - grid[v, at, :])
            new = centre - scale * (flux[v] + physical + coupling)
            state[v, x] = new
            face_yl[v, x : x + 1, :] = new[0:1]
            face_yh[v, x : x + 1, :] = new[size_y - 1 : size_y]
            if x == 0:
                face_xl[v] = new
            if x == size_x - 1:
                face_xh[v] = new


def second_kernel(coef, state, q_now, q_prev, jac, target, hits, x_low, x_high, y_low, y_high, out, weights, planes, sides, buffer, sems, *, size):
    nvars, size_x, size_y, size_z = size
    mixing_weights(coef, weights.at[0], weights.at[1], size)
    fill_planes(state, x_low, x_high, y_low, y_high, planes, sides, size)
    part = size_x // 4
    copies = []
    for x in range(size_x):
        at = slice(x * size_y, (x + 1) * size_y)
        flux = flux_at(x, weights, planes, sides, size)
        landed = hits[at, :]
        scale = step_tau * jac[x]
        for v in range(nvars):
            centre = state[v, x]
            physical = (3.0 * centre - 4.0 * q_now[v, x] + q_prev[v, x]) / (2.0 * step_phys)
            coupling = penalty * (landed * centre - target[v, at, :])
            buffer[v, x] = centre - scale * (flux[v] + physical + coupling)
        if (x + 1) % part == 0:
            some = pl.ds(x + 1 - part, part)
            copies.append(pltpu.make_async_copy(buffer.at[:, some], out.at[:, some], sems.at[x // part]))
            copies[-1].start()
    for copy in copies:
        copy.wait()


def swap_pairs(axis, odd):
    count = lax.axis_size(axis)
    pairs = []
    for i in range(odd, count - 1, 2):
        pairs += [(i, i + 1), (i + 1, i)]
    return pairs


def exchanged(low_face, high_face, axis):
    here = lax.axis_index(axis)
    even = here % 2 == 0
    inner = lax.ppermute(jnp.where(even, high_face, low_face), axis, swap_pairs(axis, 0))
    outer = lax.ppermute(jnp.where(even, low_face, high_face), axis, swap_pairs(axis, 1))
    return jnp.where(even, outer, inner), jnp.where(even, inner, outer)


def params(limit):
    return pltpu.CompilerParams(vmem_limit_bytes=limit * MIB)


def body(q_now, q_prev, jacobian, flux_split, donor_base, donor_frac, fringe_dest, receptor_cell, fringe_count):
    size = q_now.shape
    nvars, size_x, size_y, size_z = size
    columns = size_x * size_y
    devices = lax.axis_size("gx") * lax.axis_size("gy")
    rows = donor_base.shape[0]
    capacity = 2 * rows // devices
    slots = devices * capacity
    f32, bf16 = jnp.float32, jnp.bfloat16
    smem = pl.BlockSpec(memory_space=pltpu.SMEM)
    hbm = pl.BlockSpec(memory_space=pltpu.HBM)
    vmem = pl.BlockSpec(memory_space=pltpu.VMEM)
    coef = flux_split.reshape(-1)
    block = nvars * size_y
    weights = pltpu.VMEM((2, 3 * block, 3 * block + CHANNELS), bf16)
    planes = pltpu.VMEM((2, (size_x + 2) * block, size_z), bf16)
    sides = pltpu.VMEM((size_x, CHANNELS, size_z), f32)
    flat = (nvars, columns, size_z)
    sent = pl.pallas_call(
        functools.partial(donor_kernel, size=size, devices=devices, capacity=capacity),
        out_shape=jax.ShapeDtypeStruct((devices, 8, 2 * capacity), f32),
        in_specs=[smem] + [hbm] * 6,
        out_specs=vmem,
        scratch_shapes=[
            pltpu.VMEM((2, nvars, columns, size_z), f32),
            pltpu.VMEM((2 * nvars * columns, 3 * size_z), bf16),
            pltpu.VMEM((3 * size_z, rows), bf16),
            pltpu.VMEM((columns, rows), f32),
            pltpu.VMEM((rows, 8), f32),
            pltpu.VMEM((CHANNELS, rows), f32),
            pltpu.VMEM((1, rows), jnp.int32),
            pltpu.VMEM((3, rows), f32),
            pltpu.VMEM((1, rows), jnp.int32),
            pltpu.VMEM((1, rows), jnp.int32),
            pltpu.SemaphoreType.DMA((6,)),
        ],
        compiler_params=params(48),
        name="donor",
    )(
        fringe_count,
        q_prev.reshape(flat),
        q_now.reshape(flat),
        donor_base.reshape(1, rows),
        donor_frac,
        fringe_dest.reshape(1, rows),
        receptor_cell.reshape(1, rows),
    )
    got = lax.all_to_all(sent, AXES, split_axis=0, concat_axis=0, tiled=True)
    x_halo = exchanged(q_now[:, 0], q_now[:, size_x - 1], "gx")
    y_halo = exchanged(q_now[:, :, 0], q_now[:, :, size_y - 1], "gy")
    face_x = jax.ShapeDtypeStruct((nvars, size_y, size_z), f32)
    face_y = jax.ShapeDtypeStruct((nvars, size_x, size_z), f32)

    def edges(halo, axis):
        here, last = lax.axis_index(axis), lax.axis_size(axis) - 1
        return jnp.where(here == 0, 0.0, halo[0]), jnp.where(here == last, 0.0, halo[1])

    x_halo, y_halo = edges(x_halo, "gx"), edges(y_halo, "gy")
    state, target, hits, *faces = pl.pallas_call(
        functools.partial(first_kernel, size=size, devices=devices, capacity=capacity),
        out_shape=[
            jax.ShapeDtypeStruct(size, f32),
            jax.ShapeDtypeStruct(flat, f32),
            jax.ShapeDtypeStruct((columns, size_z), f32),
            face_x,
            face_x,
            face_y,
            face_y,
        ],
        in_specs=[smem] + [vmem] * 8,
        out_specs=[vmem] * 7,
        scratch_shapes=[
            weights,
            pltpu.VMEM((CHANNELS, slots), f32),
            pltpu.VMEM((columns, slots), bf16),
            pltpu.VMEM((slots, size_z), bf16),
            pltpu.VMEM((2 * nvars, columns, size_z), f32),
            planes,
            sides,
        ],
        compiler_params=params(48),
        name="first",
    )(coef, q_now, q_prev, jacobian, got, *x_halo, *y_halo)
    x_halo = edges(exchanged(faces[0], faces[1], "gx"), "gx")
    y_halo = edges(exchanged(faces[2], faces[3], "gy"), "gy")
    return pl.pallas_call(
        functools.partial(second_kernel, size=size),
        out_shape=jax.ShapeDtypeStruct(size, f32),
        in_specs=[smem] + [vmem] * 10,
        out_specs=hbm,
        scratch_shapes=[weights, planes, sides, pltpu.VMEM(size, f32), pltpu.SemaphoreType.DMA((4,))],
        compiler_params=params(40),
        name="second",
    )(coef, state, q_now, q_prev, jacobian, target, hits, *x_halo, *y_halo)


def solution(mesh):
    return jax.shard_map(
        body,
        mesh=mesh,
        in_specs=(
            P(None, "gx", "gy", None),
            P(None, "gx", "gy", None),
            P("gx", "gy", None),
            P(),
            P(("gx", "gy")),
            P(None, ("gx", "gy")),
            P(("gx", "gy"), None),
            P(("gx", "gy")),
            P(("gx", "gy")),
        ),
        out_specs=P(None, "gx", "gy", None),
        check_vma=False,
    )
```

```python
import functools

import jax
import jax.numpy as jnp
from jax import lax
from jax.experimental import pallas as pl
from jax.experimental.pallas import tpu as pltpu
from jax.sharding import PartitionSpec as P


step_tau = 0.2
step_phys = 0.5
penalty = 2.0

AXES = ("gx", "gy")
LANES = 256
CHANNELS = 16
MIB = 1 << 20


def iota(shape, dim):
    return lax.broadcasted_iota(jnp.int32, shape, dim)


def dot(a, b, dims):
    return lax.dot_general(a, b, (dims, ((), ())), preferred_element_type=jnp.float32)


def halves(x):
    high = x.astype(jnp.bfloat16)
    return high, (x - high.astype(jnp.float32)).astype(jnp.bfloat16)


def ranks(dest, devices):
    rows = dest.shape[1]
    blocks = rows // LANES
    hot = (iota((devices, rows), 0) == dest).astype(jnp.float32)
    stacked = jnp.concatenate([hot[:, b * LANES : (b + 1) * LANES] for b in range(blocks)], axis=0)
    before = (iota((LANES, LANES), 0) < iota((LANES, LANES), 1)).astype(jnp.float32)
    local = dot(stacked.astype(jnp.bfloat16), before.astype(jnp.bfloat16), ((1,), (0,)))
    carried = jnp.zeros((devices, 1), jnp.float32)
    pieces = []
    for b in range(blocks):
        part = local[b * devices : (b + 1) * devices]
        own = hot[:, b * LANES : (b + 1) * LANES]
        pieces.append(jnp.sum((part + carried) * own, axis=0, keepdims=True))
        carried = carried + jnp.sum(own, axis=1, keepdims=True)
    return jnp.concatenate(pieces, axis=1)


def donor_kernel(count, q_prev, q_now, base_in, frac_in, dest_in, cell_in, out, planes, lhs, spread, corner, place, values, base, frac, dest, cell, sems, *, size, devices, capacity):
    nvars, size_x, size_y, size_z = size
    columns = size_x * size_y
    rows = base.shape[1]
    small = [pltpu.make_async_copy(a, b, sems.at[2 + k]) for k, (a, b) in enumerate(((base_in, base), (frac_in, frac), (dest_in, dest), (cell_in, cell)))]
    copies = [pltpu.make_async_copy(ref, planes.at[k], sems.at[k]) for k, ref in enumerate((q_prev, q_now))]
    for copy in small + copies:
        copy.start()
    for copy in small:
        copy.wait()
    start = base[...].astype(jnp.float32)
    in_y = jnp.floor((start + 0.5) * (1.0 / (size_z - 1)))
    base_z = start - in_y * (size_z - 1)
    base_x = jnp.floor((in_y + 0.5) * (1.0 / (size_y - 1)))
    base_y = in_y - base_x * (size_y - 1)
    frac_x, frac_y, frac_z = frac[0:1, :], frac[1:2, :], frac[2:3, :]

    def weights(first, part, shape):
        at = iota(shape, 0).astype(jnp.float32) - first
        return jnp.where(at == 0.0, 1.0 - part, jnp.where(at == 1.0, part, 0.0))

    along_z = weights(base_z, frac_z, (size_z, rows))
    high, low = halves(along_z)
    spread[0:size_z, :] = high
    spread[size_z : 2 * size_z, :] = low
    spread[2 * size_z : 3 * size_z, :] = high
    along_x = weights(base_x, frac_x, (size_x, rows))
    along_y = weights(base_y, frac_y, (size_y, rows))
    for x in range(size_x):
        corner[x * size_y : (x + 1) * size_y, :] = along_x[x : x + 1, :] * along_y
    alive = iota((1, rows), 1) < count[0]
    slot = ranks(dest[...], devices)
    where_to = jnp.where(alive, dest[...].astype(jnp.float32) * capacity + slot, -1.0)
    place[...] = jnp.transpose(jnp.broadcast_to(where_to, (8, rows)))
    landing = cell[...].astype(jnp.float32)
    land_xy = jnp.floor((landing + 0.5) * (1.0 / size_z))
    values[...] = jnp.zeros(values.shape, jnp.float32)
    values[2 * nvars : 2 * nvars + 1, :] = land_xy + 1.0
    values[2 * nvars + 1 : 2 * nvars + 2, :] = landing - land_xy * size_z
    for k in range(2):
        copies[k].wait()
        for v in range(nvars):
            at = pl.ds((k * nvars + v) * columns, columns)
            high, low = halves(planes[k, v])
            lhs[at, 0:size_z] = high
            lhs[at, size_z : 2 * size_z] = high
            lhs[at, 2 * size_z : 3 * size_z] = low
    for n in range(rows // LANES):
        lanes = slice(n * LANES, (n + 1) * LANES)
        for k in range(2):
            part = dot(lhs[k * nvars * columns : (k + 1) * nvars * columns, :], spread[:, lanes], ((1,), (0,)))
            for v in range(nvars):
                picked = part[v * columns : (v + 1) * columns] * corner[:, lanes]
                values[k * nvars + v : k * nvars + v + 1, lanes] = jnp.sum(picked, axis=0, keepdims=True)
    first = values[...]
    high, rest = first.astype(jnp.bfloat16), None
    rest = first - high.astype(jnp.float32)
    middle = rest.astype(jnp.bfloat16)
    last = (rest - middle.astype(jnp.float32)).astype(jnp.bfloat16)
    three = jnp.concatenate([high, middle, last], axis=0)
    column = jnp.broadcast_to(place[:, 0:1], (rows, LANES))
    for n in range(devices * capacity // LANES):
        chosen = (column == (iota((rows, LANES), 1) + n * LANES).astype(jnp.float32)).astype(jnp.float32).astype(jnp.bfloat16)
        moved = dot(three, chosen, ((1,), (0,)))
        moved = moved[0:CHANNELS] + moved[CHANNELS : 2 * CHANNELS] + moved[2 * CHANNELS : 3 * CHANNELS]
        for d in range(LANES // capacity):
            piece = moved[:, d * capacity : (d + 1) * capacity]
            to = n * (LANES // capacity) + d
            out[to] = jnp.concatenate([piece[0:8], piece[8:16]], axis=1)


def mixing_weights(coef, high, low, size):
    nvars, _, size_y, _ = size
    block = nvars * size_y
    width = 3 * block + CHANNELS
    row = iota((size_y, width), 0)
    offset = iota((size_y, width), 1) - row
    lane = iota((size_y, width), 1)

    def at(d, side, a, b):
        return coef[((d * 2 + side) * nvars + a) * nvars + b]

    for a in range(nvars):
        main = jnp.zeros((size_y, width), jnp.float32)
        back = main
        fore = main
        for b in range(nvars):
            first = b * size_y
            same = at(0, 0, a, b) - at(0, 1, a, b) + at(1, 0, a, b) - at(1, 1, a, b) + at(2, 0, a, b) - at(2, 1, a, b)
            main = jnp.where(offset == first, -at(0, 0, a, b), main)
            main = jnp.where(offset == block + first, same, main)
            main = jnp.where((offset == block + first - 1) & (row > 0), -at(1, 0, a, b), main)
            main = jnp.where((offset == block + first + 1) & (row < size_y - 1), at(1, 1, a, b), main)
            main = jnp.where(offset == 2 * block + first, at(0, 1, a, b), main)
            main = jnp.where((lane == 3 * block + b) & (row == 0), -at(1, 0, a, b), main)
            main = jnp.where((lane == 3 * block + nvars + b) & (row == size_y - 1), at(1, 1, a, b), main)
            back = jnp.where(offset == block + first, -at(2, 0, a, b), back)
            fore = jnp.where(offset == block + first, at(2, 1, a, b), fore)
        for k, part in enumerate((main, back, fore)):
            rows = slice(k * block + a * size_y, k * block + (a + 1) * size_y)
            high[rows, :], low[rows, :] = halves(part)


def fill_planes(state, x_low, x_high, y_low, y_high, planes, sides, size):
    nvars, size_x, size_y, _ = size
    block = nvars * size_y
    for x in range(size_x + 2):
        for v in range(nvars):
            value = x_low[v] if x == 0 else x_high[v] if x == size_x + 1 else state[v, x - 1]
            rows = slice(x * block + v * size_y, x * block + (v + 1) * size_y)
            planes[0, rows, :], planes[1, rows, :] = halves(value)
    sides[...] = jnp.zeros(sides.shape, jnp.float32)
    for v in range(nvars):
        sides[:, v, :] = y_low[v]
        sides[:, nvars + v, :] = y_high[v]


def flux_at(x, weights, planes, sides, size):
    nvars, _, size_y, size_z = size
    block = nvars * size_y
    high, low = halves(sides[x])
    rows = slice(x * block, (x + 3) * block)
    around_high = jnp.concatenate([planes[0, rows, :], high], axis=0)
    around_low = jnp.concatenate([planes[1, rows, :], low], axis=0)
    both = jnp.concatenate([weights[0], weights[1]], axis=0)
    mixed = dot(both, around_high, ((1,), (0,)))
    mixed = mixed[0 : 3 * block] + mixed[3 * block :] + dot(weights[0], around_low, ((1,), (0,)))
    z_at = iota((block, size_z), 1)
    back = jnp.where(z_at == 0, 0.0, pltpu.roll(mixed[block : 2 * block], 1, 1))
    fore = jnp.where(z_at == size_z - 1, 0.0, pltpu.roll(mixed[2 * block :], size_z - 1, 1))
    flux = mixed[0:block] + back + fore
    return [flux[v * size_y : (v + 1) * size_y] for v in range(nvars)]


def early_kernel(coef, q_now, q_prev, jac, x_low, x_high, y_low, y_high, base, weights, planes, sides, *, size):
    nvars, size_x, _, _ = size
    mixing_weights(coef, weights.at[0], weights.at[1], size)
    fill_planes(q_now, x_low, x_high, y_low, y_high, planes, sides, size)
    for x in range(size_x):
        flux = flux_at(x, weights, planes, sides, size)
        scale = step_tau * jac[x]
        for v in range(nvars):
            centre = q_now[v, x]
            physical = (q_prev[v, x] - centre) / (2.0 * step_phys)
            base[v, x] = centre - scale * (flux[v] + physical)


def land(rows, hot_xy, hot_z, store, nvars):
    columns = hot_xy.shape[0]
    for first in range(0, nvars, 2):
        some = range(first, min(first + 2, nvars))
        pieces = []
        for c in some:
            for half in halves(rows[c : c + 1, :]):
                pieces.append(hot_xy[...] * half)
        landed = dot(jnp.concatenate(pieces, axis=0), hot_z[...], ((1,), (0,)))
        for c in some:
            at = 2 * (c - first) * columns
            store(c, landed[at : at + columns] + landed[at + columns : at + 2 * columns])


def first_kernel(got, base, q_now, jac, state, hits, face_xl, face_xh, face_yl, face_yh, later, hot_xy, hot_z, rows, grid, *, size, devices, capacity):
    nvars, size_x, size_y, size_z = size
    columns = size_x * size_y
    slots = devices * capacity
    for d in range(devices):
        piece = got[d]
        lanes = slice(d * capacity, (d + 1) * capacity)
        rows[0:8, lanes] = piece[:, 0:capacity]
        rows[8:16, lanes] = piece[:, capacity : 2 * capacity]
    turned = jnp.transpose(rows[8:16, :])
    land_z = turned[:, 2 * nvars + 1 - 8 : 2 * nvars + 2 - 8]
    hot_z[...] = (iota((slots, size_z), 1).astype(jnp.float32) == land_z).astype(jnp.float32).astype(jnp.bfloat16)
    land_xy = rows[2 * nvars : 2 * nvars + 1, :]
    hot_xy[...] = ((iota((columns, slots), 0) + 1).astype(jnp.float32) == land_xy).astype(jnp.float32).astype(jnp.bfloat16)
    later[...] = rows[nvars : 2 * nvars, :]

    def keep(c, value):
        grid[c] = value

    hits[...] = dot(hot_xy[...], hot_z[...], ((1,), (0,)))
    land(rows, hot_xy, hot_z, keep, nvars)
    for x in range(size_x):
        at = slice(x * size_y, (x + 1) * size_y)
        landed = hits[at, :]
        scale = (step_tau * penalty) * jac[x]
        for v in range(nvars):
            new = base[v, x] - scale * (landed * q_now[v, x] - grid[v, at, :])
            state[v, x] = new
            face_yl[v, x : x + 1, :] = new[0:1]
            face_yh[v, x : x + 1, :] = new[size_y - 1 : size_y]
            if x == 0:
                face_xl[v] = new
            if x == size_x - 1:
                face_xh[v] = new


def late_kernel(rows, hot_xy, hot_z, target):
    def keep(c, value):
        target[c] = value

    land(rows, hot_xy, hot_z, keep, rows.shape[0])


def second_kernel(state, weights, q_now, q_prev, jac, target, hits, x_low, x_high, y_low, y_high, out, planes, sides, buffer, sems, *, size):
    nvars, size_x, size_y, _ = size
    fill_planes(state, x_low, x_high, y_low, y_high, planes, sides, size)
    part = size_x // 4
    copies = []
    for x in range(size_x):
        at = slice(x * size_y, (x + 1) * size_y)
        flux = flux_at(x, weights, planes, sides, size)
        landed = hits[at, :]
        scale = step_tau * jac[x]
        for v in range(nvars):
            centre = state[v, x]
            physical = (3.0 * centre - 4.0 * q_now[v, x] + q_prev[v, x]) / (2.0 * step_phys)
            coupling = penalty * (landed * centre - target[v, at, :])
            buffer[v, x] = centre - scale * (flux[v] + physical + coupling)
        if (x + 1) % part == 0:
            some = pl.ds(x + 1 - part, part)
            copies.append(pltpu.make_async_copy(buffer.at[:, some], out.at[:, some], sems.at[x // part]))
            copies[-1].start()
    for copy in copies:
        copy.wait()


def swap_pairs(axis, odd):
    count = lax.axis_size(axis)
    pairs = []
    for i in range(odd, count - 1, 2):
        pairs += [(i, i + 1), (i + 1, i)]
    return pairs


def exchanged(low_face, high_face, axis):
    here = lax.axis_index(axis)
    even = here % 2 == 0
    inner = lax.ppermute(jnp.where(even, high_face, low_face), axis, swap_pairs(axis, 0))
    outer = lax.ppermute(jnp.where(even, low_face, high_face), axis, swap_pairs(axis, 1))
    return jnp.where(even, outer, inner), jnp.where(even, inner, outer)


def params(limit):
    return pltpu.CompilerParams(vmem_limit_bytes=limit)


def edges(halo, axis):
    here, last = lax.axis_index(axis), lax.axis_size(axis) - 1
    return jnp.where(here == 0, 0.0, halo[0]), jnp.where(here == last, 0.0, halo[1])


def body(q_now, q_prev, jacobian, flux_split, donor_base, donor_frac, fringe_dest, receptor_cell, fringe_count):
    size = q_now.shape
    nvars, size_x, size_y, size_z = size
    columns = size_x * size_y
    block = nvars * size_y
    devices = lax.axis_size("gx") * lax.axis_size("gy")
    rows = donor_base.shape[0]
    capacity = 2 * rows // devices
    slots = devices * capacity
    f32, bf16 = jnp.float32, jnp.bfloat16
    smem = pl.BlockSpec(memory_space=pltpu.SMEM)
    hbm = pl.BlockSpec(memory_space=pltpu.HBM)
    vmem = pl.BlockSpec(memory_space=pltpu.VMEM)
    flat = (nvars, columns, size_z)
    shape = jax.ShapeDtypeStruct
    weights_shape = (2, 3 * block, 3 * block + CHANNELS)
    planes = pltpu.VMEM((2, (size_x + 2) * block, size_z), bf16)
    sides = pltpu.VMEM((size_x, CHANNELS, size_z), f32)
    face_x, face_y = shape((nvars, size_y, size_z), f32), shape((nvars, size_x, size_z), f32)

    def halos(low_x, high_x, low_y, high_y):
        x_halo = exchanged(low_x, high_x, "gx")
        y_halo = exchanged(low_y, high_y, "gy")
        return *edges(x_halo, "gx"), *edges(y_halo, "gy")

    around = halos(q_now[:, 0], q_now[:, size_x - 1], q_now[:, :, 0], q_now[:, :, size_y - 1])
    sent = pl.pallas_call(
        functools.partial(donor_kernel, size=size, devices=devices, capacity=capacity),
        out_shape=shape((devices, 8, 2 * capacity), f32),
        in_specs=[smem] + [hbm] * 6,
        out_specs=vmem,
        scratch_shapes=[
            pltpu.VMEM((2, nvars, columns, size_z), f32),
            pltpu.VMEM((2 * nvars * columns, 3 * size_z), bf16),
            pltpu.VMEM((3 * size_z, rows), bf16),
            pltpu.VMEM((columns, rows), f32),
            pltpu.VMEM((rows, 8), f32),
            pltpu.VMEM((CHANNELS, rows), f32),
            pltpu.VMEM((1, rows), jnp.int32),
            pltpu.VMEM((3, rows), f32),
            pltpu.VMEM((1, rows), jnp.int32),
            pltpu.VMEM((1, rows), jnp.int32),
            pltpu.SemaphoreType.DMA((6,)),
        ],
        compiler_params=params(60 * 1024 * 1024),
        name="donor",
    )(
        fringe_count,
        q_prev.reshape(flat),
        q_now.reshape(flat),
        donor_base.reshape(1, rows),
        donor_frac,
        fringe_dest.reshape(1, rows),
        receptor_cell.reshape(1, rows),
    )
    got = lax.all_to_all(sent, AXES, split_axis=0, concat_axis=0, tiled=True)
    base, weights = pl.pallas_call(
        functools.partial(early_kernel, size=size),
        out_shape=[shape(size, f32), shape(weights_shape, bf16)],
        in_specs=[smem] + [vmem] * 7,
        out_specs=[vmem] * 2,
        scratch_shapes=[planes, sides],
        compiler_params=params(20 * MIB),
        name="early",
    )(flux_split.reshape(-1), q_now, q_prev, jacobian, *around)
    state, hits, *faces, later, hot_xy, hot_z = pl.pallas_call(
        functools.partial(first_kernel, size=size, devices=devices, capacity=capacity),
        out_shape=[
            shape(size, f32),
            shape((columns, size_z), f32),
            face_x,
            face_x,
            face_y,
            face_y,
            shape((nvars, slots), f32),
            shape((columns, slots), bf16),
            shape((slots, size_z), bf16),
        ],
        in_specs=[vmem] * 4,
        out_specs=[vmem] * 9,
        scratch_shapes=[pltpu.VMEM((CHANNELS, slots), f32), pltpu.VMEM((nvars, columns, size_z), f32)],
        compiler_params=params(20 * MIB),
        name="first",
    )(got, base, q_now, jacobian)
    around = halos(*faces)
    target = pl.pallas_call(
        late_kernel,
        out_shape=shape(flat, f32),
        in_specs=[vmem] * 3,
        out_specs=vmem,
        compiler_params=params(20 * MIB),
        name="late",
    )(later, hot_xy, hot_z)
    return pl.pallas_call(
        functools.partial(second_kernel, size=size),
        out_shape=shape(size, f32),
        in_specs=[vmem] * 11,
        out_specs=hbm,
        scratch_shapes=[planes, sides, pltpu.VMEM(size, f32), pltpu.SemaphoreType.DMA((4,))],
        compiler_params=params(20 * MIB),
        name="second",
    )(state, weights, q_now, q_prev, jacobian, target, hits, *around)


def solution(mesh):
    return jax.shard_map(
        body,
        mesh=mesh,
        in_specs=(
            P(None, "gx", "gy", None),
            P(None, "gx", "gy", None),
            P("gx", "gy", None),
            P(),
            P(("gx", "gy")),
            P(None, ("gx", "gy")),
            P(("gx", "gy"), None),
            P(("gx", "gy")),
            P(("gx", "gy")),
        ),
        out_specs=P(None, "gx", "gy", None),
        check_vma=False,
    )
```

```python
import functools

import jax
import jax.numpy as jnp
from jax import lax
from jax.experimental import pallas as pl
from jax.experimental.pallas import tpu as pltpu
from jax.sharding import PartitionSpec as P


step_tau = 0.2
step_phys = 0.5
penalty = 2.0

AXES = ("gx", "gy")
LANES = 256
CHANNELS = 16
MIB = 1 << 20


def iota(shape, dim):
    return lax.broadcasted_iota(jnp.int32, shape, dim)


def dot(a, b, dims):
    return lax.dot_general(a, b, (dims, ((), ())), preferred_element_type=jnp.float32)


def halves(x):
    high = x.astype(jnp.bfloat16)
    return high, (x - high.astype(jnp.float32)).astype(jnp.bfloat16)


def ranks(dest, devices):
    rows = dest.shape[1]
    blocks = rows // LANES
    hot = (iota((devices, rows), 0) == dest).astype(jnp.float32)
    stacked = jnp.concatenate([hot[:, b * LANES : (b + 1) * LANES] for b in range(blocks)], axis=0)
    before = (iota((LANES, LANES), 0) < iota((LANES, LANES), 1)).astype(jnp.float32)
    local = dot(stacked.astype(jnp.bfloat16), before.astype(jnp.bfloat16), ((1,), (0,)))
    carried = jnp.zeros((devices, 1), jnp.float32)
    pieces = []
    for b in range(blocks):
        part = local[b * devices : (b + 1) * devices]
        own = hot[:, b * LANES : (b + 1) * LANES]
        pieces.append(jnp.sum((part + carried) * own, axis=0, keepdims=True))
        carried = carried + jnp.sum(own, axis=1, keepdims=True)
    return jnp.concatenate(pieces, axis=1)


def donor_kernel(count, q_prev, q_now, base_in, frac_in, dest_in, cell_in, out, planes, lhs, spread, corner, place, values, base, frac, dest, cell, sems, *, size, devices, capacity):
    nvars, size_x, size_y, size_z = size
    columns = size_x * size_y
    rows = base.shape[1]
    small = [pltpu.make_async_copy(a, b, sems.at[2 + k]) for k, (a, b) in enumerate(((base_in, base), (frac_in, frac), (dest_in, dest), (cell_in, cell)))]
    copies = [pltpu.make_async_copy(ref, planes.at[k], sems.at[k]) for k, ref in enumerate((q_prev, q_now))]
    for copy in small + copies:
        copy.start()
    for copy in small:
        copy.wait()
    start = base[...].astype(jnp.float32)
    in_y = jnp.floor((start + 0.5) * (1.0 / (size_z - 1)))
    base_z = start - in_y * (size_z - 1)
    base_x = jnp.floor((in_y + 0.5) * (1.0 / (size_y - 1)))
    base_y = in_y - base_x * (size_y - 1)
    frac_x, frac_y, frac_z = frac[0:1, :], frac[1:2, :], frac[2:3, :]

    def weights(first, part, shape):
        at = iota(shape, 0).astype(jnp.float32) - first
        return jnp.where(at == 0.0, 1.0 - part, jnp.where(at == 1.0, part, 0.0))

    along_z = weights(base_z, frac_z, (size_z, rows))
    high, low = halves(along_z)
    spread[0] = high
    spread[1] = low
    along_x = weights(base_x, frac_x, (size_x, rows))
    along_y = weights(base_y, frac_y, (size_y, rows))
    for x in range(size_x):
        corner[x * size_y : (x + 1) * size_y, :] = along_x[x : x + 1, :] * along_y
    alive = iota((1, rows), 1) < count[0]
    slot = ranks(dest[...], devices)
    where_to = jnp.where(alive, dest[...].astype(jnp.float32) * capacity + slot, -1.0)
    place[...] = jnp.transpose(jnp.broadcast_to(where_to, (8, rows)))
    landing = cell[...].astype(jnp.float32)
    land_xy = jnp.floor((landing + 0.5) * (1.0 / size_z))
    values[...] = jnp.zeros(values.shape, jnp.float32)
    values[2 * nvars : 2 * nvars + 1, :] = land_xy + 1.0
    values[2 * nvars + 1 : 2 * nvars + 2, :] = landing - land_xy * size_z
    for k in range(2):
        copies[k].wait()
        for v in range(nvars):
            at = pl.ds((k * nvars + v) * columns, columns)
            high, low = halves(planes[k, v])
            lhs[0, at, :] = high
            lhs[1, at, :] = low
    for n in range(rows // LANES):
        lanes = slice(n * LANES, (n + 1) * LANES)
        for k in range(2):
            at = slice(k * nvars * columns, (k + 1) * nvars * columns)
            part = dot(lhs[0, at, :], spread[0, :, lanes], ((1,), (0,)))
            part = part + dot(lhs[0, at, :], spread[1, :, lanes], ((1,), (0,)))
            part = part + dot(lhs[1, at, :], spread[0, :, lanes], ((1,), (0,)))
            for v in range(nvars):
                picked = part[v * columns : (v + 1) * columns] * corner[:, lanes]
                values[k * nvars + v : k * nvars + v + 1, lanes] = jnp.sum(picked, axis=0, keepdims=True)
    first = values[...]
    high, rest = first.astype(jnp.bfloat16), None
    rest = first - high.astype(jnp.float32)
    middle = rest.astype(jnp.bfloat16)
    last = (rest - middle.astype(jnp.float32)).astype(jnp.bfloat16)
    three = jnp.concatenate([high, middle, last], axis=0)
    column = jnp.broadcast_to(place[:, 0:1], (rows, LANES))
    for n in range(devices * capacity // LANES):
        chosen = (column == (iota((rows, LANES), 1) + n * LANES).astype(jnp.float32)).astype(jnp.float32).astype(jnp.bfloat16)
        moved = dot(three, chosen, ((1,), (0,)))
        moved = moved[0:CHANNELS] + moved[CHANNELS : 2 * CHANNELS] + moved[2 * CHANNELS : 3 * CHANNELS]
        for d in range(LANES // capacity):
            piece = moved[:, d * capacity : (d + 1) * capacity]
            to = n * (LANES // capacity) + d
            out[to] = jnp.concatenate([piece[0:8], piece[8:16]], axis=1)


def mixing_weights(coef, high, low, size):
    nvars, _, size_y, _ = size
    block = nvars * size_y
    width = 3 * block + CHANNELS
    row = iota((size_y, width), 0)
    offset = iota((size_y, width), 1) - row
    lane = iota((size_y, width), 1)

    def at(d, side, a, b):
        return coef[((d * 2 + side) * nvars + a) * nvars + b]

    for a in range(nvars):
        main = jnp.zeros((size_y, width), jnp.float32)
        back = main
        fore = main
        for b in range(nvars):
            first = b * size_y
            same = at(0, 0, a, b) - at(0, 1, a, b) + at(1, 0, a, b) - at(1, 1, a, b) + at(2, 0, a, b) - at(2, 1, a, b)
            main = jnp.where(offset == first, -at(0, 0, a, b), main)
            main = jnp.where(offset == block + first, same, main)
            main = jnp.where((offset == block + first - 1) & (row > 0), -at(1, 0, a, b), main)
            main = jnp.where((offset == block + first + 1) & (row < size_y - 1), at(1, 1, a, b), main)
            main = jnp.where(offset == 2 * block + first, at(0, 1, a, b), main)
            main = jnp.where((lane == 3 * block + b) & (row == 0), -at(1, 0, a, b), main)
            main = jnp.where((lane == 3 * block + nvars + b) & (row == size_y - 1), at(1, 1, a, b), main)
            back = jnp.where(offset == block + first, -at(2, 0, a, b), back)
            fore = jnp.where(offset == block + first, at(2, 1, a, b), fore)
        for k, part in enumerate((main, back, fore)):
            rows = slice(k * block + a * size_y, k * block + (a + 1) * size_y)
            high[rows, :], low[rows, :] = halves(part)


def fill_planes(state, around, planes, sides, size):
    nvars, size_x, size_y, size_z = size
    block = nvars * size_y
    for x in range(size_x + 2):
        for v in range(nvars):
            rows = slice(x * block + v * size_y, x * block + (v + 1) * size_y)
            if 0 < x <= size_x:
                planes[0, rows, :], planes[1, rows, :] = halves(state[v, x - 1])
            elif around is None:
                planes[0, rows, :] = planes[1, rows, :] = jnp.zeros((size_y, size_z), jnp.bfloat16)
            else:
                planes[0, rows, :], planes[1, rows, :] = halves(around[0 if x == 0 else 1][v])
    if around is not None:
        sides[...] = jnp.zeros(sides.shape, jnp.float32)
        for v in range(nvars):
            sides[:, v, :] = around[2][v]
            sides[:, nvars + v, :] = around[3][v]


def flux_at(x, weights, planes, sides, size):
    nvars, _, size_y, size_z = size
    block = nvars * size_y
    if sides is None:
        high = low = jnp.zeros((CHANNELS, size_z), jnp.bfloat16)
    else:
        high, low = halves(sides[x])
    rows = slice(x * block, (x + 3) * block)
    around_high = jnp.concatenate([planes[0, rows, :], high], axis=0)
    around_low = jnp.concatenate([planes[1, rows, :], low], axis=0)
    both = jnp.concatenate([weights[0], weights[1]], axis=0)
    mixed = dot(both, around_high, ((1,), (0,)))
    mixed = mixed[0 : 3 * block] + mixed[3 * block :] + dot(weights[0], around_low, ((1,), (0,)))
    z_at = iota((block, size_z), 1)
    back = jnp.where(z_at == 0, 0.0, pltpu.roll(mixed[block : 2 * block], 1, 1))
    fore = jnp.where(z_at == size_z - 1, 0.0, pltpu.roll(mixed[2 * block :], size_z - 1, 1))
    flux = mixed[0:block] + back + fore
    return [flux[v * size_y : (v + 1) * size_y] for v in range(nvars)]


def sent_out(x, size_x, buffer, out, sems, copies):
    part = size_x // 4
    if (x + 1) % part == 0:
        some = pl.ds(x + 1 - part, part)
        copies.append(pltpu.make_async_copy(buffer.at[:, some], out.at[:, some], sems.at[x // part]))
        copies[-1].start()


def early_kernel(coef, q_now, q_prev, jac, base, weights, planes, buffer, sems, *, size):
    nvars, size_x, _, _ = size
    mixing_weights(coef, weights.at[0], weights.at[1], size)
    fill_planes(q_now, None, planes, None, size)
    copies = []
    for x in range(size_x):
        flux = flux_at(x, weights, planes, None, size)
        scale = step_tau * jac[x]
        for v in range(nvars):
            centre = q_now[v, x]
            physical = (q_prev[v, x] - centre) / (2.0 * step_phys)
            buffer[v, x] = centre - scale * (flux[v] + physical)
        sent_out(x, size_x, buffer, base, sems, copies)
    for copy in copies:
        copy.wait()


def crossing(coef, direction, low, high, nvars):
    parts = []
    for side, face in enumerate((low, high)):
        mixed = []
        for a in range(nvars):
            total = None
            for b in range(nvars):
                term = coef[((direction * 2 + side) * nvars + a) * nvars + b] * face[b]
                total = term if total is None else total + term
            mixed.append(total if side else -total)
        parts.append(mixed)
    return parts


def land(rows, hot_xy, hot_z, store, nvars):
    columns = hot_xy.shape[0]
    for first in range(0, nvars, 2):
        some = range(first, min(first + 2, nvars))
        pieces = []
        for c in some:
            for half in halves(rows[c : c + 1, :]):
                pieces.append(hot_xy[...] * half)
        landed = dot(jnp.concatenate(pieces, axis=0), hot_z[...], ((1,), (0,)))
        for c in some:
            at = 2 * (c - first) * columns
            store(c, landed[at : at + columns] + landed[at + columns : at + 2 * columns])


def first_kernel(coef, got, base_in, q_now, jac, x_low, x_high, y_low, y_high, state, hits, face_xl, face_xh, face_yl, face_yh, later, hot_xy, hot_z, rows, grid, base, sem, *, size, devices, capacity):
    nvars, size_x, size_y, size_z = size
    columns = size_x * size_y
    slots = devices * capacity
    fetch = pltpu.make_async_copy(base_in, base, sem)
    fetch.start()
    for d in range(devices):
        piece = got[d]
        lanes = slice(d * capacity, (d + 1) * capacity)
        rows[0:8, lanes] = piece[:, 0:capacity]
        rows[8:16, lanes] = piece[:, capacity : 2 * capacity]
    turned = jnp.transpose(rows[8:16, :])
    land_z = turned[:, 2 * nvars + 1 - 8 : 2 * nvars + 2 - 8]
    hot_z[...] = (iota((slots, size_z), 1).astype(jnp.float32) == land_z).astype(jnp.float32).astype(jnp.bfloat16)
    land_xy = rows[2 * nvars : 2 * nvars + 1, :]
    hot_xy[...] = ((iota((columns, slots), 0) + 1).astype(jnp.float32) == land_xy).astype(jnp.float32).astype(jnp.bfloat16)
    later[...] = rows[nvars : 2 * nvars, :]

    def keep(c, value):
        grid[c] = value

    hits[...] = dot(hot_xy[...], hot_z[...], ((1,), (0,)))
    land(rows, hot_xy, hot_z, keep, nvars)
    from_x = crossing(coef, 0, x_low, x_high, nvars)
    from_y = crossing(coef, 1, y_low, y_high, nvars)
    row_at = iota((size_y, size_z), 0)
    fetch.wait()
    for x in range(size_x):
        at = slice(x * size_y, (x + 1) * size_y)
        landed = hits[at, :]
        scale = step_tau * jac[x]
        for v in range(nvars):
            change = penalty * (landed * q_now[v, x] - grid[v, at, :])
            change = change + jnp.where(row_at == 0, from_y[0][v][x : x + 1], 0.0)
            change = change + jnp.where(row_at == size_y - 1, from_y[1][v][x : x + 1], 0.0)
            if x == 0:
                change = change + from_x[0][v]
            if x == size_x - 1:
                change = change + from_x[1][v]
            new = base[v, x] - scale * change
            state[v, x] = new
            face_yl[v, x : x + 1, :] = new[0:1]
            face_yh[v, x : x + 1, :] = new[size_y - 1 : size_y]
            if x == 0:
                face_xl[v] = new
            if x == size_x - 1:
                face_xh[v] = new


def late_kernel(rows, hot_xy, hot_z, target):
    def keep(c, value):
        target[c] = value

    land(rows, hot_xy, hot_z, keep, rows.shape[0])


def second_kernel(state, weights, q_now, q_prev, jac, target, hits, x_low, x_high, y_low, y_high, out, planes, sides, buffer, sems, *, size):
    nvars, size_x, size_y, _ = size
    fill_planes(state, (x_low, x_high, y_low, y_high), planes, sides, size)
    copies = []
    for x in range(size_x):
        at = slice(x * size_y, (x + 1) * size_y)
        flux = flux_at(x, weights, planes, sides, size)
        landed = hits[at, :]
        scale = step_tau * jac[x]
        for v in range(nvars):
            centre = state[v, x]
            physical = (3.0 * centre - 4.0 * q_now[v, x] + q_prev[v, x]) / (2.0 * step_phys)
            coupling = penalty * (landed * centre - target[v, at, :])
            buffer[v, x] = centre - scale * (flux[v] + physical + coupling)
        sent_out(x, size_x, buffer, out, sems, copies)
    for copy in copies:
        copy.wait()


def swap_pairs(axis, odd):
    count = lax.axis_size(axis)
    pairs = []
    for i in range(odd, count - 1, 2):
        pairs += [(i, i + 1), (i + 1, i)]
    return pairs


def exchanged(low_face, high_face, axis):
    here = lax.axis_index(axis)
    even = here % 2 == 0
    inner = lax.ppermute(jnp.where(even, high_face, low_face), axis, swap_pairs(axis, 0))
    outer = lax.ppermute(jnp.where(even, low_face, high_face), axis, swap_pairs(axis, 1))
    return jnp.where(even, outer, inner), jnp.where(even, inner, outer)


def params(limit):
    return pltpu.CompilerParams(vmem_limit_bytes=limit)


def edges(halo, axis):
    here, last = lax.axis_index(axis), lax.axis_size(axis) - 1
    return jnp.where(here == 0, 0.0, halo[0]), jnp.where(here == last, 0.0, halo[1])


def body(q_now, q_prev, jacobian, flux_split, donor_base, donor_frac, fringe_dest, receptor_cell, fringe_count):
    size = q_now.shape
    nvars, size_x, size_y, size_z = size
    columns = size_x * size_y
    block = nvars * size_y
    devices = lax.axis_size("gx") * lax.axis_size("gy")
    rows = donor_base.shape[0]
    capacity = 2 * rows // devices
    slots = devices * capacity
    f32, bf16 = jnp.float32, jnp.bfloat16
    smem = pl.BlockSpec(memory_space=pltpu.SMEM)
    hbm = pl.BlockSpec(memory_space=pltpu.HBM)
    vmem = pl.BlockSpec(memory_space=pltpu.VMEM)
    flat = (nvars, columns, size_z)
    shape = jax.ShapeDtypeStruct
    weights_shape = (2, 3 * block, 3 * block + CHANNELS)
    planes = pltpu.VMEM((2, (size_x + 2) * block, size_z), bf16)
    sides = pltpu.VMEM((size_x, CHANNELS, size_z), f32)
    face_x, face_y = shape((nvars, size_y, size_z), f32), shape((nvars, size_x, size_z), f32)

    def halos(low_x, high_x, low_y, high_y):
        x_halo = exchanged(low_x, high_x, "gx")
        y_halo = exchanged(low_y, high_y, "gy")
        return *edges(x_halo, "gx"), *edges(y_halo, "gy")

    coef = flux_split.reshape(-1)
    around = halos(q_now[:, 0], q_now[:, size_x - 1], q_now[:, :, 0], q_now[:, :, size_y - 1])
    sent = pl.pallas_call(
        functools.partial(donor_kernel, size=size, devices=devices, capacity=capacity),
        out_shape=shape((devices, 8, 2 * capacity), f32),
        in_specs=[smem] + [hbm] * 6,
        out_specs=vmem,
        scratch_shapes=[
            pltpu.VMEM((2, nvars, columns, size_z), f32),
            pltpu.VMEM((2, 2 * nvars * columns, size_z), bf16),
            pltpu.VMEM((2, size_z, rows), bf16),
            pltpu.VMEM((columns, rows), f32),
            pltpu.VMEM((rows, 8), f32),
            pltpu.VMEM((CHANNELS, rows), f32),
            pltpu.VMEM((1, rows), jnp.int32),
            pltpu.VMEM((3, rows), f32),
            pltpu.VMEM((1, rows), jnp.int32),
            pltpu.VMEM((1, rows), jnp.int32),
            pltpu.SemaphoreType.DMA((6,)),
        ],
        compiler_params=params(60 * 1024 * 1024),
        name="donor",
    )(
        fringe_count,
        q_prev.reshape(flat),
        q_now.reshape(flat),
        donor_base.reshape(1, rows),
        donor_frac,
        fringe_dest.reshape(1, rows),
        receptor_cell.reshape(1, rows),
    )
    got = lax.all_to_all(sent, AXES, split_axis=0, concat_axis=0, tiled=True)
    base, weights = pl.pallas_call(
        functools.partial(early_kernel, size=size),
        out_shape=[pltpu.HBM(size, f32), shape(weights_shape, bf16)],
        in_specs=[smem] + [vmem] * 3,
        out_specs=[hbm, vmem],
        scratch_shapes=[planes, pltpu.VMEM(size, f32), pltpu.SemaphoreType.DMA((4,))],
        compiler_params=params(20 * MIB),
        name="early",
    )(coef, q_now, q_prev, jacobian)
    state, hits, *faces, later, hot_xy, hot_z = pl.pallas_call(
        functools.partial(first_kernel, size=size, devices=devices, capacity=capacity),
        out_shape=[
            shape(size, f32),
            shape((columns, size_z), f32),
            face_x,
            face_x,
            face_y,
            face_y,
            shape((nvars, slots), f32),
            shape((columns, slots), bf16),
            shape((slots, size_z), bf16),
        ],
        in_specs=[smem, vmem, hbm] + [vmem] * 6,
        out_specs=[vmem] * 9,
        scratch_shapes=[
            pltpu.VMEM((CHANNELS, slots), f32),
            pltpu.VMEM((nvars, columns, size_z), f32),
            pltpu.VMEM(size, f32),
            pltpu.SemaphoreType.DMA,
        ],
        compiler_params=params(20 * MIB),
        name="first",
    )(coef, got, pltpu.with_memory_space_constraint(base, pltpu.HBM), q_now, jacobian, *around)
    around = halos(*faces)
    target = pl.pallas_call(
        late_kernel,
        out_shape=shape(flat, f32),
        in_specs=[vmem] * 3,
        out_specs=vmem,
        compiler_params=params(20 * MIB),
        name="late",
    )(later, hot_xy, hot_z)
    return pl.pallas_call(
        functools.partial(second_kernel, size=size),
        out_shape=shape(size, f32),
        in_specs=[vmem] * 11,
        out_specs=hbm,
        scratch_shapes=[planes, sides, pltpu.VMEM(size, f32), pltpu.SemaphoreType.DMA((4,))],
        compiler_params=params(20 * MIB),
        name="second",
    )(state, weights, q_now, q_prev, jacobian, target, hits, *around)


def solution(mesh):
    return jax.shard_map(
        body,
        mesh=mesh,
        in_specs=(
            P(None, "gx", "gy", None),
            P(None, "gx", "gy", None),
            P("gx", "gy", None),
            P(),
            P(("gx", "gy")),
            P(None, ("gx", "gy")),
            P(("gx", "gy"), None),
            P(("gx", "gy")),
            P(("gx", "gy")),
        ),
        out_specs=P(None, "gx", "gy", None),
        check_vma=False,
    )
```

```python
import functools

import jax
import jax.numpy as jnp
from jax import lax
from jax.experimental import pallas as pl
from jax.experimental.pallas import tpu as pltpu
from jax.sharding import PartitionSpec as P


step_tau = 0.2
step_phys = 0.5
penalty = 2.0

AXES = ("gx", "gy")
LANES = 256
CHANNELS = 16
MIB = 1 << 20
DONOR_LIMIT = 44 * MIB


def iota(shape, dim):
    return lax.broadcasted_iota(jnp.int32, shape, dim)


def dot(a, b, dims):
    return lax.dot_general(a, b, (dims, ((), ())), preferred_element_type=jnp.float32)


def halves(x):
    high = x.astype(jnp.bfloat16)
    return high, (x - high.astype(jnp.float32)).astype(jnp.bfloat16)


def ranks(dest, devices):
    rows = dest.shape[1]
    blocks = rows // LANES
    hot = (iota((devices, rows), 0) == dest).astype(jnp.float32)
    stacked = jnp.concatenate([hot[:, b * LANES : (b + 1) * LANES] for b in range(blocks)], axis=0)
    before = (iota((LANES, LANES), 0) < iota((LANES, LANES), 1)).astype(jnp.float32)
    local = dot(stacked.astype(jnp.bfloat16), before.astype(jnp.bfloat16), ((1,), (0,)))
    carried = jnp.zeros((devices, 1), jnp.float32)
    pieces = []
    for b in range(blocks):
        part = local[b * devices : (b + 1) * devices]
        own = hot[:, b * LANES : (b + 1) * LANES]
        pieces.append(jnp.sum((part + carried) * own, axis=0, keepdims=True))
        carried = carried + jnp.sum(own, axis=1, keepdims=True)
    return jnp.concatenate(pieces, axis=1)


def donor_kernel(count, parity, q_prev, q_now, base_in, frac_in, dest_in, cell_in, jac_in, out, y_inner, y_outer, planes, jac, lhs, spread, corner, place, values, base, frac, dest, cell, sems, *, size, devices, capacity):
    nvars, size_x, size_y, size_z = size
    columns = size_x * size_y
    rows = base.shape[1]
    small = [pltpu.make_async_copy(a, b, sems.at[2 + k]) for k, (a, b) in enumerate(((base_in, base), (frac_in, frac), (dest_in, dest), (cell_in, cell), (jac_in, jac)))]
    copies = [pltpu.make_async_copy(ref, planes.at[k], sems.at[k]) for k, ref in enumerate((q_prev, q_now))]
    for copy in small + copies:
        copy.start()
    for copy in small[0:4]:
        copy.wait()
    start = base[...].astype(jnp.float32)
    in_y = jnp.floor((start + 0.5) * (1.0 / (size_z - 1)))
    base_z = start - in_y * (size_z - 1)
    base_x = jnp.floor((in_y + 0.5) * (1.0 / (size_y - 1)))
    base_y = in_y - base_x * (size_y - 1)
    frac_x, frac_y, frac_z = frac[0:1, :], frac[1:2, :], frac[2:3, :]

    def weights(first, part, shape):
        at = iota(shape, 0).astype(jnp.float32) - first
        return jnp.where(at == 0.0, 1.0 - part, jnp.where(at == 1.0, part, 0.0))

    along_z = weights(base_z, frac_z, (size_z, rows))
    high, low = halves(along_z)
    spread[0] = high
    spread[1] = low
    along_x = weights(base_x, frac_x, (size_x, rows))
    along_y = weights(base_y, frac_y, (size_y, rows))
    for x in range(size_x):
        corner[x * size_y : (x + 1) * size_y, :] = along_x[x : x + 1, :] * along_y
    alive = iota((1, rows), 1) < count[0]
    slot = ranks(dest[...], devices)
    where_to = jnp.where(alive, dest[...].astype(jnp.float32) * capacity + slot, -1.0)
    place[...] = jnp.transpose(jnp.broadcast_to(where_to, (8, rows)))
    landing = cell[...].astype(jnp.float32)
    land_xy = jnp.floor((landing + 0.5) * (1.0 / size_z))
    values[...] = jnp.zeros(values.shape, jnp.float32)
    values[2 * nvars : 2 * nvars + 1, :] = land_xy + 1.0
    values[2 * nvars + 1 : 2 * nvars + 2, :] = landing - land_xy * size_z
    for k in range(2):
        copies[k].wait()
        if k == 1:
            small[4].wait()
            even = parity[1] == 0
            for v in range(nvars + 1):
                for x in range(size_x):
                    line = planes.at[1, v] if v < nvars else jac
                    low = line[x * size_y : x * size_y + 1, :]
                    high = line[(x + 1) * size_y - 1 : (x + 1) * size_y, :]
                    y_inner[v, x : x + 1, :] = jnp.where(even, high, low)
                    y_outer[v, x : x + 1, :] = jnp.where(even, low, high)
        for v in range(nvars):
            at = pl.ds((k * nvars + v) * columns, columns)
            high, low = halves(planes[k, v])
            lhs[0, at, :] = high
            lhs[1, at, :] = low
    for n in range(rows // LANES):
        lanes = slice(n * LANES, (n + 1) * LANES)
        for k in range(2):
            at = slice(k * nvars * columns, (k + 1) * nvars * columns)
            part = dot(lhs[0, at, :], spread[0, :, lanes], ((1,), (0,)))
            part = part + dot(lhs[0, at, :], spread[1, :, lanes], ((1,), (0,)))
            part = part + dot(lhs[1, at, :], spread[0, :, lanes], ((1,), (0,)))
            for v in range(nvars):
                picked = part[v * columns : (v + 1) * columns] * corner[:, lanes]
                values[k * nvars + v : k * nvars + v + 1, lanes] = jnp.sum(picked, axis=0, keepdims=True)
    first = values[...]
    high, rest = first.astype(jnp.bfloat16), None
    rest = first - high.astype(jnp.float32)
    middle = rest.astype(jnp.bfloat16)
    last = (rest - middle.astype(jnp.float32)).astype(jnp.bfloat16)
    three = jnp.concatenate([high, middle, last], axis=0)
    column = jnp.broadcast_to(place[:, 0:1], (rows, LANES))
    for n in range(devices * capacity // LANES):
        chosen = (column == (iota((rows, LANES), 1) + n * LANES).astype(jnp.float32)).astype(jnp.float32).astype(jnp.bfloat16)
        moved = dot(three, chosen, ((1,), (0,)))
        moved = moved[0:CHANNELS] + moved[CHANNELS : 2 * CHANNELS] + moved[2 * CHANNELS : 3 * CHANNELS]
        for d in range(LANES // capacity):
            piece = moved[:, d * capacity : (d + 1) * capacity]
            to = n * (LANES // capacity) + d
            out[to] = jnp.concatenate([piece[0:8], piece[8:16]], axis=1)


def mixing_weights(coef, high, low, size):
    nvars, _, size_y, _ = size
    block = nvars * size_y
    width = 3 * block + CHANNELS
    row = iota((size_y, width), 0)
    offset = iota((size_y, width), 1) - row
    lane = iota((size_y, width), 1)

    def at(d, side, a, b):
        return coef[((d * 2 + side) * nvars + a) * nvars + b]

    for a in range(nvars):
        main = jnp.zeros((size_y, width), jnp.float32)
        back = main
        fore = main
        for b in range(nvars):
            first = b * size_y
            same = at(0, 0, a, b) - at(0, 1, a, b) + at(1, 0, a, b) - at(1, 1, a, b) + at(2, 0, a, b) - at(2, 1, a, b)
            main = jnp.where(offset == first, -at(0, 0, a, b), main)
            main = jnp.where(offset == block + first, same, main)
            main = jnp.where((offset == block + first - 1) & (row > 0), -at(1, 0, a, b), main)
            main = jnp.where((offset == block + first + 1) & (row < size_y - 1), at(1, 1, a, b), main)
            main = jnp.where(offset == 2 * block + first, at(0, 1, a, b), main)
            main = jnp.where((lane == 3 * block + b) & (row == 0), -at(1, 0, a, b), main)
            main = jnp.where((lane == 3 * block + nvars + b) & (row == size_y - 1), at(1, 1, a, b), main)
            back = jnp.where(offset == block + first, -at(2, 0, a, b), back)
            fore = jnp.where(offset == block + first, at(2, 1, a, b), fore)
        for k, part in enumerate((main, back, fore)):
            rows = slice(k * block + a * size_y, k * block + (a + 1) * size_y)
            high[rows, :], low[rows, :] = halves(part)


def fill_planes(at_plane, around, planes, sides, size):
    nvars, size_x, size_y, size_z = size
    block = nvars * size_y
    for x in range(size_x + 2):
        for v in range(nvars):
            rows = slice(x * block + v * size_y, x * block + (v + 1) * size_y)
            if 0 < x <= size_x:
                planes[0, rows, :], planes[1, rows, :] = halves(at_plane(v, x - 1))
            elif around is None:
                planes[0, rows, :] = planes[1, rows, :] = jnp.zeros((size_y, size_z), jnp.bfloat16)
            else:
                planes[0, rows, :], planes[1, rows, :] = halves(around[0 if x == 0 else 1][v])
    if around is not None:
        sides[...] = jnp.zeros(sides.shape, jnp.float32)
        for v in range(nvars):
            sides[:, v, :] = around[2][v]
            sides[:, nvars + v, :] = around[3][v]


def flux_at(x, weights, planes, sides, size):
    nvars, _, size_y, size_z = size
    block = nvars * size_y
    if sides is None:
        high = low = jnp.zeros((CHANNELS, size_z), jnp.bfloat16)
    else:
        high, low = halves(sides[x])
    rows = slice(x * block, (x + 3) * block)
    around_high = jnp.concatenate([planes[0, rows, :], high], axis=0)
    around_low = jnp.concatenate([planes[1, rows, :], low], axis=0)
    both = jnp.concatenate([weights[0], weights[1]], axis=0)
    mixed = dot(both, around_high, ((1,), (0,)))
    mixed = mixed[0 : 3 * block] + mixed[3 * block :] + dot(weights[0], around_low, ((1,), (0,)))
    z_at = iota((block, size_z), 1)
    back = jnp.where(z_at == 0, 0.0, pltpu.roll(mixed[block : 2 * block], 1, 1))
    fore = jnp.where(z_at == size_z - 1, 0.0, pltpu.roll(mixed[2 * block :], size_z - 1, 1))
    flux = mixed[0:block] + back + fore
    return [flux[v * size_y : (v + 1) * size_y] for v in range(nvars)]


def sent_out(x, size_x, buffer, out, sems, copies):
    part = size_x // 4
    if (x + 1) % part == 0:
        some = pl.ds(x + 1 - part, part)
        copies.append(pltpu.make_async_copy(buffer.at[:, some], out.at[:, some], sems.at[x // part]))
        copies[-1].start()


def early_kernel(coef, q_now, q_prev, jac, base, weights, planes, buffer, sems, *, size):
    nvars, size_x, _, _ = size
    mixing_weights(coef, weights.at[0], weights.at[1], size)
    fill_planes(lambda v, x: q_now[v, x], None, planes, None, size)
    copies = []
    for x in range(size_x):
        flux = flux_at(x, weights, planes, None, size)
        scale = step_tau * jac[x]
        for v in range(nvars):
            centre = q_now[v, x]
            physical = (q_prev[v, x] - centre) / (2.0 * step_phys)
            buffer[v, x] = centre - scale * (flux[v] + physical)
        sent_out(x, size_x, buffer, base, sems, copies)
    for copy in copies:
        copy.wait()


def mixed_by(coef, direction, side, lines):
    nvars = len(lines)
    out = []
    for a in range(nvars):
        total = None
        for b in range(nvars):
            term = coef[((direction * 2 + side) * nvars + a) * nvars + b] * lines[b]
            total = term if total is None else total + term
        out.append(total)
    return out


def land(rows, hot_xy, hot_z, store, nvars):
    columns = hot_xy.shape[0]
    for first in range(0, nvars, 2):
        some = range(first, min(first + 2, nvars))
        pieces = []
        for c in some:
            for half in halves(rows[c : c + 1, :]):
                pieces.append(hot_xy[...] * half)
        landed = dot(jnp.concatenate(pieces, axis=0), hot_z[...], ((1,), (0,)))
        for c in some:
            at = 2 * (c - first) * columns
            store(c, landed[at : at + columns] + landed[at + columns : at + 2 * columns])


def first_kernel(coef, parity, got, base_in, q_now, jac, line_inner, line_outer, state, hits, x_inner, x_outer, y_inner, y_outer, later, hot_xy, hot_z, rows, grid, base, sem, *, size, devices, capacity):
    nvars, size_x, size_y, size_z = size
    columns = size_x * size_y
    slots = devices * capacity
    fetch = pltpu.make_async_copy(base_in, base, sem)
    fetch.start()
    for d in range(devices):
        piece = got[d]
        lanes = slice(d * capacity, (d + 1) * capacity)
        rows[0:8, lanes] = piece[:, 0:capacity]
        rows[8:16, lanes] = piece[:, capacity : 2 * capacity]
    turned = jnp.transpose(rows[8:16, :])
    land_z = turned[:, 2 * nvars + 1 - 8 : 2 * nvars + 2 - 8]
    hot_z[...] = (iota((slots, size_z), 1).astype(jnp.float32) == land_z).astype(jnp.float32).astype(jnp.bfloat16)
    land_xy = rows[2 * nvars : 2 * nvars + 1, :]
    hot_xy[...] = ((iota((columns, slots), 0) + 1).astype(jnp.float32) == land_xy).astype(jnp.float32).astype(jnp.bfloat16)
    later[...] = rows[nvars : 2 * nvars, :]

    def keep(c, value):
        grid[c] = value

    hits[...] = dot(hot_xy[...], hot_z[...], ((1,), (0,)))
    land(rows, hot_xy, hot_z, keep, nvars)
    even_x, even_y = parity[0] == 0, parity[1] == 0
    y_low = [jnp.where(even_y, line_outer[v], line_inner[v]) for v in range(nvars)]
    y_high = [jnp.where(even_y, line_inner[v], line_outer[v]) for v in range(nvars)]
    from_low, from_high = mixed_by(coef, 1, 0, y_low), mixed_by(coef, 1, 1, y_high)
    row_at = iota((size_y, size_z), 0)
    fetch.wait()
    faces = {}
    for x in range(size_x):
        at = slice(x * size_y, (x + 1) * size_y)
        landed = hits[at, :]
        scale = step_tau * jac[x]
        for v in range(nvars):
            change = penalty * (landed * q_now[v, x] - grid[v, at, :])
            change = change - jnp.where(row_at == 0, from_low[v][x : x + 1], 0.0)
            change = change + jnp.where(row_at == size_y - 1, from_high[v][x : x + 1], 0.0)
            new = base[v, x] - scale * change
            state[v, x] = new
            low, high = new[0:1], new[size_y - 1 : size_y]
            y_inner[v, x : x + 1, :] = jnp.where(even_y, high, low)
            y_outer[v, x : x + 1, :] = jnp.where(even_y, low, high)
            if x in (0, size_x - 1):
                faces[x, v] = new
    ends = [y_low[v] for v in range(nvars)] + [y_high[v] for v in range(nvars)]
    for v in range(nvars):
        for k, pair in enumerate(((faces[0, v], faces[size_x - 1, v]), (q_now[v, 0], q_now[v, size_x - 1]))):
            x_inner[k * nvars + v] = jnp.where(even_x, pair[1], pair[0])
            x_outer[k * nvars + v] = jnp.where(even_x, pair[0], pair[1])
    x_inner[2 * nvars] = jnp.where(even_x, jac[size_x - 1], jac[0])
    x_outer[2 * nvars] = jnp.where(even_x, jac[0], jac[size_x - 1])
    x_inner[2 * nvars + 1] = x_outer[2 * nvars + 1] = jnp.zeros((size_y, size_z), jnp.float32)
    for k, line in enumerate(ends):
        low, high = line[0:1], line[size_x - 1 : size_x]
        x_inner[2 * nvars + 1, k : k + 1, :] = jnp.where(even_x, high, low)
        x_outer[2 * nvars + 1, k : k + 1, :] = jnp.where(even_x, low, high)


def late_kernel(rows, hot_xy, hot_z, target):
    def keep(c, value):
        target[c] = value

    land(rows, hot_xy, hot_z, keep, rows.shape[0])


def second_kernel(coef, parity, state, weights, q_now, q_prev, jac, target, hits, x_inner, x_outer, y_inner, y_outer, line_inner, line_outer, out, planes, sides, edge, buffer, sems, *, size):
    nvars, size_x, size_y, size_z = size
    last = size_x - 1
    even_x, even_y = parity[0] == 0, parity[1] == 0
    x_low = [jnp.where(even_x, x_outer[k], x_inner[k]) for k in range(2 * nvars + 2)]
    x_high = [jnp.where(even_x, x_inner[k], x_outer[k]) for k in range(2 * nvars + 2)]
    own_low = mixed_by(coef, 0, 0, x_low[nvars : 2 * nvars])
    own_high = mixed_by(coef, 0, 1, x_high[nvars : 2 * nvars])
    ring_low = mixed_by(coef, 0, 1, [q_now[v, 0] for v in range(nvars)])
    ring_high = mixed_by(coef, 0, 0, [q_now[v, last] for v in range(nvars)])
    around = [[], [], [], []]
    for v in range(nvars):
        edge[0, v] = state[v, 0] + step_tau * jac[0] * own_low[v]
        edge[1, v] = state[v, last] - step_tau * jac[last] * own_high[v]
        around[0].append(x_low[v] - step_tau * x_low[2 * nvars] * ring_low[v])
        around[1].append(x_high[v] + step_tau * x_high[2 * nvars] * ring_high[v])
    row_at = iota((size_x, size_z), 0)
    for side in range(2):
        pick = (y_outer, y_inner, line_outer, line_inner) if side == 0 else (y_inner, y_outer, line_inner, line_outer)
        scale = step_tau * jnp.where(even_y, pick[2][nvars], pick[3][nvars])
        corner = slice(side * nvars, (side + 1) * nvars)
        low = mixed_by(coef, 0, 0, [x_low[2 * nvars + 1][k : k + 1] for k in range(corner.start, corner.stop)])
        high = mixed_by(coef, 0, 1, [x_high[2 * nvars + 1][k : k + 1] for k in range(corner.start, corner.stop)])
        for v in range(nvars):
            change = jnp.where(row_at == 0, low[v], 0.0) - jnp.where(row_at == last, high[v], 0.0)
            around[2 + side].append(jnp.where(even_y, pick[0][v], pick[1][v]) + scale * change)

    def at_plane(v, x):
        return edge[0, v] if x == 0 else edge[1, v] if x == last else state[v, x]

    fill_planes(at_plane, around, planes, sides, size)
    copies = []
    for x in range(size_x):
        at = slice(x * size_y, (x + 1) * size_y)
        flux = flux_at(x, weights, planes, sides, size)
        landed = hits[at, :]
        scale = step_tau * jac[x]
        for v in range(nvars):
            centre = at_plane(v, x)
            physical = (3.0 * centre - 4.0 * q_now[v, x] + q_prev[v, x]) / (2.0 * step_phys)
            coupling = penalty * (landed * centre - target[v, at, :])
            buffer[v, x] = centre - scale * (flux[v] + physical + coupling)
        sent_out(x, size_x, buffer, out, sems, copies)
    for copy in copies:
        copy.wait()


def swap_pairs(axis, odd):
    count = lax.axis_size(axis)
    pairs = []
    for i in range(odd, count - 1, 2):
        pairs += [(i, i + 1), (i + 1, i)]
    return pairs


def swapped(inner, outer, axis):
    return lax.ppermute(inner, axis, swap_pairs(axis, 0)), lax.ppermute(outer, axis, swap_pairs(axis, 1))


def params(limit):
    return pltpu.CompilerParams(vmem_limit_bytes=limit)


def body(q_now, q_prev, jacobian, flux_split, donor_base, donor_frac, fringe_dest, receptor_cell, fringe_count):
    size = q_now.shape
    nvars, size_x, size_y, size_z = size
    columns = size_x * size_y
    block = nvars * size_y
    devices = lax.axis_size("gx") * lax.axis_size("gy")
    rows = donor_base.shape[0]
    capacity = 2 * rows // devices
    slots = devices * capacity
    f32, bf16 = jnp.float32, jnp.bfloat16
    smem = pl.BlockSpec(memory_space=pltpu.SMEM)
    hbm = pl.BlockSpec(memory_space=pltpu.HBM)
    vmem = pl.BlockSpec(memory_space=pltpu.VMEM)
    flat = (nvars, columns, size_z)
    shape = jax.ShapeDtypeStruct
    weights_shape = (2, 3 * block, 3 * block + CHANNELS)
    planes = pltpu.VMEM((2, (size_x + 2) * block, size_z), bf16)
    sides = pltpu.VMEM((size_x, CHANNELS, size_z), f32)
    face_y = shape((nvars, size_x, size_z), f32)

    line, line_x = shape((nvars + 1, size_x, size_z), f32), shape((2 * nvars + 2, size_y, size_z), f32)
    coef = flux_split.reshape(-1)
    parity = jnp.stack([lax.axis_index("gx") % 2, lax.axis_index("gy") % 2]).astype(jnp.int32)

    def there(x):
        return pltpu.with_memory_space_constraint(x, pltpu.HBM)

    sent, *lines = pl.pallas_call(
        functools.partial(donor_kernel, size=size, devices=devices, capacity=capacity),
        out_shape=[shape((devices, 8, 2 * capacity), f32), line, line],
        in_specs=[smem, smem] + [hbm] * 7,
        out_specs=[vmem] * 3,
        scratch_shapes=[
            pltpu.VMEM((2, nvars, columns, size_z), f32),
            pltpu.VMEM((columns, size_z), f32),
            pltpu.VMEM((2, 2 * nvars * columns, size_z), bf16),
            pltpu.VMEM((2, size_z, rows), bf16),
            pltpu.VMEM((columns, rows), f32),
            pltpu.VMEM((rows, 8), f32),
            pltpu.VMEM((CHANNELS, rows), f32),
            pltpu.VMEM((1, rows), jnp.int32),
            pltpu.VMEM((3, rows), f32),
            pltpu.VMEM((1, rows), jnp.int32),
            pltpu.VMEM((1, rows), jnp.int32),
            pltpu.SemaphoreType.DMA((7,)),
        ],
        compiler_params=params(DONOR_LIMIT),
        name="donor",
    )(
        fringe_count,
        parity,
        there(q_prev.reshape(flat)),
        there(q_now.reshape(flat)),
        there(donor_base.reshape(1, rows)),
        there(donor_frac),
        there(fringe_dest.reshape(1, rows)),
        there(receptor_cell.reshape(1, rows)),
        there(jacobian.reshape(columns, size_z)),
    )
    got = lax.all_to_all(sent, AXES, split_axis=0, concat_axis=0, tiled=True)
    lines = swapped(*lines, "gy")
    base, weights = pl.pallas_call(
        functools.partial(early_kernel, size=size),
        out_shape=[pltpu.HBM(size, f32), shape(weights_shape, bf16)],
        in_specs=[smem] + [vmem] * 3,
        out_specs=[hbm, vmem],
        scratch_shapes=[planes, pltpu.VMEM(size, f32), pltpu.SemaphoreType.DMA((4,))],
        compiler_params=params(20 * MIB),
        name="early",
    )(coef, q_now, q_prev, jacobian)
    state, hits, *faces, later, hot_xy, hot_z = pl.pallas_call(
        functools.partial(first_kernel, size=size, devices=devices, capacity=capacity),
        out_shape=[
            shape(size, f32),
            shape((columns, size_z), f32),
            line_x,
            line_x,
            face_y,
            face_y,
            shape((nvars, slots), f32),
            shape((columns, slots), bf16),
            shape((slots, size_z), bf16),
        ],
        in_specs=[smem, smem, vmem, hbm] + [vmem] * 4,
        out_specs=[vmem] * 9,
        scratch_shapes=[
            pltpu.VMEM((CHANNELS, slots), f32),
            pltpu.VMEM((nvars, columns, size_z), f32),
            pltpu.VMEM(size, f32),
            pltpu.SemaphoreType.DMA,
        ],
        compiler_params=params(20 * MIB),
        name="first",
    )(coef, parity, got, there(base), q_now, jacobian, *lines)
    around = (*swapped(*faces[0:2], "gx"), *swapped(*faces[2:4], "gy"))
    target = pl.pallas_call(
        late_kernel,
        out_shape=shape(flat, f32),
        in_specs=[vmem] * 3,
        out_specs=vmem,
        compiler_params=params(20 * MIB),
        name="late",
    )(later, hot_xy, hot_z)
    return pl.pallas_call(
        functools.partial(second_kernel, size=size),
        out_shape=shape(size, f32),
        in_specs=[smem, smem] + [vmem] * 13,
        out_specs=hbm,
        scratch_shapes=[planes, sides, pltpu.VMEM((2, nvars, size_y, size_z), f32), pltpu.VMEM(size, f32), pltpu.SemaphoreType.DMA((4,))],
        compiler_params=params(20 * MIB),
        name="second",
    )(coef, parity, state, weights, q_now, q_prev, jacobian, target, hits, *around, *lines)


def solution(mesh):
    return jax.shard_map(
        body,
        mesh=mesh,
        in_specs=(
            P(None, "gx", "gy", None),
            P(None, "gx", "gy", None),
            P("gx", "gy", None),
            P(),
            P(("gx", "gy")),
            P(None, ("gx", "gy")),
            P(("gx", "gy"), None),
            P(("gx", "gy")),
            P(("gx", "gy")),
        ),
        out_specs=P(None, "gx", "gy", None),
        check_vma=False,
    )
```

```python
import functools

import jax
import jax.numpy as jnp
from jax import lax
from jax.experimental import pallas as pl
from jax.experimental.pallas import tpu as pltpu
from jax.sharding import PartitionSpec as P


step_tau = 0.2
step_phys = 0.5
penalty = 2.0

AXES = ("gx", "gy")
LANES = 256
CHANNELS = 16
MIB = 1 << 20
DONOR_LIMIT = 44 * MIB


def iota(shape, dim):
    return lax.broadcasted_iota(jnp.int32, shape, dim)


def dot(a, b, dims):
    return lax.dot_general(a, b, (dims, ((), ())), preferred_element_type=jnp.float32)


def halves(x):
    high = x.astype(jnp.bfloat16)
    return high, (x - high.astype(jnp.float32)).astype(jnp.bfloat16)


def ranks(dest, devices):
    rows = dest.shape[1]
    blocks = rows // LANES
    hot = (iota((devices, rows), 0) == dest).astype(jnp.float32)
    stacked = jnp.concatenate([hot[:, b * LANES : (b + 1) * LANES] for b in range(blocks)], axis=0)
    before = (iota((LANES, LANES), 0) < iota((LANES, LANES), 1)).astype(jnp.float32)
    local = dot(stacked.astype(jnp.bfloat16), before.astype(jnp.bfloat16), ((1,), (0,)))
    carried = jnp.zeros((devices, 1), jnp.float32)
    pieces = []
    for b in range(blocks):
        part = local[b * devices : (b + 1) * devices]
        own = hot[:, b * LANES : (b + 1) * LANES]
        pieces.append(jnp.sum((part + carried) * own, axis=0, keepdims=True))
        carried = carried + jnp.sum(own, axis=1, keepdims=True)
    return jnp.concatenate(pieces, axis=1)


def donor_kernel(count, q_prev, q_now, base_in, frac_in, dest_in, cell_in, jac_in, out, y_inner, y_outer, planes, jac, lhs, spread, corner, place, values, base, frac, dest, cell, sems, *, size, devices, capacity):
    nvars, size_x, size_y, size_z = size
    columns = size_x * size_y
    rows = base.shape[1]
    small = [pltpu.make_async_copy(a, b, sems.at[2 + k]) for k, (a, b) in enumerate(((base_in, base), (frac_in, frac), (dest_in, dest), (cell_in, cell), (jac_in, jac)))]
    copies = [pltpu.make_async_copy(ref, planes.at[k], sems.at[k]) for k, ref in enumerate((q_prev, q_now))]
    for copy in small + copies:
        copy.start()
    for copy in small[0:4]:
        copy.wait()
    start = base[...].astype(jnp.float32)
    in_y = jnp.floor((start + 0.5) * (1.0 / (size_z - 1)))
    base_z = start - in_y * (size_z - 1)
    base_x = jnp.floor((in_y + 0.5) * (1.0 / (size_y - 1)))
    base_y = in_y - base_x * (size_y - 1)
    frac_x, frac_y, frac_z = frac[0:1, :], frac[1:2, :], frac[2:3, :]

    def weights(first, part, shape):
        at = iota(shape, 0).astype(jnp.float32) - first
        return jnp.where(at == 0.0, 1.0 - part, jnp.where(at == 1.0, part, 0.0))

    along_z = weights(base_z, frac_z, (size_z, rows))
    high, low = halves(along_z)
    spread[0] = high
    spread[1] = low
    along_x = weights(base_x, frac_x, (size_x, rows))
    along_y = weights(base_y, frac_y, (size_y, rows))
    for x in range(size_x):
        corner[x * size_y : (x + 1) * size_y, :] = along_x[x : x + 1, :] * along_y
    alive = iota((1, rows), 1) < count[0]
    slot = ranks(dest[...], devices)
    where_to = jnp.where(alive, dest[...].astype(jnp.float32) * capacity + slot, -1.0)
    place[...] = jnp.transpose(jnp.broadcast_to(where_to, (8, rows)))
    landing = cell[...].astype(jnp.float32)
    land_xy = jnp.floor((landing + 0.5) * (1.0 / size_z))
    values[...] = jnp.zeros(values.shape, jnp.float32)
    values[2 * nvars : 2 * nvars + 1, :] = land_xy + 1.0
    values[2 * nvars + 1 : 2 * nvars + 2, :] = landing - land_xy * size_z
    for k in range(2):
        copies[k].wait()
        if k == 1:
            small[4].wait()
            even = lax.axis_index("gy") % 2 == 0
            for v in range(nvars + 1):
                for x in range(size_x):
                    line = planes.at[1, v] if v < nvars else jac
                    low = line[x * size_y : x * size_y + 1, :]
                    high = line[(x + 1) * size_y - 1 : (x + 1) * size_y, :]
                    y_inner[v, x : x + 1, :] = jnp.where(even, high, low)
                    y_outer[v, x : x + 1, :] = jnp.where(even, low, high)
        for v in range(nvars):
            at = pl.ds((k * nvars + v) * columns, columns)
            high, low = halves(planes[k, v])
            lhs[0, at, :] = high
            lhs[1, at, :] = low
    for n in range(rows // LANES):
        lanes = slice(n * LANES, (n + 1) * LANES)
        for k in range(2):
            at = slice(k * nvars * columns, (k + 1) * nvars * columns)
            part = dot(lhs[0, at, :], spread[0, :, lanes], ((1,), (0,)))
            part = part + dot(lhs[0, at, :], spread[1, :, lanes], ((1,), (0,)))
            part = part + dot(lhs[1, at, :], spread[0, :, lanes], ((1,), (0,)))
            for v in range(nvars):
                picked = part[v * columns : (v + 1) * columns] * corner[:, lanes]
                values[k * nvars + v : k * nvars + v + 1, lanes] = jnp.sum(picked, axis=0, keepdims=True)
    first = values[...]
    high, rest = first.astype(jnp.bfloat16), None
    rest = first - high.astype(jnp.float32)
    middle = rest.astype(jnp.bfloat16)
    last = (rest - middle.astype(jnp.float32)).astype(jnp.bfloat16)
    three = jnp.concatenate([high, middle, last], axis=0)
    column = jnp.broadcast_to(place[:, 0:1], (rows, LANES))
    for n in range(devices * capacity // LANES):
        chosen = (column == (iota((rows, LANES), 1) + n * LANES).astype(jnp.float32)).astype(jnp.float32).astype(jnp.bfloat16)
        moved = dot(three, chosen, ((1,), (0,)))
        moved = moved[0:CHANNELS] + moved[CHANNELS : 2 * CHANNELS] + moved[2 * CHANNELS : 3 * CHANNELS]
        for d in range(LANES // capacity):
            piece = moved[:, d * capacity : (d + 1) * capacity]
            to = n * (LANES // capacity) + d
            out[to] = jnp.concatenate([piece[0:8], piece[8:16]], axis=1)


def mixing_weights(coef, high, low, size):
    nvars, _, size_y, _ = size
    block = nvars * size_y
    width = 3 * block + CHANNELS
    row = iota((size_y, width), 0)
    offset = iota((size_y, width), 1) - row
    lane = iota((size_y, width), 1)

    def at(d, side, a, b):
        return coef[((d * 2 + side) * nvars + a) * nvars + b]

    for a in range(nvars):
        main = jnp.zeros((size_y, width), jnp.float32)
        back = main
        fore = main
        for b in range(nvars):
            first = b * size_y
            same = at(0, 0, a, b) - at(0, 1, a, b) + at(1, 0, a, b) - at(1, 1, a, b) + at(2, 0, a, b) - at(2, 1, a, b)
            main = jnp.where(offset == first, -at(0, 0, a, b), main)
            main = jnp.where(offset == block + first, same, main)
            main = jnp.where((offset == block + first - 1) & (row > 0), -at(1, 0, a, b), main)
            main = jnp.where((offset == block + first + 1) & (row < size_y - 1), at(1, 1, a, b), main)
            main = jnp.where(offset == 2 * block + first, at(0, 1, a, b), main)
            main = jnp.where((lane == 3 * block + b) & (row == 0), -at(1, 0, a, b), main)
            main = jnp.where((lane == 3 * block + nvars + b) & (row == size_y - 1), at(1, 1, a, b), main)
            back = jnp.where(offset == block + first, -at(2, 0, a, b), back)
            fore = jnp.where(offset == block + first, at(2, 1, a, b), fore)
        for k, part in enumerate((main, back, fore)):
            rows = slice(k * block + a * size_y, k * block + (a + 1) * size_y)
            high[rows, :], low[rows, :] = halves(part)


def fill_planes(at_plane, around, planes, sides, size):
    nvars, size_x, size_y, size_z = size
    block = nvars * size_y
    for x in range(size_x + 2):
        for v in range(nvars):
            rows = slice(x * block + v * size_y, x * block + (v + 1) * size_y)
            if 0 < x <= size_x:
                planes[0, rows, :], planes[1, rows, :] = halves(at_plane(v, x - 1))
            elif around is None:
                planes[0, rows, :] = planes[1, rows, :] = jnp.zeros((size_y, size_z), jnp.bfloat16)
            else:
                planes[0, rows, :], planes[1, rows, :] = halves(around[0 if x == 0 else 1][v])
    if around is not None:
        sides[...] = jnp.zeros(sides.shape, jnp.float32)
        for v in range(nvars):
            sides[:, v, :] = around[2][v]
            sides[:, nvars + v, :] = around[3][v]


def flux_at(x, weights, planes, sides, size):
    nvars, _, size_y, size_z = size
    block = nvars * size_y
    if sides is None:
        high = low = jnp.zeros((CHANNELS, size_z), jnp.bfloat16)
    else:
        high, low = halves(sides[x])
    rows = slice(x * block, (x + 3) * block)
    around_high = jnp.concatenate([planes[0, rows, :], high], axis=0)
    around_low = jnp.concatenate([planes[1, rows, :], low], axis=0)
    both = jnp.concatenate([weights[0], weights[1]], axis=0)
    mixed = dot(both, around_high, ((1,), (0,)))
    mixed = mixed[0 : 3 * block] + mixed[3 * block :] + dot(weights[0], around_low, ((1,), (0,)))
    z_at = iota((block, size_z), 1)
    back = jnp.where(z_at == 0, 0.0, pltpu.roll(mixed[block : 2 * block], 1, 1))
    fore = jnp.where(z_at == size_z - 1, 0.0, pltpu.roll(mixed[2 * block :], size_z - 1, 1))
    flux = mixed[0:block] + back + fore
    return [flux[v * size_y : (v + 1) * size_y] for v in range(nvars)]


def sent_out(x, size_x, buffer, out, sems, copies):
    part = size_x // 4
    if (x + 1) % part == 0:
        some = pl.ds(x + 1 - part, part)
        copies.append(pltpu.make_async_copy(buffer.at[:, some], out.at[:, some], sems.at[x // part]))
        copies[-1].start()


def early_kernel(coef_in, q_now, q_prev, jac, base, weights, table, planes, coef, buffer, sems, *, size):
    nvars, size_x, _, size_z = size
    fetch = pltpu.make_async_copy(coef_in, coef, sems.at[4])
    fetch.start()
    fill_planes(lambda v, x: q_now[v, x], None, planes, None, size)
    fetch.wait()
    for k in range(table.shape[0]):
        table[k : k + 1, :] = jnp.full((1, size_z), coef[k], jnp.float32)
    mixing_weights(coef, weights.at[0], weights.at[1], size)
    copies = []
    for x in range(size_x):
        flux = flux_at(x, weights, planes, None, size)
        scale = step_tau * jac[x]
        for v in range(nvars):
            centre = q_now[v, x]
            physical = (q_prev[v, x] - centre) / (2.0 * step_phys)
            buffer[v, x] = centre - scale * (flux[v] + physical)
        sent_out(x, size_x, buffer, base, sems, copies)
    for copy in copies:
        copy.wait()


def mixed_by(table, direction, side, lines):
    nvars = len(lines)
    out = []
    for a in range(nvars):
        total = None
        for b in range(nvars):
            k = ((direction * 2 + side) * nvars + a) * nvars + b
            term = table[k : k + 1, :] * lines[b]
            total = term if total is None else total + term
        out.append(total)
    return out


def land(rows, hot_xy, hot_z, store, nvars):
    columns = hot_xy.shape[0]
    for first in range(0, nvars, 2):
        some = range(first, min(first + 2, nvars))
        pieces = []
        for c in some:
            for half in halves(rows[c : c + 1, :]):
                pieces.append(hot_xy[...] * half)
        landed = dot(jnp.concatenate(pieces, axis=0), hot_z[...], ((1,), (0,)))
        for c in some:
            at = 2 * (c - first) * columns
            store(c, landed[at : at + columns] + landed[at + columns : at + 2 * columns])


def first_kernel(table, got, base_in, q_now, jac, line_inner, line_outer, state, hits, x_inner, x_outer, y_inner, y_outer, later, hot_xy, hot_z, rows, grid, base, sems, *, size, devices, capacity):
    nvars, size_x, size_y, size_z = size
    columns = size_x * size_y
    slots = devices * capacity
    part = size_x // 4
    fetches = []
    for k in range(4):
        some = pl.ds(k * part, part)
        fetches.append(pltpu.make_async_copy(base_in.at[:, some], base.at[:, some], sems.at[k]))
        fetches[-1].start()
    for d in range(devices):
        piece = got[d]
        lanes = slice(d * capacity, (d + 1) * capacity)
        rows[0:8, lanes] = piece[:, 0:capacity]
        rows[8:16, lanes] = piece[:, capacity : 2 * capacity]
    turned = jnp.transpose(rows[8:16, :])
    land_z = turned[:, 2 * nvars + 1 - 8 : 2 * nvars + 2 - 8]
    hot_z[...] = (iota((slots, size_z), 1).astype(jnp.float32) == land_z).astype(jnp.float32).astype(jnp.bfloat16)
    land_xy = rows[2 * nvars : 2 * nvars + 1, :]
    hot_xy[...] = ((iota((columns, slots), 0) + 1).astype(jnp.float32) == land_xy).astype(jnp.float32).astype(jnp.bfloat16)
    later[...] = rows[nvars : 2 * nvars, :]

    def keep(c, value):
        grid[c] = value

    hits[...] = dot(hot_xy[...], hot_z[...], ((1,), (0,)))
    land(rows, hot_xy, hot_z, keep, nvars)
    even_x, even_y = lax.axis_index("gx") % 2 == 0, lax.axis_index("gy") % 2 == 0
    y_low = [jnp.where(even_y, line_outer[v], line_inner[v]) for v in range(nvars)]
    y_high = [jnp.where(even_y, line_inner[v], line_outer[v]) for v in range(nvars)]
    from_low, from_high = mixed_by(table, 1, 0, y_low), mixed_by(table, 1, 1, y_high)
    row_at = iota((size_y, size_z), 0)
    faces = {}
    for fetch in fetches:
        fetch.wait()
    for x in range(size_x):
        at = slice(x * size_y, (x + 1) * size_y)
        landed = hits[at, :]
        scale = step_tau * jac[x]
        for v in range(nvars):
            change = penalty * (landed * q_now[v, x] - grid[v, at, :])
            change = change - jnp.where(row_at == 0, from_low[v][x : x + 1], 0.0)
            change = change + jnp.where(row_at == size_y - 1, from_high[v][x : x + 1], 0.0)
            new = base[v, x] - scale * change
            state[v, x] = new
            low, high = new[0:1], new[size_y - 1 : size_y]
            y_inner[v, x : x + 1, :] = jnp.where(even_y, high, low)
            y_outer[v, x : x + 1, :] = jnp.where(even_y, low, high)
            if x in (0, size_x - 1):
                faces[x, v] = new
    ends = [y_low[v] for v in range(nvars)] + [y_high[v] for v in range(nvars)]
    for v in range(nvars):
        for k, pair in enumerate(((faces[0, v], faces[size_x - 1, v]), (q_now[v, 0], q_now[v, size_x - 1]))):
            x_inner[k * nvars + v] = jnp.where(even_x, pair[1], pair[0])
            x_outer[k * nvars + v] = jnp.where(even_x, pair[0], pair[1])
    x_inner[2 * nvars] = jnp.where(even_x, jac[size_x - 1], jac[0])
    x_outer[2 * nvars] = jnp.where(even_x, jac[0], jac[size_x - 1])
    x_inner[2 * nvars + 1] = x_outer[2 * nvars + 1] = jnp.zeros((size_y, size_z), jnp.float32)
    for k, line in enumerate(ends):
        low, high = line[0:1], line[size_x - 1 : size_x]
        x_inner[2 * nvars + 1, k : k + 1, :] = jnp.where(even_x, high, low)
        x_outer[2 * nvars + 1, k : k + 1, :] = jnp.where(even_x, low, high)


def late_kernel(rows, hot_xy, hot_z, target):
    def keep(c, value):
        target[c] = value

    land(rows, hot_xy, hot_z, keep, rows.shape[0])


def second_kernel(table, state, weights, q_now, q_prev, jac, target, hits, x_inner, x_outer, y_inner, y_outer, line_inner, line_outer, out, planes, sides, edge, buffer, sems, *, size):
    nvars, size_x, size_y, size_z = size
    last = size_x - 1
    even_x, even_y = lax.axis_index("gx") % 2 == 0, lax.axis_index("gy") % 2 == 0
    x_low = [jnp.where(even_x, x_outer[k], x_inner[k]) for k in range(2 * nvars + 2)]
    x_high = [jnp.where(even_x, x_inner[k], x_outer[k]) for k in range(2 * nvars + 2)]
    own_low = mixed_by(table, 0, 0, x_low[nvars : 2 * nvars])
    own_high = mixed_by(table, 0, 1, x_high[nvars : 2 * nvars])
    ring_low = mixed_by(table, 0, 1, [q_now[v, 0] for v in range(nvars)])
    ring_high = mixed_by(table, 0, 0, [q_now[v, last] for v in range(nvars)])
    around = [[], [], [], []]
    for v in range(nvars):
        edge[0, v] = state[v, 0] + step_tau * jac[0] * own_low[v]
        edge[1, v] = state[v, last] - step_tau * jac[last] * own_high[v]
        around[0].append(x_low[v] - step_tau * x_low[2 * nvars] * ring_low[v])
        around[1].append(x_high[v] + step_tau * x_high[2 * nvars] * ring_high[v])
    row_at = iota((size_x, size_z), 0)
    for side in range(2):
        pick = (y_outer, y_inner, line_outer, line_inner) if side == 0 else (y_inner, y_outer, line_inner, line_outer)
        scale = step_tau * jnp.where(even_y, pick[2][nvars], pick[3][nvars])
        corner = slice(side * nvars, (side + 1) * nvars)
        low = mixed_by(table, 0, 0, [x_low[2 * nvars + 1][k : k + 1] for k in range(corner.start, corner.stop)])
        high = mixed_by(table, 0, 1, [x_high[2 * nvars + 1][k : k + 1] for k in range(corner.start, corner.stop)])
        for v in range(nvars):
            change = jnp.where(row_at == 0, low[v], 0.0) - jnp.where(row_at == last, high[v], 0.0)
            around[2 + side].append(jnp.where(even_y, pick[0][v], pick[1][v]) + scale * change)

    def at_plane(v, x):
        return edge[0, v] if x == 0 else edge[1, v] if x == last else state[v, x]

    fill_planes(at_plane, around, planes, sides, size)
    copies = []
    for x in range(size_x):
        at = slice(x * size_y, (x + 1) * size_y)
        flux = flux_at(x, weights, planes, sides, size)
        landed = hits[at, :]
        scale = step_tau * jac[x]
        for v in range(nvars):
            centre = at_plane(v, x)
            physical = (3.0 * centre - 4.0 * q_now[v, x] + q_prev[v, x]) / (2.0 * step_phys)
            coupling = penalty * (landed * centre - target[v, at, :])
            buffer[v, x] = centre - scale * (flux[v] + physical + coupling)
        sent_out(x, size_x, buffer, out, sems, copies)
    for copy in copies:
        copy.wait()


def swap_pairs(axis, odd):
    count = lax.axis_size(axis)
    pairs = []
    for i in range(odd, count - 1, 2):
        pairs += [(i, i + 1), (i + 1, i)]
    return pairs


def swapped(inner, outer, axis):
    return lax.ppermute(inner, axis, swap_pairs(axis, 0)), lax.ppermute(outer, axis, swap_pairs(axis, 1))


def params(limit):
    return pltpu.CompilerParams(vmem_limit_bytes=limit)


def body(q_now, q_prev, jacobian, flux_split, donor_base, donor_frac, fringe_dest, receptor_cell, fringe_count):
    size = q_now.shape
    nvars, size_x, size_y, size_z = size
    columns = size_x * size_y
    block = nvars * size_y
    devices = lax.axis_size("gx") * lax.axis_size("gy")
    rows = donor_base.shape[0]
    capacity = 2 * rows // devices
    slots = devices * capacity
    f32, bf16 = jnp.float32, jnp.bfloat16
    hbm = pl.BlockSpec(memory_space=pltpu.HBM)
    vmem = pl.BlockSpec(memory_space=pltpu.VMEM)
    flat = (nvars, columns, size_z)
    shape = jax.ShapeDtypeStruct
    weights_shape = (2, 3 * block, 3 * block + CHANNELS)
    planes = pltpu.VMEM((2, (size_x + 2) * block, size_z), bf16)
    sides = pltpu.VMEM((size_x, CHANNELS, size_z), f32)
    face_y = shape((nvars, size_x, size_z), f32)

    line, line_x = pltpu.VMEM((nvars + 1, size_x, size_z), f32), shape((2 * nvars + 2, size_y, size_z), f32)
    coef = flux_split.reshape(-1)

    def there(x):
        return pltpu.with_memory_space_constraint(x, pltpu.HBM)

    sent, *lines = pl.pallas_call(
        functools.partial(donor_kernel, size=size, devices=devices, capacity=capacity),
        out_shape=[pltpu.VMEM((devices, 8, 2 * capacity), f32), line, line],
        in_specs=[pl.BlockSpec(memory_space=pltpu.SMEM)] + [hbm] * 7,
        out_specs=[vmem] * 3,
        scratch_shapes=[
            pltpu.VMEM((2, nvars, columns, size_z), f32),
            pltpu.VMEM((columns, size_z), f32),
            pltpu.VMEM((2, 2 * nvars * columns, size_z), bf16),
            pltpu.VMEM((2, size_z, rows), bf16),
            pltpu.VMEM((columns, rows), f32),
            pltpu.VMEM((rows, 8), f32),
            pltpu.VMEM((CHANNELS, rows), f32),
            pltpu.VMEM((1, rows), jnp.int32),
            pltpu.VMEM((3, rows), f32),
            pltpu.VMEM((1, rows), jnp.int32),
            pltpu.VMEM((1, rows), jnp.int32),
            pltpu.SemaphoreType.DMA((7,)),
        ],
        compiler_params=params(DONOR_LIMIT),
        name="donor",
    )(
        fringe_count,
        there(q_prev.reshape(flat)),
        there(q_now.reshape(flat)),
        there(donor_base.reshape(1, rows)),
        there(donor_frac),
        there(fringe_dest.reshape(1, rows)),
        there(receptor_cell.reshape(1, rows)),
        there(jacobian.reshape(columns, size_z)),
    )
    got = lax.all_to_all(sent, AXES, split_axis=0, concat_axis=0, tiled=True)
    lines = swapped(*lines, "gy")
    base, weights, table = pl.pallas_call(
        functools.partial(early_kernel, size=size),
        out_shape=[pltpu.HBM(size, f32), shape(weights_shape, bf16), shape((4 * nvars * nvars, size_z), f32)],
        in_specs=[hbm] + [vmem] * 3,
        out_specs=[hbm, vmem, vmem],
        scratch_shapes=[planes, pltpu.SMEM((6 * nvars * nvars,), f32), pltpu.VMEM(size, f32), pltpu.SemaphoreType.DMA((5,))],
        compiler_params=params(20 * MIB),
        name="early",
    )(there(coef), q_now, q_prev, jacobian)
    state, hits, *faces, later, hot_xy, hot_z = pl.pallas_call(
        functools.partial(first_kernel, size=size, devices=devices, capacity=capacity),
        out_shape=[
            shape(size, f32),
            shape((columns, size_z), f32),
            line_x,
            line_x,
            face_y,
            face_y,
            shape((nvars, slots), f32),
            shape((columns, slots), bf16),
            shape((slots, size_z), bf16),
        ],
        in_specs=[vmem, vmem, hbm] + [vmem] * 4,
        out_specs=[vmem] * 9,
        scratch_shapes=[
            pltpu.VMEM((CHANNELS, slots), f32),
            pltpu.VMEM((nvars, columns, size_z), f32),
            pltpu.VMEM(size, f32),
            pltpu.SemaphoreType.DMA((4,)),
        ],
        compiler_params=params(20 * MIB),
        name="first",
    )(table, got, there(base), q_now, jacobian, *lines)
    around = (*swapped(*faces[0:2], "gx"), *swapped(*faces[2:4], "gy"))
    target = pl.pallas_call(
        late_kernel,
        out_shape=shape(flat, f32),
        in_specs=[vmem] * 3,
        out_specs=vmem,
        compiler_params=params(20 * MIB),
        name="late",
    )(later, hot_xy, hot_z)
    return pl.pallas_call(
        functools.partial(second_kernel, size=size),
        out_shape=shape(size, f32),
        in_specs=[vmem] * 14,
        out_specs=hbm,
        scratch_shapes=[planes, sides, pltpu.VMEM((2, nvars, size_y, size_z), f32), pltpu.VMEM(size, f32), pltpu.SemaphoreType.DMA((4,))],
        compiler_params=params(20 * MIB),
        name="second",
    )(table, state, weights, q_now, q_prev, jacobian, target, hits, *around, *lines)


def solution(mesh):
    return jax.shard_map(
        body,
        mesh=mesh,
        in_specs=(
            P(None, "gx", "gy", None),
            P(None, "gx", "gy", None),
            P("gx", "gy", None),
            P(),
            P(("gx", "gy")),
            P(None, ("gx", "gy")),
            P(("gx", "gy"), None),
            P(("gx", "gy")),
            P(("gx", "gy")),
        ),
        out_specs=P(None, "gx", "gy", None),
        check_vma=False,
    )
```

```python
import functools

import jax
import jax.numpy as jnp
from jax import lax
from jax.experimental import pallas as pl
from jax.experimental.pallas import tpu as pltpu
from jax.sharding import PartitionSpec as P


step_tau = 0.2
step_phys = 0.5
penalty = 2.0

AXES = ("gx", "gy")
LANES = 256
CHANNELS = 16
MIB = 1 << 20
DONOR_LIMIT = 44 * MIB


def iota(shape, dim):
    return lax.broadcasted_iota(jnp.int32, shape, dim)


def dot(a, b, dims):
    return lax.dot_general(a, b, (dims, ((), ())), preferred_element_type=jnp.float32)


def halves(x):
    high = x.astype(jnp.bfloat16)
    return high, (x - high.astype(jnp.float32)).astype(jnp.bfloat16)


def ranks(dest, devices):
    rows = dest.shape[1]
    blocks = rows // LANES
    hot = (iota((devices, rows), 0) == dest).astype(jnp.float32)
    stacked = jnp.concatenate([hot[:, b * LANES : (b + 1) * LANES] for b in range(blocks)], axis=0)
    before = (iota((LANES, LANES), 0) < iota((LANES, LANES), 1)).astype(jnp.float32)
    local = dot(stacked.astype(jnp.bfloat16), before.astype(jnp.bfloat16), ((1,), (0,)))
    carried = jnp.zeros((devices, 1), jnp.float32)
    pieces = []
    for b in range(blocks):
        part = local[b * devices : (b + 1) * devices]
        own = hot[:, b * LANES : (b + 1) * LANES]
        pieces.append(jnp.sum((part + carried) * own, axis=0, keepdims=True))
        carried = carried + jnp.sum(own, axis=1, keepdims=True)
    return jnp.concatenate(pieces, axis=1)


def donor_kernel(count, q_prev, q_now, base_in, frac_in, dest_in, cell_in, jac_in, out, y_inner, y_outer, planes, jac, lhs, spread, corner, place, values, base, frac, dest, cell, sems, *, size, devices, capacity):
    nvars, size_x, size_y, size_z = size
    columns = size_x * size_y
    rows = base.shape[1]
    small = [pltpu.make_async_copy(a, b, sems.at[k]) for k, (a, b) in enumerate(((base_in, base), (frac_in, frac), (dest_in, dest), (cell_in, cell), (jac_in, jac)))]
    copies = [pltpu.make_async_copy(ref.at[v], planes.at[k, v], sems.at[5 + k * nvars + v]) for k, ref in enumerate((q_prev, q_now)) for v in range(nvars)]
    for copy in small + copies:
        copy.start()
    for copy in small[0:4]:
        copy.wait()
    start = base[...].astype(jnp.float32)
    in_y = jnp.floor((start + 0.5) * (1.0 / (size_z - 1)))
    base_z = start - in_y * (size_z - 1)
    base_x = jnp.floor((in_y + 0.5) * (1.0 / (size_y - 1)))
    base_y = in_y - base_x * (size_y - 1)
    frac_x, frac_y, frac_z = frac[0:1, :], frac[1:2, :], frac[2:3, :]

    def weights(first, part, shape):
        at = iota(shape, 0).astype(jnp.float32) - first
        return jnp.where(at == 0.0, 1.0 - part, jnp.where(at == 1.0, part, 0.0))

    along_z = weights(base_z, frac_z, (size_z, rows))
    high, low = halves(along_z)
    spread[0] = high
    spread[1] = low
    along_x = weights(base_x, frac_x, (size_x, rows))
    along_y = weights(base_y, frac_y, (size_y, rows))
    for x in range(size_x):
        corner[x * size_y : (x + 1) * size_y, :] = along_x[x : x + 1, :] * along_y
    alive = iota((1, rows), 1) < count[0]
    slot = ranks(dest[...], devices)
    where_to = jnp.where(alive, dest[...].astype(jnp.float32) * capacity + slot, -1.0)
    place[...] = jnp.transpose(jnp.broadcast_to(where_to, (8, rows)))
    landing = cell[...].astype(jnp.float32)
    land_xy = jnp.floor((landing + 0.5) * (1.0 / size_z))
    values[...] = jnp.zeros(values.shape, jnp.float32)
    values[2 * nvars : 2 * nvars + 1, :] = land_xy + 1.0
    values[2 * nvars + 1 : 2 * nvars + 2, :] = landing - land_xy * size_z
    for k in range(2):
        if k == 1:
            for v in range(nvars):
                copies[nvars + v].wait()
            small[4].wait()
            even = lax.axis_index("gy") % 2 == 0
            for v in range(nvars + 1):
                for x in range(size_x):
                    line = planes.at[1, v] if v < nvars else jac
                    low = line[x * size_y : x * size_y + 1, :]
                    high = line[(x + 1) * size_y - 1 : (x + 1) * size_y, :]
                    y_inner[v, x : x + 1, :] = jnp.where(even, high, low)
                    y_outer[v, x : x + 1, :] = jnp.where(even, low, high)
        for v in range(nvars):
            if k == 0:
                copies[v].wait()
            at = pl.ds((k * nvars + v) * columns, columns)
            high, low = halves(planes[k, v])
            lhs[0, at, :] = high
            lhs[1, at, :] = low
    for n in range(rows // LANES):
        lanes = slice(n * LANES, (n + 1) * LANES)
        for k in range(2):
            at = slice(k * nvars * columns, (k + 1) * nvars * columns)
            part = dot(lhs[0, at, :], spread[0, :, lanes], ((1,), (0,)))
            part = part + dot(lhs[0, at, :], spread[1, :, lanes], ((1,), (0,)))
            part = part + dot(lhs[1, at, :], spread[0, :, lanes], ((1,), (0,)))
            for v in range(nvars):
                picked = part[v * columns : (v + 1) * columns] * corner[:, lanes]
                values[k * nvars + v : k * nvars + v + 1, lanes] = jnp.sum(picked, axis=0, keepdims=True)
    first = values[...]
    high, rest = first.astype(jnp.bfloat16), None
    rest = first - high.astype(jnp.float32)
    middle = rest.astype(jnp.bfloat16)
    last = (rest - middle.astype(jnp.float32)).astype(jnp.bfloat16)
    three = jnp.concatenate([high, middle, last], axis=0)
    column = jnp.broadcast_to(place[:, 0:1], (rows, LANES))
    for n in range(devices * capacity // LANES):
        chosen = (column == (iota((rows, LANES), 1) + n * LANES).astype(jnp.float32)).astype(jnp.float32).astype(jnp.bfloat16)
        moved = dot(three, chosen, ((1,), (0,)))
        moved = moved[0:CHANNELS] + moved[CHANNELS : 2 * CHANNELS] + moved[2 * CHANNELS : 3 * CHANNELS]
        for d in range(LANES // capacity):
            piece = moved[:, d * capacity : (d + 1) * capacity]
            to = n * (LANES // capacity) + d
            out[to] = jnp.concatenate([piece[0:8], piece[8:16]], axis=1)


def mixing_weights(coef, high, low, size):
    nvars, _, size_y, _ = size
    block = nvars * size_y
    width = 3 * block + CHANNELS
    row = iota((size_y, width), 0)
    offset = iota((size_y, width), 1) - row
    lane = iota((size_y, width), 1)

    def at(d, side, a, b):
        return coef[((d * 2 + side) * nvars + a) * nvars + b]

    for a in range(nvars):
        main = jnp.zeros((size_y, width), jnp.float32)
        back = main
        fore = main
        for b in range(nvars):
            first = b * size_y
            same = at(0, 0, a, b) - at(0, 1, a, b) + at(1, 0, a, b) - at(1, 1, a, b) + at(2, 0, a, b) - at(2, 1, a, b)
            main = jnp.where(offset == first, -at(0, 0, a, b), main)
            main = jnp.where(offset == block + first, same, main)
            main = jnp.where((offset == block + first - 1) & (row > 0), -at(1, 0, a, b), main)
            main = jnp.where((offset == block + first + 1) & (row < size_y - 1), at(1, 1, a, b), main)
            main = jnp.where(offset == 2 * block + first, at(0, 1, a, b), main)
            main = jnp.where((lane == 3 * block + b) & (row == 0), -at(1, 0, a, b), main)
            main = jnp.where((lane == 3 * block + nvars + b) & (row == size_y - 1), at(1, 1, a, b), main)
            back = jnp.where(offset == block + first, -at(2, 0, a, b), back)
            fore = jnp.where(offset == block + first, at(2, 1, a, b), fore)
        for k, part in enumerate((main, back, fore)):
            rows = slice(k * block + a * size_y, k * block + (a + 1) * size_y)
            high[rows, :], low[rows, :] = halves(part)


def fill_planes(at_plane, around, planes, sides, size):
    nvars, size_x, size_y, size_z = size
    block = nvars * size_y
    for x in range(size_x + 2):
        for v in range(nvars):
            rows = slice(x * block + v * size_y, x * block + (v + 1) * size_y)
            if 0 < x <= size_x:
                planes[0, rows, :], planes[1, rows, :] = halves(at_plane(v, x - 1))
            elif around is None:
                planes[0, rows, :] = planes[1, rows, :] = jnp.zeros((size_y, size_z), jnp.bfloat16)
            else:
                planes[0, rows, :], planes[1, rows, :] = halves(around[0 if x == 0 else 1][v])
    if around is not None:
        sides[...] = jnp.zeros(sides.shape, jnp.float32)
        for v in range(nvars):
            sides[:, v, :] = around[2][v]
            sides[:, nvars + v, :] = around[3][v]


def flux_at(x, weights, planes, sides, size):
    nvars, _, size_y, size_z = size
    block = nvars * size_y
    if sides is None:
        high = low = jnp.zeros((CHANNELS, size_z), jnp.bfloat16)
    else:
        high, low = halves(sides[x])
    rows = slice(x * block, (x + 3) * block)
    around_high = jnp.concatenate([planes[0, rows, :], high], axis=0)
    around_low = jnp.concatenate([planes[1, rows, :], low], axis=0)
    both = jnp.concatenate([weights[0], weights[1]], axis=0)
    mixed = dot(both, around_high, ((1,), (0,)))
    mixed = mixed[0 : 3 * block] + mixed[3 * block :] + dot(weights[0], around_low, ((1,), (0,)))
    z_at = iota((block, size_z), 1)
    back = jnp.where(z_at == 0, 0.0, pltpu.roll(mixed[block : 2 * block], 1, 1))
    fore = jnp.where(z_at == size_z - 1, 0.0, pltpu.roll(mixed[2 * block :], size_z - 1, 1))
    flux = mixed[0:block] + back + fore
    return [flux[v * size_y : (v + 1) * size_y] for v in range(nvars)]


def sent_out(x, size_x, buffer, out, sems, copies):
    part = size_x // 4
    if (x + 1) % part == 0:
        some = pl.ds(x + 1 - part, part)
        copies.append(pltpu.make_async_copy(buffer.at[:, some], out.at[:, some], sems.at[x // part]))
        copies[-1].start()


def early_kernel(coef_in, q_now, q_prev, jac, base, weights_out, table, planes, coef, buffer, weights, sems, *, size):
    nvars, size_x, _, size_z = size
    fetch = pltpu.make_async_copy(coef_in, coef, sems.at[4])
    fetch.start()
    fill_planes(lambda v, x: q_now[v, x], None, planes, None, size)
    fetch.wait()
    for k in range(table.shape[0]):
        table[k : k + 1, :] = jnp.full((1, size_z), coef[k], jnp.float32)
    mixing_weights(coef, weights.at[0], weights.at[1], size)
    copies = [pltpu.make_async_copy(weights, weights_out, sems.at[5])]
    copies[0].start()
    for x in range(size_x):
        flux = flux_at(x, weights, planes, None, size)
        scale = step_tau * jac[x]
        for v in range(nvars):
            centre = q_now[v, x]
            physical = (q_prev[v, x] - centre) / (2.0 * step_phys)
            buffer[v, x] = centre - scale * (flux[v] + physical)
        sent_out(x, size_x, buffer, base, sems, copies)
    for copy in copies:
        copy.wait()


def mixed_by(table, direction, side, lines):
    nvars = len(lines)
    out = []
    for a in range(nvars):
        total = None
        for b in range(nvars):
            k = ((direction * 2 + side) * nvars + a) * nvars + b
            term = table[k : k + 1, :] * lines[b]
            total = term if total is None else total + term
        out.append(total)
    return out


def land(rows, hot_xy, hot_z, store, nvars):
    columns = hot_xy.shape[0]
    for first in range(0, nvars, 2):
        some = range(first, min(first + 2, nvars))
        pieces = []
        for c in some:
            for half in halves(rows[c : c + 1, :]):
                pieces.append(hot_xy[...] * half)
        landed = dot(jnp.concatenate(pieces, axis=0), hot_z[...], ((1,), (0,)))
        for c in some:
            at = 2 * (c - first) * columns
            store(c, landed[at : at + columns] + landed[at + columns : at + 2 * columns])


def first_kernel(table, got, base_in, q_now, jac, line_inner, line_outer, state, hits, x_inner, x_outer, y_inner, y_outer, later, hot_xy, hot_z, rows, grid, base, sems, *, size, devices, capacity):
    nvars, size_x, size_y, size_z = size
    columns = size_x * size_y
    slots = devices * capacity

    def fetch(x):
        return pltpu.make_async_copy(base_in.at[:, pl.ds(x, 1)], base.at[:, pl.ds(x, 1)], sems.at[x])

    @pl.loop(0, size_x)
    def _(x):
        fetch(x).start()

    for d in range(devices):
        piece = got[d]
        lanes = slice(d * capacity, (d + 1) * capacity)
        rows[0:8, lanes] = piece[:, 0:capacity]
        rows[8:16, lanes] = piece[:, capacity : 2 * capacity]
    turned = jnp.transpose(rows[8:16, :])
    land_z = turned[:, 2 * nvars + 1 - 8 : 2 * nvars + 2 - 8]
    hot_z[...] = (iota((slots, size_z), 1).astype(jnp.float32) == land_z).astype(jnp.float32).astype(jnp.bfloat16)
    land_xy = rows[2 * nvars : 2 * nvars + 1, :]
    hot_xy[...] = ((iota((columns, slots), 0) + 1).astype(jnp.float32) == land_xy).astype(jnp.float32).astype(jnp.bfloat16)
    later[...] = rows[nvars : 2 * nvars, :]

    def keep(c, value):
        grid[c] = value

    hits[...] = dot(hot_xy[...], hot_z[...], ((1,), (0,)))
    land(rows, hot_xy, hot_z, keep, nvars)
    even_x, even_y = lax.axis_index("gx") % 2 == 0, lax.axis_index("gy") % 2 == 0
    y_low, y_high = zip(*(sides_of("gy", line_inner[v], line_outer[v]) for v in range(nvars)))
    from_low, from_high = mixed_by(table, 1, 0, y_low), mixed_by(table, 1, 1, y_high)
    row_at = iota((size_y, size_z), 0)
    faces = {}
    for x in range(size_x):
        fetch(x).wait()
    for x in range(size_x):
        at = slice(x * size_y, (x + 1) * size_y)
        landed = hits[at, :]
        scale = step_tau * jac[x]
        for v in range(nvars):
            change = penalty * (landed * q_now[v, x] - grid[v, at, :])
            change = change - jnp.where(row_at == 0, from_low[v][x : x + 1], 0.0)
            change = change + jnp.where(row_at == size_y - 1, from_high[v][x : x + 1], 0.0)
            new = base[v, x] - scale * change
            state[v, x] = new
            low, high = new[0:1], new[size_y - 1 : size_y]
            y_inner[v, x : x + 1, :] = jnp.where(even_y, high, low)
            y_outer[v, x : x + 1, :] = jnp.where(even_y, low, high)
            if x in (0, size_x - 1):
                faces[x, v] = new
    ends = [y_low[v] for v in range(nvars)] + [y_high[v] for v in range(nvars)]
    for v in range(nvars):
        for k, pair in enumerate(((faces[0, v], faces[size_x - 1, v]), (q_now[v, 0], q_now[v, size_x - 1]))):
            x_inner[k * nvars + v] = jnp.where(even_x, pair[1], pair[0])
            x_outer[k * nvars + v] = jnp.where(even_x, pair[0], pair[1])
    x_inner[2 * nvars] = jnp.where(even_x, jac[size_x - 1], jac[0])
    x_outer[2 * nvars] = jnp.where(even_x, jac[0], jac[size_x - 1])
    x_inner[2 * nvars + 1] = x_outer[2 * nvars + 1] = jnp.zeros((size_y, size_z), jnp.float32)
    for k, line in enumerate(ends):
        low, high = line[0:1], line[size_x - 1 : size_x]
        x_inner[2 * nvars + 1, k : k + 1, :] = jnp.where(even_x, high, low)
        x_outer[2 * nvars + 1, k : k + 1, :] = jnp.where(even_x, low, high)


def late_kernel(rows, hot_xy, hot_z, target):
    def keep(c, value):
        target[c] = value

    land(rows, hot_xy, hot_z, keep, rows.shape[0])


def second_kernel(table, state, weights, q_now, q_prev, jac, target, hits, x_inner, x_outer, y_inner, y_outer, line_inner, line_outer, out, planes, sides, edge, buffer, sems, *, size):
    nvars, size_x, size_y, size_z = size
    last = size_x - 1
    x_low, x_high = zip(*(sides_of("gx", x_inner[k], x_outer[k]) for k in range(2 * nvars + 2)))
    own_low = mixed_by(table, 0, 0, x_low[nvars : 2 * nvars])
    own_high = mixed_by(table, 0, 1, x_high[nvars : 2 * nvars])
    ring_low = mixed_by(table, 0, 1, [q_now[v, 0] for v in range(nvars)])
    ring_high = mixed_by(table, 0, 0, [q_now[v, last] for v in range(nvars)])
    around = [[], [], [], []]
    for v in range(nvars):
        edge[0, v] = state[v, 0] + step_tau * jac[0] * own_low[v]
        edge[1, v] = state[v, last] - step_tau * jac[last] * own_high[v]
        around[0].append(x_low[v] - step_tau * x_low[2 * nvars] * ring_low[v])
        around[1].append(x_high[v] + step_tau * x_high[2 * nvars] * ring_high[v])
    row_at = iota((size_x, size_z), 0)
    for side in range(2):
        scale = step_tau * sides_of("gy", line_inner[nvars], line_outer[nvars])[side]
        corner = slice(side * nvars, (side + 1) * nvars)
        low = mixed_by(table, 0, 0, [x_low[2 * nvars + 1][k : k + 1] for k in range(corner.start, corner.stop)])
        high = mixed_by(table, 0, 1, [x_high[2 * nvars + 1][k : k + 1] for k in range(corner.start, corner.stop)])
        for v in range(nvars):
            change = jnp.where(row_at == 0, low[v], 0.0) - jnp.where(row_at == last, high[v], 0.0)
            around[2 + side].append(sides_of("gy", y_inner[v], y_outer[v])[side] + scale * change)

    def at_plane(v, x):
        return edge[0, v] if x == 0 else edge[1, v] if x == last else state[v, x]

    fill_planes(at_plane, around, planes, sides, size)
    copies = []
    for x in range(size_x):
        at = slice(x * size_y, (x + 1) * size_y)
        flux = flux_at(x, weights, planes, sides, size)
        landed = hits[at, :]
        scale = step_tau * jac[x]
        for v in range(nvars):
            centre = at_plane(v, x)
            physical = (3.0 * centre - 4.0 * q_now[v, x] + q_prev[v, x]) / (2.0 * step_phys)
            coupling = penalty * (landed * centre - target[v, at, :])
            buffer[v, x] = centre - scale * (flux[v] + physical + coupling)
        sent_out(x, size_x, buffer, out, sems, copies)
    for copy in copies:
        copy.wait()


def swapped(inner, outer, axis):
    count_x, count_y = lax.axis_size("gx"), lax.axis_size("gy")
    inner_pairs, outer_pairs = [], []
    for i in range(count_x):
        for j in range(count_y):
            at, count = (i, count_x) if axis == "gx" else (j, count_y)
            for pairs, to in ((inner_pairs, at ^ 1), (outer_pairs, ((at + 1) ^ 1) - 1)):
                x, y = (to, j) if axis == "gx" else (i, to)
                if axis == "gx" and not 0 <= to < count:
                    x = count - 1 - at
                if axis == "gy" and not 0 <= to < count:
                    x, y = i ^ 1, j
                pairs.append((i * count_y + j, x * count_y + y))
    return lax.ppermute(inner, AXES, inner_pairs), lax.ppermute(outer, AXES, outer_pairs)


def sides_of(axis, inner, outer):
    here, last = lax.axis_index(axis), lax.axis_size(axis) - 1
    even = here % 2 == 0
    inside = (here > 0) & (here < last)
    masked = jnp.where(inside, outer, 0.0)
    return jnp.where(even, masked, inner), jnp.where(even, inner, masked)


def params(limit):
    return pltpu.CompilerParams(vmem_limit_bytes=limit)


def body(q_now, q_prev, jacobian, flux_split, donor_base, donor_frac, fringe_dest, receptor_cell, fringe_count):
    size = q_now.shape
    nvars, size_x, size_y, size_z = size
    columns = size_x * size_y
    block = nvars * size_y
    devices = lax.axis_size("gx") * lax.axis_size("gy")
    rows = donor_base.shape[0]
    capacity = 2 * rows // devices
    slots = devices * capacity
    f32, bf16 = jnp.float32, jnp.bfloat16
    hbm = pl.BlockSpec(memory_space=pltpu.HBM)
    vmem = pl.BlockSpec(memory_space=pltpu.VMEM)
    flat = (nvars, columns, size_z)
    shape = jax.ShapeDtypeStruct
    weights_shape = (2, 3 * block, 3 * block + CHANNELS)
    planes = pltpu.VMEM((2, (size_x + 2) * block, size_z), bf16)
    sides = pltpu.VMEM((size_x, CHANNELS, size_z), f32)
    face_y = shape((nvars, size_x, size_z), f32)

    line, line_x = pltpu.VMEM((nvars + 1, size_x, size_z), f32), shape((2 * nvars + 2, size_y, size_z), f32)
    coef = flux_split.reshape(-1)

    def there(x):
        return pltpu.with_memory_space_constraint(x, pltpu.HBM)

    sent, *lines = pl.pallas_call(
        functools.partial(donor_kernel, size=size, devices=devices, capacity=capacity),
        out_shape=[pltpu.VMEM((devices, 8, 2 * capacity), f32), line, line],
        in_specs=[pl.BlockSpec(memory_space=pltpu.SMEM)] + [hbm] * 7,
        out_specs=[vmem] * 3,
        scratch_shapes=[
            pltpu.VMEM((2, nvars, columns, size_z), f32),
            pltpu.VMEM((columns, size_z), f32),
            pltpu.VMEM((2, 2 * nvars * columns, size_z), bf16),
            pltpu.VMEM((2, size_z, rows), bf16),
            pltpu.VMEM((columns, rows), f32),
            pltpu.VMEM((rows, 8), f32),
            pltpu.VMEM((CHANNELS, rows), f32),
            pltpu.VMEM((1, rows), jnp.int32),
            pltpu.VMEM((3, rows), f32),
            pltpu.VMEM((1, rows), jnp.int32),
            pltpu.VMEM((1, rows), jnp.int32),
            pltpu.SemaphoreType.DMA((5 + 2 * nvars,)),
        ],
        compiler_params=params(DONOR_LIMIT),
        name="donor",
    )(
        fringe_count,
        there(q_prev.reshape(flat)),
        there(q_now.reshape(flat)),
        there(donor_base.reshape(1, rows)),
        there(donor_frac),
        there(fringe_dest.reshape(1, rows)),
        there(receptor_cell.reshape(1, rows)),
        there(jacobian.reshape(columns, size_z)),
    )
    got = lax.all_to_all(sent, AXES, split_axis=0, concat_axis=0, tiled=True)
    lines = swapped(*lines, "gy")
    base, weights, table = pl.pallas_call(
        functools.partial(early_kernel, size=size),
        out_shape=[pltpu.HBM(size, f32), pltpu.HBM(weights_shape, bf16), shape((4 * nvars * nvars, size_z), f32)],
        in_specs=[hbm] + [vmem] * 3,
        out_specs=[hbm, hbm, vmem],
        scratch_shapes=[planes, pltpu.SMEM((6 * nvars * nvars,), f32), pltpu.VMEM(size, f32), pltpu.VMEM(weights_shape, bf16), pltpu.SemaphoreType.DMA((6,))],
        compiler_params=params(20 * MIB),
        name="early",
    )(coef, q_now, q_prev, jacobian)
    state, hits, *faces, later, hot_xy, hot_z = pl.pallas_call(
        functools.partial(first_kernel, size=size, devices=devices, capacity=capacity),
        out_shape=[
            shape(size, f32),
            shape((columns, size_z), f32),
            line_x,
            line_x,
            face_y,
            face_y,
            shape((nvars, slots), f32),
            shape((columns, slots), bf16),
            shape((slots, size_z), bf16),
        ],
        in_specs=[vmem, vmem, hbm] + [vmem] * 4,
        out_specs=[vmem] * 9,
        scratch_shapes=[
            pltpu.VMEM((CHANNELS, slots), f32),
            pltpu.VMEM((nvars, columns, size_z), f32),
            pltpu.VMEM(size, f32),
            pltpu.SemaphoreType.DMA((size_x,)),
        ],
        compiler_params=params(20 * MIB),
        name="first",
    )(table, got, there(base), q_now, jacobian, *lines)
    around = (*swapped(*faces[0:2], "gx"), *swapped(*faces[2:4], "gy"))
    target = pl.pallas_call(
        late_kernel,
        out_shape=shape(flat, f32),
        in_specs=[vmem] * 3,
        out_specs=vmem,
        compiler_params=params(20 * MIB),
        name="late",
    )(later, hot_xy, hot_z)
    return pl.pallas_call(
        functools.partial(second_kernel, size=size),
        out_shape=shape(size, f32),
        in_specs=[vmem] * 14,
        out_specs=hbm,
        scratch_shapes=[planes, sides, pltpu.VMEM((2, nvars, size_y, size_z), f32), pltpu.VMEM(size, f32), pltpu.SemaphoreType.DMA((4,))],
        compiler_params=params(20 * MIB),
        name="second",
    )(table, state, weights, q_now, q_prev, jacobian, target, hits, *around, *lines)


def solution(mesh):
    return jax.shard_map(
        body,
        mesh=mesh,
        in_specs=(
            P(None, "gx", "gy", None),
            P(None, "gx", "gy", None),
            P("gx", "gy", None),
            P(),
            P(("gx", "gy")),
            P(None, ("gx", "gy")),
            P(("gx", "gy"), None),
            P(("gx", "gy")),
            P(("gx", "gy")),
        ),
        out_specs=P(None, "gx", "gy", None),
        check_vma=False,
    )
```

```python
import functools

import jax
import jax.numpy as jnp
from jax import lax
from jax.experimental import pallas as pl
from jax.experimental.pallas import tpu as pltpu
from jax.sharding import PartitionSpec as P


step_tau = 0.2
step_phys = 0.5
penalty = 2.0

AXES = ("gx", "gy")
LANES = 256
CHANNELS = 16
MIB = 1 << 20
DONOR_LIMIT = 44 * MIB
PIECES = 8


def iota(shape, dim):
    return lax.broadcasted_iota(jnp.int32, shape, dim)


def dot(a, b, dims):
    return lax.dot_general(a, b, (dims, ((), ())), preferred_element_type=jnp.float32)


def halves(x):
    high = x.astype(jnp.bfloat16)
    return high, (x - high.astype(jnp.float32)).astype(jnp.bfloat16)


def ranks(dest, devices):
    rows = dest.shape[1]
    blocks = rows // LANES
    hot = (iota((devices, rows), 0) == dest).astype(jnp.float32)
    stacked = jnp.concatenate([hot[:, b * LANES : (b + 1) * LANES] for b in range(blocks)], axis=0)
    before = (iota((LANES, LANES), 0) < iota((LANES, LANES), 1)).astype(jnp.float32)
    local = dot(stacked.astype(jnp.bfloat16), before.astype(jnp.bfloat16), ((1,), (0,)))
    carried = jnp.zeros((devices, 1), jnp.float32)
    pieces = []
    for b in range(blocks):
        part = local[b * devices : (b + 1) * devices]
        own = hot[:, b * LANES : (b + 1) * LANES]
        pieces.append(jnp.sum((part + carried) * own, axis=0, keepdims=True))
        carried = carried + jnp.sum(own, axis=1, keepdims=True)
    return jnp.concatenate(pieces, axis=1)


def donor_kernel(count, q_prev, q_now, base_in, frac_in, dest_in, cell_in, out_there, y_inner, y_outer, out, planes, lhs, spread, corner, place, values, base, frac, dest, cell, sems, *, size, devices, capacity):
    nvars, size_x, size_y, size_z = size
    columns = size_x * size_y
    rows = base.shape[1]
    small = [pltpu.make_async_copy(a, b, sems.at[k]) for k, (a, b) in enumerate(((base_in, base), (frac_in, frac), (dest_in, dest), (cell_in, cell)))]
    copies = [pltpu.make_async_copy(ref.at[v], planes.at[k, v], sems.at[5 + k * nvars + v]) for k, ref in enumerate((q_prev, q_now)) for v in range(nvars)]
    for copy in small + copies:
        copy.start()
    for copy in small:
        copy.wait()
    start = base[...].astype(jnp.float32)
    in_y = jnp.floor((start + 0.5) * (1.0 / (size_z - 1)))
    base_z = start - in_y * (size_z - 1)
    base_x = jnp.floor((in_y + 0.5) * (1.0 / (size_y - 1)))
    base_y = in_y - base_x * (size_y - 1)
    frac_x, frac_y, frac_z = frac[0:1, :], frac[1:2, :], frac[2:3, :]

    def weights(first, part, shape):
        at = iota(shape, 0).astype(jnp.float32) - first
        return jnp.where(at == 0.0, 1.0 - part, jnp.where(at == 1.0, part, 0.0))

    along_z = weights(base_z, frac_z, (size_z, rows))
    high, low = halves(along_z)
    spread[0] = high
    spread[1] = low
    along_x = weights(base_x, frac_x, (size_x, rows))
    along_y = weights(base_y, frac_y, (size_y, rows))
    for x in range(size_x):
        corner[x * size_y : (x + 1) * size_y, :] = along_x[x : x + 1, :] * along_y
    alive = iota((1, rows), 1) < count[0]
    slot = ranks(dest[...], devices)
    where_to = jnp.where(alive, dest[...].astype(jnp.float32) * capacity + slot, -1.0)
    place[...] = jnp.transpose(jnp.broadcast_to(where_to, (8, rows)))
    landing = cell[...].astype(jnp.float32)
    land_xy = jnp.floor((landing + 0.5) * (1.0 / size_z))
    values[...] = jnp.zeros(values.shape, jnp.float32)
    values[2 * nvars : 2 * nvars + 1, :] = land_xy + 1.0
    values[2 * nvars + 1 : 2 * nvars + 2, :] = landing - land_xy * size_z
    for k in range(2):
        if k == 1:
            for v in range(nvars):
                copies[nvars + v].wait()
            even = lax.axis_index("gy") % 2 == 0
            for v in range(nvars):
                for x in range(size_x):
                    line = planes.at[1, v]
                    low = line[x * size_y : x * size_y + 1, :]
                    high = line[(x + 1) * size_y - 1 : (x + 1) * size_y, :]
                    y_inner[v, x : x + 1, :] = jnp.where(even, high, low)
                    y_outer[v, x : x + 1, :] = jnp.where(even, low, high)
        for v in range(nvars):
            if k == 0:
                copies[v].wait()
            at = pl.ds((k * nvars + v) * columns, columns)
            high, low = halves(planes[k, v])
            lhs[0, at, :] = high
            lhs[1, at, :] = low
    for n in range(rows // LANES):
        lanes = slice(n * LANES, (n + 1) * LANES)
        for k in range(2):
            at = slice(k * nvars * columns, (k + 1) * nvars * columns)
            part = dot(lhs[0, at, :], spread[0, :, lanes], ((1,), (0,)))
            part = part + dot(lhs[0, at, :], spread[1, :, lanes], ((1,), (0,)))
            part = part + dot(lhs[1, at, :], spread[0, :, lanes], ((1,), (0,)))
            for v in range(nvars):
                picked = part[v * columns : (v + 1) * columns] * corner[:, lanes]
                values[k * nvars + v : k * nvars + v + 1, lanes] = jnp.sum(picked, axis=0, keepdims=True)
    first = values[...]
    high, rest = first.astype(jnp.bfloat16), None
    rest = first - high.astype(jnp.float32)
    middle = rest.astype(jnp.bfloat16)
    last = (rest - middle.astype(jnp.float32)).astype(jnp.bfloat16)
    three = jnp.concatenate([high, middle, last], axis=0)
    leaving = []
    column = jnp.broadcast_to(place[:, 0:1], (rows, LANES))
    for n in range(devices * capacity // LANES):
        chosen = (column == (iota((rows, LANES), 1) + n * LANES).astype(jnp.float32)).astype(jnp.float32).astype(jnp.bfloat16)
        moved = dot(three, chosen, ((1,), (0,)))
        moved = moved[0:CHANNELS] + moved[CHANNELS : 2 * CHANNELS] + moved[2 * CHANNELS : 3 * CHANNELS]
        for d in range(LANES // capacity):
            piece = moved[:, d * capacity : (d + 1) * capacity]
            to = n * (LANES // capacity) + d
            out[to] = jnp.concatenate([piece[0:8], piece[8:16]], axis=1)
        some = pl.ds(n * (LANES // capacity), LANES // capacity)
        leaving.append(pltpu.make_async_copy(out.at[some], out_there.at[some], sems.at[n]))
        leaving[-1].start()
    for copy in leaving:
        copy.wait()


def mixing_weights(coef, high, low, size):
    nvars, _, size_y, _ = size
    block = nvars * size_y
    width = 3 * block + CHANNELS
    row = iota((size_y, width), 0)
    offset = iota((size_y, width), 1) - row
    lane = iota((size_y, width), 1)

    def at(d, side, a, b):
        return coef[((d * 2 + side) * nvars + a) * nvars + b]

    for a in range(nvars):
        main = jnp.zeros((size_y, width), jnp.float32)
        back = main
        fore = main
        for b in range(nvars):
            first = b * size_y
            same = at(0, 0, a, b) - at(0, 1, a, b) + at(1, 0, a, b) - at(1, 1, a, b) + at(2, 0, a, b) - at(2, 1, a, b)
            main = jnp.where(offset == first, -at(0, 0, a, b), main)
            main = jnp.where(offset == block + first, same, main)
            main = jnp.where((offset == block + first - 1) & (row > 0), -at(1, 0, a, b), main)
            main = jnp.where((offset == block + first + 1) & (row < size_y - 1), at(1, 1, a, b), main)
            main = jnp.where(offset == 2 * block + first, at(0, 1, a, b), main)
            main = jnp.where((lane == 3 * block + b) & (row == 0), -at(1, 0, a, b), main)
            main = jnp.where((lane == 3 * block + nvars + b) & (row == size_y - 1), at(1, 1, a, b), main)
            back = jnp.where(offset == block + first, -at(2, 0, a, b), back)
            fore = jnp.where(offset == block + first, at(2, 1, a, b), fore)
        for k, part in enumerate((main, back, fore)):
            rows = slice(k * block + a * size_y, k * block + (a + 1) * size_y)
            high[rows, :], low[rows, :] = halves(part)


def fill_planes(at_plane, around, planes, sides, size):
    nvars, size_x, size_y, size_z = size
    block = nvars * size_y
    for x in range(size_x + 2):
        for v in range(nvars):
            rows = slice(x * block + v * size_y, x * block + (v + 1) * size_y)
            if 0 < x <= size_x:
                planes[0, rows, :], planes[1, rows, :] = halves(at_plane(v, x - 1))
            elif around is None:
                planes[0, rows, :] = planes[1, rows, :] = jnp.zeros((size_y, size_z), jnp.bfloat16)
            else:
                planes[0, rows, :], planes[1, rows, :] = halves(around[0 if x == 0 else 1][v])
    if around is not None:
        sides[...] = jnp.zeros(sides.shape, jnp.float32)
        for v in range(nvars):
            sides[:, v, :] = around[2][v]
            sides[:, nvars + v, :] = around[3][v]


def flux_at(x, weights, planes, sides, size):
    nvars, _, size_y, size_z = size
    block = nvars * size_y
    if sides is None:
        high = low = jnp.zeros((CHANNELS, size_z), jnp.bfloat16)
    else:
        high, low = halves(sides[x])
    rows = slice(x * block, (x + 3) * block)
    around_high = jnp.concatenate([planes[0, rows, :], high], axis=0)
    around_low = jnp.concatenate([planes[1, rows, :], low], axis=0)
    both = jnp.concatenate([weights[0], weights[1]], axis=0)
    mixed = dot(both, around_high, ((1,), (0,)))
    mixed = mixed[0 : 3 * block] + mixed[3 * block :] + dot(weights[0], around_low, ((1,), (0,)))
    z_at = iota((block, size_z), 1)
    back = jnp.where(z_at == 0, 0.0, pltpu.roll(mixed[block : 2 * block], 1, 1))
    fore = jnp.where(z_at == size_z - 1, 0.0, pltpu.roll(mixed[2 * block :], size_z - 1, 1))
    flux = mixed[0:block] + back + fore
    return [flux[v * size_y : (v + 1) * size_y] for v in range(nvars)]


def sent_out(x, size_x, buffer, out, sems, copies):
    part = size_x // PIECES
    if (x + 1) % part == 0:
        some = pl.ds(x + 1 - part, part)
        copies.append(pltpu.make_async_copy(buffer.at[:, some], out.at[:, some], sems.at[x // part]))
        copies[-1].start()


def early_kernel(coef_in, q_now, q_prev, jac, base, weights_out, table, planes, coef, buffer, weights, sems, *, size):
    nvars, size_x, _, size_z = size
    fetch = pltpu.make_async_copy(coef_in, coef, sems.at[PIECES])
    fetch.start()
    fill_planes(lambda v, x: q_now[v, x], None, planes, None, size)
    fetch.wait()
    for k in range(table.shape[0]):
        table[k : k + 1, :] = jnp.full((1, size_z), coef[k], jnp.float32)
    mixing_weights(coef, weights.at[0], weights.at[1], size)
    copies = [pltpu.make_async_copy(weights, weights_out, sems.at[PIECES + 1])]
    copies[0].start()
    for x in range(size_x):
        flux = flux_at(x, weights, planes, None, size)
        scale = step_tau * jac[x]
        for v in range(nvars):
            centre = q_now[v, x]
            physical = (q_prev[v, x] - centre) / (2.0 * step_phys)
            buffer[v, x] = centre - scale * (flux[v] + physical)
        sent_out(x, size_x, buffer, base, sems, copies)
    for copy in copies:
        copy.wait()


def mixed_by(table, direction, side, lines):
    nvars = len(lines)
    out = []
    for a in range(nvars):
        total = None
        for b in range(nvars):
            k = ((direction * 2 + side) * nvars + a) * nvars + b
            term = table[k : k + 1, :] * lines[b]
            total = term if total is None else total + term
        out.append(total)
    return out


def land(rows, hot_xy, hot_z, store, nvars):
    columns = hot_xy.shape[0]
    for first in range(0, nvars, 2):
        some = range(first, min(first + 2, nvars))
        pieces = []
        for c in some:
            for half in halves(rows[c : c + 1, :]):
                pieces.append(hot_xy[...] * half)
        landed = dot(jnp.concatenate(pieces, axis=0), hot_z[...], ((1,), (0,)))
        for c in some:
            at = 2 * (c - first) * columns
            store(c, landed[at : at + columns] + landed[at + columns : at + 2 * columns])


def first_kernel(table, got, base_in, q_now, jac, line_inner, line_outer, state, hits, x_inner, x_outer, y_inner, y_outer, later, hot_xy, hot_z, rows, grid, base, sems, *, size, devices, capacity):
    nvars, size_x, size_y, size_z = size
    columns = size_x * size_y
    slots = devices * capacity

    def fetch(x):
        return pltpu.make_async_copy(base_in.at[:, pl.ds(x, 1)], base.at[:, pl.ds(x, 1)], sems.at[x])

    @pl.loop(0, size_x)
    def _(x):
        fetch(x).start()

    for d in range(devices):
        piece = got[d]
        lanes = slice(d * capacity, (d + 1) * capacity)
        rows[0:8, lanes] = piece[:, 0:capacity]
        rows[8:16, lanes] = piece[:, capacity : 2 * capacity]
    turned = jnp.transpose(rows[8:16, :])
    land_z = turned[:, 2 * nvars + 1 - 8 : 2 * nvars + 2 - 8]
    hot_z[...] = (iota((slots, size_z), 1).astype(jnp.float32) == land_z).astype(jnp.float32).astype(jnp.bfloat16)
    land_xy = rows[2 * nvars : 2 * nvars + 1, :]
    hot_xy[...] = ((iota((columns, slots), 0) + 1).astype(jnp.float32) == land_xy).astype(jnp.float32).astype(jnp.bfloat16)
    later[...] = rows[nvars : 2 * nvars, :]

    hits[...] = dot(hot_xy[...], hot_z[...], ((1,), (0,)))
    even_x, even_y = lax.axis_index("gx") % 2 == 0, lax.axis_index("gy") % 2 == 0
    y_low, y_high = zip(*(sides_of("gy", line_inner[v], line_outer[v]) for v in range(nvars)))
    from_low, from_high = mixed_by(table, 1, 0, y_low), mixed_by(table, 1, 1, y_high)
    row_at = iota((size_y, size_z), 0)
    faces = {}

    def keep(c, value):
        grid[c] = value

    land(rows, hot_xy, hot_z, keep, nvars)
    for x in range(size_x):
        fetch(x).wait()
    for x in range(size_x):
        at = slice(x * size_y, (x + 1) * size_y)
        landed = hits[at, :]
        scale = step_tau * jac[x]
        for v in range(nvars):
            change = penalty * (landed * q_now[v, x] - grid[v, at, :])
            change = change - jnp.where(row_at == 0, from_low[v][x : x + 1], 0.0)
            change = change + jnp.where(row_at == size_y - 1, from_high[v][x : x + 1], 0.0)
            new = base[v, x] - scale * change
            state[v, x] = new
            low, high = new[0:1], new[size_y - 1 : size_y]
            y_inner[v * size_x + x : v * size_x + x + 1, :] = jnp.where(even_y, high, low)
            y_outer[v * size_x + x : v * size_x + x + 1, :] = jnp.where(even_y, low, high)
            if x in (0, size_x - 1):
                faces[x, v] = new
    tail = nvars * size_x
    y_inner[tail:, :] = y_outer[tail:, :] = jnp.zeros((8, size_z), jnp.float32)
    for k, x in enumerate((0, size_x - 1)):
        low, high = jac[x][0:1], jac[x][size_y - 1 : size_y]
        y_inner[tail + k : tail + k + 1, :] = jnp.where(even_y, high, low)
        y_outer[tail + k : tail + k + 1, :] = jnp.where(even_y, low, high)
    ends = [y_low[v] for v in range(nvars)] + [y_high[v] for v in range(nvars)]
    for v in range(nvars):
        for k, pair in enumerate(((faces[0, v], faces[size_x - 1, v]), (q_now[v, 0], q_now[v, size_x - 1]))):
            x_inner[k * nvars + v] = jnp.where(even_x, pair[1], pair[0])
            x_outer[k * nvars + v] = jnp.where(even_x, pair[0], pair[1])
    x_inner[2 * nvars] = jnp.where(even_x, jac[size_x - 1], jac[0])
    x_outer[2 * nvars] = jnp.where(even_x, jac[0], jac[size_x - 1])
    x_inner[2 * nvars + 1] = x_outer[2 * nvars + 1] = jnp.zeros((size_y, size_z), jnp.float32)
    for k, line in enumerate(ends):
        low, high = line[0:1], line[size_x - 1 : size_x]
        x_inner[2 * nvars + 1, k : k + 1, :] = jnp.where(even_x, high, low)
        x_outer[2 * nvars + 1, k : k + 1, :] = jnp.where(even_x, low, high)


def late_kernel(rows, hot_xy, hot_z, target):
    def keep(c, value):
        target[c] = value

    land(rows, hot_xy, hot_z, keep, rows.shape[0])


def second_kernel(table, state, weights, q_now, q_prev, jac, target, hits, x_inner, x_outer, y_inner, y_outer, out, planes, sides, edge, buffer, sems, *, size):
    nvars, size_x, size_y, size_z = size
    last = size_x - 1
    x_low, x_high = zip(*(sides_of("gx", x_inner[k], x_outer[k]) for k in range(2 * nvars + 2)))
    own_low = mixed_by(table, 0, 0, x_low[nvars : 2 * nvars])
    own_high = mixed_by(table, 0, 1, x_high[nvars : 2 * nvars])
    ring_low = mixed_by(table, 0, 1, [q_now[v, 0] for v in range(nvars)])
    ring_high = mixed_by(table, 0, 0, [q_now[v, last] for v in range(nvars)])
    around = [[], [], [], []]
    for v in range(nvars):
        edge[0, v] = state[v, 0] + step_tau * jac[0] * own_low[v]
        edge[1, v] = state[v, last] - step_tau * jac[last] * own_high[v]
        around[0].append(x_low[v] - step_tau * x_low[2 * nvars] * ring_low[v])
        around[1].append(x_high[v] + step_tau * x_high[2 * nvars] * ring_high[v])
    row_at = iota((size_x, size_z), 0)
    tail = nvars * size_x
    for side in range(2):
        scale = sides_of("gy", y_inner[tail:, :], y_outer[tail:, :])[side]
        corner = range(side * nvars, (side + 1) * nvars)
        low = mixed_by(table, 0, 0, [x_low[2 * nvars + 1][k : k + 1] for k in corner])
        high = mixed_by(table, 0, 1, [x_high[2 * nvars + 1][k : k + 1] for k in corner])
        for v in range(nvars):
            change = jnp.where(row_at == 0, scale[0:1] * low[v], 0.0) - jnp.where(row_at == last, scale[1:2] * high[v], 0.0)
            face = slice(v * size_x, (v + 1) * size_x)
            around[2 + side].append(sides_of("gy", y_inner[face, :], y_outer[face, :])[side] + step_tau * change)

    def at_plane(v, x):
        return edge[0, v] if x == 0 else edge[1, v] if x == last else state[v, x]

    fill_planes(at_plane, around, planes, sides, size)
    copies = []
    for x in range(size_x):
        at = slice(x * size_y, (x + 1) * size_y)
        flux = flux_at(x, weights, planes, sides, size)
        landed = hits[at, :]
        scale = step_tau * jac[x]
        for v in range(nvars):
            centre = at_plane(v, x)
            physical = (3.0 * centre - 4.0 * q_now[v, x] + q_prev[v, x]) / (2.0 * step_phys)
            coupling = penalty * (landed * centre - target[v, at, :])
            buffer[v, x] = centre - scale * (flux[v] + physical + coupling)
        sent_out(x, size_x, buffer, out, sems, copies)
    for copy in copies:
        copy.wait()


def swapped(inner, outer, axis):
    count_x, count_y = lax.axis_size("gx"), lax.axis_size("gy")
    inner_pairs, outer_pairs = [], []
    for i in range(count_x):
        for j in range(count_y):
            at, count = (i, count_x) if axis == "gx" else (j, count_y)
            for pairs, to in ((inner_pairs, at ^ 1), (outer_pairs, ((at + 1) ^ 1) - 1)):
                x, y = (to, j) if axis == "gx" else (i, to)
                if axis == "gx" and not 0 <= to < count:
                    x, y = i, j ^ 2
                if axis == "gy" and not 0 <= to < count:
                    x, y = i ^ 1, j
                pairs.append((i * count_y + j, x * count_y + y))
    return lax.ppermute(inner, AXES, inner_pairs), lax.ppermute(outer, AXES, outer_pairs)


def sides_of(axis, inner, outer):
    here, last = lax.axis_index(axis), lax.axis_size(axis) - 1
    even = here % 2 == 0
    inside = (here > 0) & (here < last)
    masked = jnp.where(inside, outer, 0.0)
    return jnp.where(even, masked, inner), jnp.where(even, inner, masked)


def params(limit):
    return pltpu.CompilerParams(vmem_limit_bytes=limit)


def body(q_now, q_prev, jacobian, flux_split, donor_base, donor_frac, fringe_dest, receptor_cell, fringe_count):
    size = q_now.shape
    nvars, size_x, size_y, size_z = size
    columns = size_x * size_y
    block = nvars * size_y
    devices = lax.axis_size("gx") * lax.axis_size("gy")
    rows = donor_base.shape[0]
    capacity = 2 * rows // devices
    slots = devices * capacity
    f32, bf16 = jnp.float32, jnp.bfloat16
    hbm = pl.BlockSpec(memory_space=pltpu.HBM)
    vmem = pl.BlockSpec(memory_space=pltpu.VMEM)
    flat = (nvars, columns, size_z)
    shape = jax.ShapeDtypeStruct
    weights_shape = (2, 3 * block, 3 * block + CHANNELS)
    planes = pltpu.VMEM((2, (size_x + 2) * block, size_z), bf16)
    sides = pltpu.VMEM((size_x, CHANNELS, size_z), f32)
    face_y = shape((nvars * size_x + 8, size_z), f32)

    line, line_x = pltpu.VMEM((nvars, size_x, size_z), f32), shape((2 * nvars + 2, size_y, size_z), f32)
    coef = flux_split.reshape(-1)

    def there(x):
        return pltpu.with_memory_space_constraint(x, pltpu.HBM)

    sent, *lines = pl.pallas_call(
        functools.partial(donor_kernel, size=size, devices=devices, capacity=capacity),
        out_shape=[pltpu.HBM((devices, 8, 2 * capacity), f32), line, line],
        in_specs=[pl.BlockSpec(memory_space=pltpu.SMEM)] + [hbm] * 6,
        out_specs=[hbm, vmem, vmem],
        scratch_shapes=[
            pltpu.VMEM((devices, 8, 2 * capacity), f32),
            pltpu.VMEM((2, nvars, columns, size_z), f32),
            pltpu.VMEM((2, 2 * nvars * columns, size_z), bf16),
            pltpu.VMEM((2, size_z, rows), bf16),
            pltpu.VMEM((columns, rows), f32),
            pltpu.VMEM((rows, 8), f32),
            pltpu.VMEM((CHANNELS, rows), f32),
            pltpu.VMEM((1, rows), jnp.int32),
            pltpu.VMEM((3, rows), f32),
            pltpu.VMEM((1, rows), jnp.int32),
            pltpu.VMEM((1, rows), jnp.int32),
            pltpu.SemaphoreType.DMA((5 + 2 * nvars,)),
        ],
        compiler_params=params(DONOR_LIMIT),
        name="donor",
    )(
        fringe_count,
        there(q_prev.reshape(flat)),
        there(q_now.reshape(flat)),
        there(donor_base.reshape(1, rows)),
        there(donor_frac),
        there(fringe_dest.reshape(1, rows)),
        there(receptor_cell.reshape(1, rows)),
    )
    got = lax.all_to_all(sent, AXES, split_axis=0, concat_axis=0, tiled=True)
    lines = swapped(*lines, "gy")
    base, weights, table = pl.pallas_call(
        functools.partial(early_kernel, size=size),
        out_shape=[pltpu.HBM(size, f32), pltpu.HBM(weights_shape, bf16), shape((4 * nvars * nvars, size_z), f32)],
        in_specs=[hbm] + [vmem] * 3,
        out_specs=[hbm, hbm, vmem],
        scratch_shapes=[planes, pltpu.SMEM((6 * nvars * nvars,), f32), pltpu.VMEM(size, f32), pltpu.VMEM(weights_shape, bf16), pltpu.SemaphoreType.DMA((PIECES + 2,))],
        compiler_params=params(20 * MIB),
        name="early",
    )(coef, q_now, q_prev, jacobian)
    state, hits, *faces, later, hot_xy, hot_z = pl.pallas_call(
        functools.partial(first_kernel, size=size, devices=devices, capacity=capacity),
        out_shape=[
            shape(size, f32),
            shape((columns, size_z), f32),
            line_x,
            line_x,
            face_y,
            face_y,
            shape((nvars, slots), f32),
            shape((columns, slots), bf16),
            shape((slots, size_z), bf16),
        ],
        in_specs=[vmem, vmem, hbm] + [vmem] * 4,
        out_specs=[vmem] * 9,
        scratch_shapes=[
            pltpu.VMEM((CHANNELS, slots), f32),
            pltpu.VMEM((nvars, columns, size_z), f32),
            pltpu.VMEM(size, f32),
            pltpu.SemaphoreType.DMA((size_x,)),
        ],
        compiler_params=params(20 * MIB),
        name="first",
    )(table, got, there(base), q_now, jacobian, *lines)
    around = (*swapped(*faces[0:2], "gx"), *swapped(*faces[2:4], "gy"))
    target = pl.pallas_call(
        late_kernel,
        out_shape=shape(flat, f32),
        in_specs=[vmem] * 3,
        out_specs=vmem,
        compiler_params=params(20 * MIB),
        name="late",
    )(later, hot_xy, hot_z)
    return pl.pallas_call(
        functools.partial(second_kernel, size=size),
        out_shape=shape(size, f32),
        in_specs=[vmem] * 12,
        out_specs=hbm,
        scratch_shapes=[planes, sides, pltpu.VMEM((2, nvars, size_y, size_z), f32), pltpu.VMEM(size, f32), pltpu.SemaphoreType.DMA((PIECES,))],
        compiler_params=params(20 * MIB),
        name="second",
    )(table, state, weights, q_now, q_prev, jacobian, target, hits, *around)


def solution(mesh):
    return jax.shard_map(
        body,
        mesh=mesh,
        in_specs=(
            P(None, "gx", "gy", None),
            P(None, "gx", "gy", None),
            P("gx", "gy", None),
            P(),
            P(("gx", "gy")),
            P(None, ("gx", "gy")),
            P(("gx", "gy"), None),
            P(("gx", "gy")),
            P(("gx", "gy")),
        ),
        out_specs=P(None, "gx", "gy", None),
        check_vma=False,
    )
```

```python
import functools

import jax
import jax.numpy as jnp
from jax import lax
from jax.experimental import pallas as pl
from jax.experimental.pallas import tpu as pltpu
from jax.sharding import PartitionSpec as P


step_tau = 0.2
step_phys = 0.5
penalty = 2.0

AXES = ("gx", "gy")
LANES = 256
CHANNELS = 16
MIB = 1 << 20
DONOR_LIMIT = 44 * MIB
PIECES = 8


def iota(shape, dim):
    return lax.broadcasted_iota(jnp.int32, shape, dim)


def dot(a, b, dims):
    return lax.dot_general(a, b, (dims, ((), ())), preferred_element_type=jnp.float32)


def halves(x):
    high = x.astype(jnp.bfloat16)
    return high, (x - high.astype(jnp.float32)).astype(jnp.bfloat16)


def eighth(x, power):
    return (x * 2.0**power).astype(jnp.float8_e4m3fn)


def ranks(dest, devices):
    rows = dest.shape[1]
    blocks = rows // LANES
    hot = (iota((devices, rows), 0) == dest).astype(jnp.float32)
    stacked = jnp.concatenate([hot[:, b * LANES : (b + 1) * LANES] for b in range(blocks)], axis=0)
    before = (iota((LANES, LANES), 0) < iota((LANES, LANES), 1)).astype(jnp.float32)
    local = dot(stacked.astype(jnp.bfloat16), before.astype(jnp.bfloat16), ((1,), (0,)))
    carried = jnp.zeros((devices, 1), jnp.float32)
    pieces = []
    for b in range(blocks):
        part = local[b * devices : (b + 1) * devices]
        own = hot[:, b * LANES : (b + 1) * LANES]
        pieces.append(jnp.sum((part + carried) * own, axis=0, keepdims=True))
        carried = carried + jnp.sum(own, axis=1, keepdims=True)
    return jnp.concatenate(pieces, axis=1)


def donor_kernel(count, q_prev, q_now, base_in, frac_in, dest_in, cell_in, out_there, y_inner, y_outer, out, planes, lhs, lhs_low, spread, spread_low, corner, place, values, base, frac, dest, cell, sems, *, size, devices, capacity):
    nvars, size_x, size_y, size_z = size
    columns = size_x * size_y
    rows = base.shape[1]
    small = [pltpu.make_async_copy(a, b, sems.at[k]) for k, (a, b) in enumerate(((base_in, base), (frac_in, frac), (dest_in, dest), (cell_in, cell)))]
    copies = [pltpu.make_async_copy(ref.at[v], planes.at[k, v], sems.at[5 + k * nvars + v]) for k, ref in enumerate((q_prev, q_now)) for v in range(nvars)]
    for copy in small + copies:
        copy.start()
    for copy in small:
        copy.wait()
    start = base[...].astype(jnp.float32)
    in_y = jnp.floor((start + 0.5) * (1.0 / (size_z - 1)))
    base_z = start - in_y * (size_z - 1)
    base_x = jnp.floor((in_y + 0.5) * (1.0 / (size_y - 1)))
    base_y = in_y - base_x * (size_y - 1)
    frac_x, frac_y, frac_z = frac[0:1, :], frac[1:2, :], frac[2:3, :]

    def weights(first, part, shape):
        at = iota(shape, 0).astype(jnp.float32) - first
        return jnp.where(at == 0.0, 1.0 - part, jnp.where(at == 1.0, part, 0.0))

    along_z = weights(base_z, frac_z, (size_z, rows))
    spread[...] = along_z.astype(jnp.bfloat16)
    rest = along_z - spread[...].astype(jnp.float32)
    spread_low[0:size_z, :] = eighth(rest, 16)
    spread_low[size_z : 2 * size_z, :] = eighth(along_z, 8)
    along_x = weights(base_x, frac_x, (size_x, rows))
    along_y = weights(base_y, frac_y, (size_y, rows))
    for x in range(size_x):
        corner[x * size_y : (x + 1) * size_y, :] = along_x[x : x + 1, :] * along_y
    alive = iota((1, rows), 1) < count[0]
    slot = ranks(dest[...], devices)
    where_to = jnp.where(alive, dest[...].astype(jnp.float32) * capacity + slot, -1.0)
    place[...] = jnp.transpose(jnp.broadcast_to(where_to, (8, rows)))
    landing = cell[...].astype(jnp.float32)
    land_xy = jnp.floor((landing + 0.5) * (1.0 / size_z))
    values[...] = jnp.zeros(values.shape, jnp.float32)
    values[2 * nvars : 2 * nvars + 1, :] = land_xy + 1.0
    values[2 * nvars + 1 : 2 * nvars + 2, :] = landing - land_xy * size_z
    for k in range(2):
        if k == 1:
            for v in range(nvars):
                copies[nvars + v].wait()
            even = lax.axis_index("gy") % 2 == 0
            for v in range(nvars):
                for x in range(size_x):
                    line = planes.at[1, v]
                    low = line[x * size_y : x * size_y + 1, :]
                    high = line[(x + 1) * size_y - 1 : (x + 1) * size_y, :]
                    y_inner[v, x : x + 1, :] = jnp.where(even, high, low)
                    y_outer[v, x : x + 1, :] = jnp.where(even, low, high)
        for v in range(nvars):
            if k == 0:
                copies[v].wait()
            at = pl.ds((k * nvars + v) * columns, columns)
            plane = planes[k, v]
            lhs[at, :] = plane.astype(jnp.bfloat16)
            lhs_low[at, 0:size_z] = eighth(plane, 6)
            lhs_low[at, size_z : 2 * size_z] = eighth(plane - plane.astype(jnp.bfloat16).astype(jnp.float32), 14)
    for n in range(rows // LANES):
        lanes = slice(n * LANES, (n + 1) * LANES)
        for k in range(2):
            at = slice(k * nvars * columns, (k + 1) * nvars * columns)
            part = dot(lhs[at, :], spread[:, lanes], ((1,), (0,)))
            part = part + 2.0**-22 * dot(lhs_low[at, :], spread_low[:, lanes], ((1,), (0,)))
            for v in range(nvars):
                picked = part[v * columns : (v + 1) * columns] * corner[:, lanes]
                values[k * nvars + v : k * nvars + v + 1, lanes] = jnp.sum(picked, axis=0, keepdims=True)
    first = values[...]
    high, rest = first.astype(jnp.bfloat16), None
    rest = first - high.astype(jnp.float32)
    middle = rest.astype(jnp.bfloat16)
    last = (rest - middle.astype(jnp.float32)).astype(jnp.bfloat16)
    three = jnp.concatenate([high, middle, last], axis=0)
    leaving = []
    column = jnp.broadcast_to(place[:, 0:1], (rows, LANES))
    for n in range(devices * capacity // LANES):
        chosen = (column == (iota((rows, LANES), 1) + n * LANES).astype(jnp.float32)).astype(jnp.float32).astype(jnp.bfloat16)
        moved = dot(three, chosen, ((1,), (0,)))
        moved = moved[0:CHANNELS] + moved[CHANNELS : 2 * CHANNELS] + moved[2 * CHANNELS : 3 * CHANNELS]
        for d in range(LANES // capacity):
            piece = moved[:, d * capacity : (d + 1) * capacity]
            to = n * (LANES // capacity) + d
            out[to] = jnp.concatenate([piece[0:8], piece[8:16]], axis=1)
        some = pl.ds(n * (LANES // capacity), LANES // capacity)
        leaving.append(pltpu.make_async_copy(out.at[some], out_there.at[some], sems.at[n]))
        leaving[-1].start()
    for copy in leaving:
        copy.wait()


def mixing_weights(coef, high, low, size):
    nvars, _, size_y, _ = size
    block = nvars * size_y
    width = 3 * block + CHANNELS
    row = iota((size_y, width), 0)
    offset = iota((size_y, width), 1) - row
    lane = iota((size_y, width), 1)

    def at(d, side, a, b):
        return coef[((d * 2 + side) * nvars + a) * nvars + b]

    for a in range(nvars):
        main = jnp.zeros((size_y, width), jnp.float32)
        back = main
        fore = main
        for b in range(nvars):
            first = b * size_y
            same = at(0, 0, a, b) - at(0, 1, a, b) + at(1, 0, a, b) - at(1, 1, a, b) + at(2, 0, a, b) - at(2, 1, a, b)
            main = jnp.where(offset == first, -at(0, 0, a, b), main)
            main = jnp.where(offset == block + first, same, main)
            main = jnp.where((offset == block + first - 1) & (row > 0), -at(1, 0, a, b), main)
            main = jnp.where((offset == block + first + 1) & (row < size_y - 1), at(1, 1, a, b), main)
            main = jnp.where(offset == 2 * block + first, at(0, 1, a, b), main)
            main = jnp.where((lane == 3 * block + b) & (row == 0), -at(1, 0, a, b), main)
            main = jnp.where((lane == 3 * block + nvars + b) & (row == size_y - 1), at(1, 1, a, b), main)
            back = jnp.where(offset == block + first, -at(2, 0, a, b), back)
            fore = jnp.where(offset == block + first, at(2, 1, a, b), fore)
        for k, part in enumerate((main, back, fore)):
            rows = slice(k * block + a * size_y, k * block + (a + 1) * size_y)
            high[rows, :], low[rows, :] = halves(part)


def fill_planes(at_plane, around, planes, sides, size):
    nvars, size_x, size_y, size_z = size
    block = nvars * size_y
    for x in range(size_x + 2):
        for v in range(nvars):
            rows = slice(x * block + v * size_y, x * block + (v + 1) * size_y)
            if 0 < x <= size_x:
                planes[0, rows, :], planes[1, rows, :] = halves(at_plane(v, x - 1))
            elif around is None:
                planes[0, rows, :] = planes[1, rows, :] = jnp.zeros((size_y, size_z), jnp.bfloat16)
            else:
                planes[0, rows, :], planes[1, rows, :] = halves(around[0 if x == 0 else 1][v])
    if around is not None:
        sides[...] = jnp.zeros(sides.shape, jnp.float32)
        for v in range(nvars):
            sides[:, v, :] = around[2][v]
            sides[:, nvars + v, :] = around[3][v]


def flux_at(x, weights, planes, sides, size):
    nvars, _, size_y, size_z = size
    block = nvars * size_y
    if sides is None:
        high = low = jnp.zeros((CHANNELS, size_z), jnp.bfloat16)
    else:
        high, low = halves(sides[x])
    rows = slice(x * block, (x + 3) * block)
    around_high = jnp.concatenate([planes[0, rows, :], high], axis=0)
    around_low = jnp.concatenate([planes[1, rows, :], low], axis=0)
    both = jnp.concatenate([weights[0], weights[1]], axis=0)
    mixed = dot(both, around_high, ((1,), (0,)))
    mixed = mixed[0 : 3 * block] + mixed[3 * block :] + dot(weights[0], around_low, ((1,), (0,)))
    z_at = iota((block, size_z), 1)
    back = jnp.where(z_at == 0, 0.0, pltpu.roll(mixed[block : 2 * block], 1, 1))
    fore = jnp.where(z_at == size_z - 1, 0.0, pltpu.roll(mixed[2 * block :], size_z - 1, 1))
    flux = mixed[0:block] + back + fore
    return [flux[v * size_y : (v + 1) * size_y] for v in range(nvars)]


def sent_out(x, size_x, buffer, out, sems, copies):
    part = size_x // PIECES
    if (x + 1) % part == 0:
        some = pl.ds(x + 1 - part, part)
        copies.append(pltpu.make_async_copy(buffer.at[:, some], out.at[:, some], sems.at[x // part]))
        copies[-1].start()


def early_kernel(coef_in, q_now, q_prev, jac, base, weights_out, table, planes, coef, buffer, weights, sems, *, size):
    nvars, size_x, _, size_z = size
    fetch = pltpu.make_async_copy(coef_in, coef, sems.at[PIECES])
    fetch.start()
    fill_planes(lambda v, x: q_now[v, x], None, planes, None, size)
    fetch.wait()
    for k in range(table.shape[0]):
        table[k : k + 1, :] = jnp.full((1, size_z), coef[k], jnp.float32)
    mixing_weights(coef, weights.at[0], weights.at[1], size)
    copies = [pltpu.make_async_copy(weights, weights_out, sems.at[PIECES + 1])]
    copies[0].start()
    for x in range(size_x):
        flux = flux_at(x, weights, planes, None, size)
        scale = step_tau * jac[x]
        for v in range(nvars):
            centre = q_now[v, x]
            physical = (q_prev[v, x] - centre) / (2.0 * step_phys)
            buffer[v, x] = centre - scale * (flux[v] + physical)
        sent_out(x, size_x, buffer, base, sems, copies)
    for copy in copies:
        copy.wait()


def mixed_by(table, direction, side, lines):
    nvars = len(lines)
    out = []
    for a in range(nvars):
        total = None
        for b in range(nvars):
            k = ((direction * 2 + side) * nvars + a) * nvars + b
            term = table[k : k + 1, :] * lines[b]
            total = term if total is None else total + term
        out.append(total)
    return out


def land(rows, hot_xy, hot_z, store, nvars):
    columns = hot_xy.shape[0]
    for first in range(0, nvars, 2):
        some = range(first, min(first + 2, nvars))
        pieces = []
        for c in some:
            for half in halves(rows[c : c + 1, :]):
                pieces.append(hot_xy[...] * half)
        landed = dot(jnp.concatenate(pieces, axis=0), hot_z[...], ((1,), (0,)))
        for c in some:
            at = 2 * (c - first) * columns
            store(c, landed[at : at + columns] + landed[at + columns : at + 2 * columns])


def first_kernel(table, got, base_in, q_now, jac, line_inner, line_outer, state, hits, x_inner, x_outer, y_inner, y_outer, later, hot_xy, hot_z, rows, grid, base, sems, *, size, devices, capacity):
    nvars, size_x, size_y, size_z = size
    columns = size_x * size_y
    slots = devices * capacity

    def fetch(x):
        return pltpu.make_async_copy(base_in.at[:, pl.ds(x, 1)], base.at[:, pl.ds(x, 1)], sems.at[x])

    @pl.loop(0, size_x)
    def _(x):
        fetch(x).start()

    for d in range(devices):
        piece = got[d]
        lanes = slice(d * capacity, (d + 1) * capacity)
        rows[0:8, lanes] = piece[:, 0:capacity]
        rows[8:16, lanes] = piece[:, capacity : 2 * capacity]
    turned = jnp.transpose(rows[8:16, :])
    land_z = turned[:, 2 * nvars + 1 - 8 : 2 * nvars + 2 - 8]
    hot_z[...] = (iota((slots, size_z), 1).astype(jnp.float32) == land_z).astype(jnp.float32).astype(jnp.bfloat16)
    land_xy = rows[2 * nvars : 2 * nvars + 1, :]
    hot_xy[...] = ((iota((columns, slots), 0) + 1).astype(jnp.float32) == land_xy).astype(jnp.float32).astype(jnp.bfloat16)
    later[...] = rows[nvars : 2 * nvars, :]

    hits[...] = dot(hot_xy[...], hot_z[...], ((1,), (0,)))
    even_x, even_y = lax.axis_index("gx") % 2 == 0, lax.axis_index("gy") % 2 == 0
    y_low, y_high = zip(*(sides_of("gy", line_inner[v], line_outer[v]) for v in range(nvars)))
    from_low, from_high = mixed_by(table, 1, 0, y_low), mixed_by(table, 1, 1, y_high)
    row_at = iota((size_y, size_z), 0)
    faces = {}

    def keep(c, value):
        grid[c] = value

    land(rows, hot_xy, hot_z, keep, nvars)
    for x in range(size_x):
        fetch(x).wait()
    for x in range(size_x):
        at = slice(x * size_y, (x + 1) * size_y)
        landed = hits[at, :]
        scale = step_tau * jac[x]
        for v in range(nvars):
            change = penalty * (landed * q_now[v, x] - grid[v, at, :])
            change = change - jnp.where(row_at == 0, from_low[v][x : x + 1], 0.0)
            change = change + jnp.where(row_at == size_y - 1, from_high[v][x : x + 1], 0.0)
            new = base[v, x] - scale * change
            state[v, x] = new
            low, high = new[0:1], new[size_y - 1 : size_y]
            y_inner[v * size_x + x : v * size_x + x + 1, :] = jnp.where(even_y, high, low)
            y_outer[v * size_x + x : v * size_x + x + 1, :] = jnp.where(even_y, low, high)
            if x in (0, size_x - 1):
                faces[x, v] = new
    tail = nvars * size_x
    y_inner[tail:, :] = y_outer[tail:, :] = jnp.zeros((8, size_z), jnp.float32)
    for k, x in enumerate((0, size_x - 1)):
        low, high = jac[x][0:1], jac[x][size_y - 1 : size_y]
        y_inner[tail + k : tail + k + 1, :] = jnp.where(even_y, high, low)
        y_outer[tail + k : tail + k + 1, :] = jnp.where(even_y, low, high)
    ends = [y_low[v] for v in range(nvars)] + [y_high[v] for v in range(nvars)]
    for v in range(nvars):
        for k, pair in enumerate(((faces[0, v], faces[size_x - 1, v]), (q_now[v, 0], q_now[v, size_x - 1]))):
            x_inner[k * nvars + v] = jnp.where(even_x, pair[1], pair[0])
            x_outer[k * nvars + v] = jnp.where(even_x, pair[0], pair[1])
    x_inner[2 * nvars] = jnp.where(even_x, jac[size_x - 1], jac[0])
    x_outer[2 * nvars] = jnp.where(even_x, jac[0], jac[size_x - 1])
    x_inner[2 * nvars + 1] = x_outer[2 * nvars + 1] = jnp.zeros((size_y, size_z), jnp.float32)
    for k, line in enumerate(ends):
        low, high = line[0:1], line[size_x - 1 : size_x]
        x_inner[2 * nvars + 1, k : k + 1, :] = jnp.where(even_x, high, low)
        x_outer[2 * nvars + 1, k : k + 1, :] = jnp.where(even_x, low, high)


def late_kernel(rows, hot_xy, hot_z, target):
    def keep(c, value):
        target[c] = value

    land(rows, hot_xy, hot_z, keep, rows.shape[0])


def second_kernel(table, state, weights, q_now, q_prev, jac, target, hits, x_inner, x_outer, y_inner, y_outer, out, planes, sides, edge, buffer, sems, *, size):
    nvars, size_x, size_y, size_z = size
    last = size_x - 1
    x_low, x_high = zip(*(sides_of("gx", x_inner[k], x_outer[k]) for k in range(2 * nvars + 2)))
    own_low = mixed_by(table, 0, 0, x_low[nvars : 2 * nvars])
    own_high = mixed_by(table, 0, 1, x_high[nvars : 2 * nvars])
    ring_low = mixed_by(table, 0, 1, [q_now[v, 0] for v in range(nvars)])
    ring_high = mixed_by(table, 0, 0, [q_now[v, last] for v in range(nvars)])
    around = [[], [], [], []]
    for v in range(nvars):
        edge[0, v] = state[v, 0] + step_tau * jac[0] * own_low[v]
        edge[1, v] = state[v, last] - step_tau * jac[last] * own_high[v]
        around[0].append(x_low[v] - step_tau * x_low[2 * nvars] * ring_low[v])
        around[1].append(x_high[v] + step_tau * x_high[2 * nvars] * ring_high[v])
    row_at = iota((size_x, size_z), 0)
    tail = nvars * size_x
    for side in range(2):
        scale = sides_of("gy", y_inner[tail:, :], y_outer[tail:, :])[side]
        corner = range(side * nvars, (side + 1) * nvars)
        low = mixed_by(table, 0, 0, [x_low[2 * nvars + 1][k : k + 1] for k in corner])
        high = mixed_by(table, 0, 1, [x_high[2 * nvars + 1][k : k + 1] for k in corner])
        for v in range(nvars):
            change = jnp.where(row_at == 0, scale[0:1] * low[v], 0.0) - jnp.where(row_at == last, scale[1:2] * high[v], 0.0)
            face = slice(v * size_x, (v + 1) * size_x)
            around[2 + side].append(sides_of("gy", y_inner[face, :], y_outer[face, :])[side] + step_tau * change)

    def at_plane(v, x):
        return edge[0, v] if x == 0 else edge[1, v] if x == last else state[v, x]

    fill_planes(at_plane, around, planes, sides, size)
    copies = []
    for x in range(size_x):
        at = slice(x * size_y, (x + 1) * size_y)
        flux = flux_at(x, weights, planes, sides, size)
        landed = hits[at, :]
        scale = step_tau * jac[x]
        for v in range(nvars):
            centre = at_plane(v, x)
            physical = (3.0 * centre - 4.0 * q_now[v, x] + q_prev[v, x]) / (2.0 * step_phys)
            coupling = penalty * (landed * centre - target[v, at, :])
            buffer[v, x] = centre - scale * (flux[v] + physical + coupling)
        sent_out(x, size_x, buffer, out, sems, copies)
    for copy in copies:
        copy.wait()


def swapped(inner, outer, axis):
    count_x, count_y = lax.axis_size("gx"), lax.axis_size("gy")
    inner_pairs, outer_pairs = [], []
    for i in range(count_x):
        for j in range(count_y):
            at, count = (i, count_x) if axis == "gx" else (j, count_y)
            for pairs, to in ((inner_pairs, at ^ 1), (outer_pairs, ((at + 1) ^ 1) - 1)):
                x, y = (to, j) if axis == "gx" else (i, to)
                if axis == "gx" and not 0 <= to < count:
                    x, y = i, j ^ 2
                if axis == "gy" and not 0 <= to < count:
                    x, y = i ^ 1, j
                pairs.append((i * count_y + j, x * count_y + y))
    return lax.ppermute(inner, AXES, inner_pairs), lax.ppermute(outer, AXES, outer_pairs)


def sides_of(axis, inner, outer):
    here, last = lax.axis_index(axis), lax.axis_size(axis) - 1
    even = here % 2 == 0
    inside = (here > 0) & (here < last)
    masked = jnp.where(inside, outer, 0.0)
    return jnp.where(even, masked, inner), jnp.where(even, inner, masked)


def params(limit):
    return pltpu.CompilerParams(vmem_limit_bytes=limit)


def body(q_now, q_prev, jacobian, flux_split, donor_base, donor_frac, fringe_dest, receptor_cell, fringe_count):
    size = q_now.shape
    nvars, size_x, size_y, size_z = size
    columns = size_x * size_y
    block = nvars * size_y
    devices = lax.axis_size("gx") * lax.axis_size("gy")
    rows = donor_base.shape[0]
    capacity = 2 * rows // devices
    slots = devices * capacity
    f32, bf16 = jnp.float32, jnp.bfloat16
    hbm = pl.BlockSpec(memory_space=pltpu.HBM)
    vmem = pl.BlockSpec(memory_space=pltpu.VMEM)
    flat = (nvars, columns, size_z)
    shape = jax.ShapeDtypeStruct
    weights_shape = (2, 3 * block, 3 * block + CHANNELS)
    planes = pltpu.VMEM((2, (size_x + 2) * block, size_z), bf16)
    sides = pltpu.VMEM((size_x, CHANNELS, size_z), f32)
    face_y = shape((nvars * size_x + 8, size_z), f32)

    line, line_x = pltpu.VMEM((nvars, size_x, size_z), f32), shape((2 * nvars + 2, size_y, size_z), f32)
    coef = flux_split.reshape(-1)

    def there(x):
        return pltpu.with_memory_space_constraint(x, pltpu.HBM)

    sent, *lines = pl.pallas_call(
        functools.partial(donor_kernel, size=size, devices=devices, capacity=capacity),
        out_shape=[pltpu.HBM((devices, 8, 2 * capacity), f32), line, line],
        in_specs=[pl.BlockSpec(memory_space=pltpu.SMEM)] + [hbm] * 6,
        out_specs=[hbm, vmem, vmem],
        scratch_shapes=[
            pltpu.VMEM((devices, 8, 2 * capacity), f32),
            pltpu.VMEM((2, nvars, columns, size_z), f32),
            pltpu.VMEM((2 * nvars * columns, size_z), bf16),
            pltpu.VMEM((2 * nvars * columns, 2 * size_z), jnp.float8_e4m3fn),
            pltpu.VMEM((size_z, rows), bf16),
            pltpu.VMEM((2 * size_z, rows), jnp.float8_e4m3fn),
            pltpu.VMEM((columns, rows), f32),
            pltpu.VMEM((rows, 8), f32),
            pltpu.VMEM((CHANNELS, rows), f32),
            pltpu.VMEM((1, rows), jnp.int32),
            pltpu.VMEM((3, rows), f32),
            pltpu.VMEM((1, rows), jnp.int32),
            pltpu.VMEM((1, rows), jnp.int32),
            pltpu.SemaphoreType.DMA((5 + 2 * nvars,)),
        ],
        compiler_params=params(DONOR_LIMIT),
        name="donor",
    )(
        fringe_count,
        there(q_prev.reshape(flat)),
        there(q_now.reshape(flat)),
        there(donor_base.reshape(1, rows)),
        there(donor_frac),
        there(fringe_dest.reshape(1, rows)),
        there(receptor_cell.reshape(1, rows)),
    )
    got = lax.all_to_all(sent, AXES, split_axis=0, concat_axis=0, tiled=True)
    lines = swapped(*lines, "gy")
    base, weights, table = pl.pallas_call(
        functools.partial(early_kernel, size=size),
        out_shape=[pltpu.HBM(size, f32), pltpu.HBM(weights_shape, bf16), shape((4 * nvars * nvars, size_z), f32)],
        in_specs=[hbm] + [vmem] * 3,
        out_specs=[hbm, hbm, vmem],
        scratch_shapes=[planes, pltpu.SMEM((6 * nvars * nvars,), f32), pltpu.VMEM(size, f32), pltpu.VMEM(weights_shape, bf16), pltpu.SemaphoreType.DMA((PIECES + 2,))],
        compiler_params=params(20 * MIB),
        name="early",
    )(coef, q_now, q_prev, jacobian)
    state, hits, *faces, later, hot_xy, hot_z = pl.pallas_call(
        functools.partial(first_kernel, size=size, devices=devices, capacity=capacity),
        out_shape=[
            shape(size, f32),
            shape((columns, size_z), f32),
            line_x,
            line_x,
            face_y,
            face_y,
            shape((nvars, slots), f32),
            shape((columns, slots), bf16),
            shape((slots, size_z), bf16),
        ],
        in_specs=[vmem, vmem, hbm] + [vmem] * 4,
        out_specs=[vmem] * 9,
        scratch_shapes=[
            pltpu.VMEM((CHANNELS, slots), f32),
            pltpu.VMEM((nvars, columns, size_z), f32),
            pltpu.VMEM(size, f32),
            pltpu.SemaphoreType.DMA((size_x,)),
        ],
        compiler_params=params(20 * MIB),
        name="first",
    )(table, got, there(base), q_now, jacobian, *lines)
    around = (*swapped(*faces[0:2], "gx"), *swapped(*faces[2:4], "gy"))
    target = pl.pallas_call(
        late_kernel,
        out_shape=shape(flat, f32),
        in_specs=[vmem] * 3,
        out_specs=vmem,
        compiler_params=params(20 * MIB),
        name="late",
    )(later, hot_xy, hot_z)
    return pl.pallas_call(
        functools.partial(second_kernel, size=size),
        out_shape=shape(size, f32),
        in_specs=[vmem] * 12,
        out_specs=hbm,
        scratch_shapes=[planes, sides, pltpu.VMEM((2, nvars, size_y, size_z), f32), pltpu.VMEM(size, f32), pltpu.SemaphoreType.DMA((PIECES,))],
        compiler_params=params(20 * MIB),
        name="second",
    )(table, state, weights, q_now, q_prev, jacobian, target, hits, *around)


def solution(mesh):
    return jax.shard_map(
        body,
        mesh=mesh,
        in_specs=(
            P(None, "gx", "gy", None),
            P(None, "gx", "gy", None),
            P("gx", "gy", None),
            P(),
            P(("gx", "gy")),
            P(None, ("gx", "gy")),
            P(("gx", "gy"), None),
            P(("gx", "gy")),
            P(("gx", "gy")),
        ),
        out_specs=P(None, "gx", "gy", None),
        check_vma=False,
    )
```

```python
import functools

import jax
import jax.numpy as jnp
from jax import lax
from jax.experimental import pallas as pl
from jax.experimental.pallas import tpu as pltpu
from jax.sharding import PartitionSpec as P


step_tau = 0.2
step_phys = 0.5
penalty = 2.0

AXES = ("gx", "gy")
LANES = 256
CHANNELS = 16
MIB = 1 << 20
DONOR_LIMIT = 44 * MIB
PIECES = 8


def iota(shape, dim):
    return lax.broadcasted_iota(jnp.int32, shape, dim)


def dot(a, b, dims):
    return lax.dot_general(a, b, (dims, ((), ())), preferred_element_type=jnp.float32)


def halves(x):
    high = x.astype(jnp.bfloat16)
    return high, (x - high.astype(jnp.float32)).astype(jnp.bfloat16)


def eighth(x, power):
    return (x * 2.0**power).astype(jnp.float8_e4m3fn)


def ranks(dest, devices):
    rows = dest.shape[1]
    blocks = rows // LANES
    hot = (iota((devices, rows), 0) == dest).astype(jnp.float32)
    stacked = jnp.concatenate([hot[:, b * LANES : (b + 1) * LANES] for b in range(blocks)], axis=0)
    before = (iota((LANES, LANES), 0) < iota((LANES, LANES), 1)).astype(jnp.float32)
    local = dot(stacked.astype(jnp.bfloat16), before.astype(jnp.bfloat16), ((1,), (0,)))
    carried = jnp.zeros((devices, 1), jnp.float32)
    pieces = []
    for b in range(blocks):
        part = local[b * devices : (b + 1) * devices]
        own = hot[:, b * LANES : (b + 1) * LANES]
        pieces.append(jnp.sum((part + carried) * own, axis=0, keepdims=True))
        carried = carried + jnp.sum(own, axis=1, keepdims=True)
    return jnp.concatenate(pieces, axis=1)


def donor_kernel(count, q_prev, q_now, base_in, frac_in, dest_in, cell_in, out_there, y_inner, y_outer, out, planes, lhs, lhs_low, spread, spread_low, corner, place, values, base, frac, dest, cell, sems, *, size, devices, capacity):
    nvars, size_x, size_y, size_z = size
    columns = size_x * size_y
    rows = base.shape[1]
    small = [pltpu.make_async_copy(a, b, sems.at[k]) for k, (a, b) in enumerate(((base_in, base), (frac_in, frac), (dest_in, dest), (cell_in, cell)))]
    copies = [pltpu.make_async_copy(ref.at[v], planes.at[k, v], sems.at[5 + k * nvars + v]) for k, ref in enumerate((q_prev, q_now)) for v in range(nvars)]
    for copy in small + copies:
        copy.start()
    for copy in small:
        copy.wait()
    start = base[...].astype(jnp.float32)
    in_y = jnp.floor((start + 0.5) * (1.0 / (size_z - 1)))
    base_z = start - in_y * (size_z - 1)
    base_x = jnp.floor((in_y + 0.5) * (1.0 / (size_y - 1)))
    base_y = in_y - base_x * (size_y - 1)
    frac_x, frac_y, frac_z = frac[0:1, :], frac[1:2, :], frac[2:3, :]

    def weights(first, part, shape):
        at = iota(shape, 0).astype(jnp.float32) - first
        return jnp.where(at == 0.0, 1.0 - part, jnp.where(at == 1.0, part, 0.0))

    along_z = weights(base_z, frac_z, (size_z, rows))
    spread[...] = along_z.astype(jnp.bfloat16)
    rest = along_z - spread[...].astype(jnp.float32)
    spread_low[0:size_z, :] = eighth(rest, 16)
    spread_low[size_z : 2 * size_z, :] = eighth(along_z, 8)
    along_x = weights(base_x, frac_x, (size_x, rows))
    along_y = weights(base_y, frac_y, (size_y, rows))
    for x in range(size_x):
        corner[x * size_y : (x + 1) * size_y, :] = along_x[x : x + 1, :] * along_y
    alive = iota((1, rows), 1) < count[0]
    slot = ranks(dest[...], devices)
    where_to = jnp.where(alive, dest[...].astype(jnp.float32) * capacity + slot, -1.0)
    place[...] = jnp.transpose(jnp.broadcast_to(where_to, (8, rows)))
    landing = cell[...].astype(jnp.float32)
    land_xy = jnp.floor((landing + 0.5) * (1.0 / size_z))
    values[...] = jnp.zeros(values.shape, jnp.float32)
    values[2 * nvars : 2 * nvars + 1, :] = land_xy + 1.0
    values[2 * nvars + 1 : 2 * nvars + 2, :] = landing - land_xy * size_z
    for k in range(2):
        if k == 1:
            for v in range(nvars):
                copies[nvars + v].wait()
            even = lax.axis_index("gy") % 2 == 0
            for v in range(nvars):
                for x in range(size_x):
                    line = planes.at[1, v]
                    low = line[x * size_y : x * size_y + 1, :]
                    high = line[(x + 1) * size_y - 1 : (x + 1) * size_y, :]
                    y_inner[v, x : x + 1, :] = jnp.where(even, high, low)
                    y_outer[v, x : x + 1, :] = jnp.where(even, low, high)
        for v in range(nvars):
            if k == 0:
                copies[v].wait()
            at = pl.ds((k * nvars + v) * columns, columns)
            plane = planes[k, v]
            lhs[at, :] = plane.astype(jnp.bfloat16)
            lhs_low[at, 0:size_z] = eighth(plane, 6)
            lhs_low[at, size_z : 2 * size_z] = eighth(plane - plane.astype(jnp.bfloat16).astype(jnp.float32), 14)
    for n in range(rows // LANES):
        lanes = slice(n * LANES, (n + 1) * LANES)
        for k in range(2):
            at = slice(k * nvars * columns, (k + 1) * nvars * columns)
            part = dot(lhs[at, :], spread[:, lanes], ((1,), (0,)))
            part = part + 2.0**-22 * dot(lhs_low[at, :], spread_low[:, lanes], ((1,), (0,)))
            for v in range(nvars):
                picked = part[v * columns : (v + 1) * columns] * corner[:, lanes]
                values[k * nvars + v : k * nvars + v + 1, lanes] = jnp.sum(picked, axis=0, keepdims=True)
    first = values[...]
    high, rest = first.astype(jnp.bfloat16), None
    rest = first - high.astype(jnp.float32)
    middle = rest.astype(jnp.bfloat16)
    last = (rest - middle.astype(jnp.float32)).astype(jnp.bfloat16)
    three = jnp.concatenate([high, middle, last], axis=0)
    leaving = []
    column = jnp.broadcast_to(place[:, 0:1], (rows, LANES))
    for n in range(devices * capacity // LANES):
        chosen = (column == (iota((rows, LANES), 1) + n * LANES).astype(jnp.float32)).astype(jnp.float32).astype(jnp.bfloat16)
        moved = dot(three, chosen, ((1,), (0,)))
        moved = moved[0:CHANNELS] + moved[CHANNELS : 2 * CHANNELS] + moved[2 * CHANNELS : 3 * CHANNELS]
        for d in range(LANES // capacity):
            piece = moved[:, d * capacity : (d + 1) * capacity]
            to = n * (LANES // capacity) + d
            out[to] = jnp.concatenate([piece[0:8], piece[8:16]], axis=1)
        some = pl.ds(n * (LANES // capacity), LANES // capacity)
        leaving.append(pltpu.make_async_copy(out.at[some], out_there.at[some], sems.at[n]))
        leaving[-1].start()
    for copy in leaving:
        copy.wait()


def mixing_weights(coef, high, low, size):
    nvars, _, size_y, _ = size
    block = nvars * size_y
    width = 3 * block + CHANNELS
    row = iota((size_y, width), 0)
    offset = iota((size_y, width), 1) - row
    lane = iota((size_y, width), 1)

    def at(d, side, a, b):
        return coef[((d * 2 + side) * nvars + a) * nvars + b]

    for a in range(nvars):
        main = jnp.zeros((size_y, width), jnp.float32)
        back = main
        fore = main
        for b in range(nvars):
            first = b * size_y
            same = at(0, 0, a, b) - at(0, 1, a, b) + at(1, 0, a, b) - at(1, 1, a, b) + at(2, 0, a, b) - at(2, 1, a, b)
            main = jnp.where(offset == first, -at(0, 0, a, b), main)
            main = jnp.where(offset == block + first, same, main)
            main = jnp.where((offset == block + first - 1) & (row > 0), -at(1, 0, a, b), main)
            main = jnp.where((offset == block + first + 1) & (row < size_y - 1), at(1, 1, a, b), main)
            main = jnp.where(offset == 2 * block + first, at(0, 1, a, b), main)
            main = jnp.where((lane == 3 * block + b) & (row == 0), -at(1, 0, a, b), main)
            main = jnp.where((lane == 3 * block + nvars + b) & (row == size_y - 1), at(1, 1, a, b), main)
            back = jnp.where(offset == block + first, -at(2, 0, a, b), back)
            fore = jnp.where(offset == block + first, at(2, 1, a, b), fore)
        for k, part in enumerate((main, back, fore)):
            rows = slice(k * block + a * size_y, k * block + (a + 1) * size_y)
            high[rows, :], low[rows, :] = halves(part)


def fill_planes(at_plane, around, planes, sides, size):
    nvars, size_x, size_y, size_z = size
    block = nvars * size_y
    for x in range(size_x + 2):
        for v in range(nvars):
            rows = slice(x * block + v * size_y, x * block + (v + 1) * size_y)
            if 0 < x <= size_x:
                planes[0, rows, :], planes[1, rows, :] = halves(at_plane(v, x - 1))
            elif around is None:
                planes[0, rows, :] = planes[1, rows, :] = jnp.zeros((size_y, size_z), jnp.bfloat16)
            else:
                planes[0, rows, :], planes[1, rows, :] = halves(around[0 if x == 0 else 1][v])
    if around is not None:
        sides[...] = jnp.zeros(sides.shape, jnp.float32)
        for v in range(nvars):
            sides[:, v, :] = around[2][v]
            sides[:, nvars + v, :] = around[3][v]


def flux_at(x, weights, planes, sides, size):
    nvars, _, size_y, size_z = size
    block = nvars * size_y
    if sides is None:
        high = low = jnp.zeros((CHANNELS, size_z), jnp.bfloat16)
    else:
        high, low = halves(sides[x])
    rows = slice(x * block, (x + 3) * block)
    around_high = jnp.concatenate([planes[0, rows, :], high], axis=0)
    around_low = jnp.concatenate([planes[1, rows, :], low], axis=0)
    both = jnp.concatenate([weights[0], weights[1]], axis=0)
    mixed = dot(both, around_high, ((1,), (0,)))
    mixed = mixed[0 : 3 * block] + mixed[3 * block :] + dot(weights[0], around_low, ((1,), (0,)))
    z_at = iota((block, size_z), 1)
    back = jnp.where(z_at == 0, 0.0, pltpu.roll(mixed[block : 2 * block], 1, 1))
    fore = jnp.where(z_at == size_z - 1, 0.0, pltpu.roll(mixed[2 * block :], size_z - 1, 1))
    flux = mixed[0:block] + back + fore
    return [flux[v * size_y : (v + 1) * size_y] for v in range(nvars)]


def sent_out(x, size_x, buffer, out, sems, copies):
    part = size_x // PIECES
    if (x + 1) % part == 0:
        some = pl.ds(x + 1 - part, part)
        copies.append(pltpu.make_async_copy(buffer.at[:, some], out.at[:, some], sems.at[x // part]))
        copies[-1].start()


def early_kernel(coef_in, q_now, q_prev, jac, base, weights_out, table, planes, coef, buffer, weights, sems, *, size):
    nvars, size_x, _, size_z = size
    fetch = pltpu.make_async_copy(coef_in, coef, sems.at[PIECES])
    fetch.start()
    fill_planes(lambda v, x: q_now[v, x], None, planes, None, size)
    fetch.wait()
    for k in range(table.shape[0]):
        table[k : k + 1, :] = jnp.full((1, size_z), coef[k], jnp.float32)
    mixing_weights(coef, weights.at[0], weights.at[1], size)
    copies = [pltpu.make_async_copy(weights, weights_out, sems.at[PIECES + 1])]
    copies[0].start()
    for x in range(size_x):
        flux = flux_at(x, weights, planes, None, size)
        scale = step_tau * jac[x]
        for v in range(nvars):
            centre = q_now[v, x]
            physical = (q_prev[v, x] - centre) / (2.0 * step_phys)
            buffer[v, x] = centre - scale * (flux[v] + physical)
        sent_out(x, size_x, buffer, base, sems, copies)
    for copy in copies:
        copy.wait()


def mixed_by(table, direction, side, lines):
    nvars = len(lines)
    out = []
    for a in range(nvars):
        total = None
        for b in range(nvars):
            k = ((direction * 2 + side) * nvars + a) * nvars + b
            term = table[k : k + 1, :] * lines[b]
            total = term if total is None else total + term
        out.append(total)
    return out


def land(rows, hot_xy, hot_z, store, nvars):
    columns = hot_xy.shape[0]
    for first in range(0, nvars, 2):
        some = range(first, min(first + 2, nvars))
        pieces = []
        for c in some:
            for half in halves(rows[c : c + 1, :]):
                pieces.append(hot_xy[...] * half)
        landed = dot(jnp.concatenate(pieces, axis=0), hot_z[...], ((1,), (0,)))
        for c in some:
            at = 2 * (c - first) * columns
            store(c, landed[at : at + columns] + landed[at + columns : at + 2 * columns])


def land_split(rows, hot_xy, hot_z, hot_z_low, store, nvars):
    columns = hot_xy.shape[0]
    for first in range(0, nvars, 2):
        some = range(first, min(first + 2, nvars))
        high, low = [], []
        for c in some:
            whole = rows[c : c + 1, :]
            part = whole.astype(jnp.bfloat16)
            high.append(hot_xy[...] * part)
            scaled = ((whole - part.astype(jnp.float32)) * 2.0**14).astype(jnp.bfloat16)
            low.append((hot_xy[...] * scaled).astype(jnp.float8_e4m3fn))
        landed = dot(jnp.concatenate(high, axis=0), hot_z[...], ((1,), (0,)))
        landed = landed + 2.0**-14 * dot(jnp.concatenate(low, axis=0), hot_z_low[...], ((1,), (0,)))
        for c in some:
            store(c, landed[(c - first) * columns : (c - first + 1) * columns])


def first_kernel(table, got, base_in, q_now, jac, line_inner, line_outer, state, hits, x_inner, x_outer, y_inner, y_outer, later, hot_xy, hot_z, hot_z_low, rows, grid, base, sems, *, size, devices, capacity):
    nvars, size_x, size_y, size_z = size
    columns = size_x * size_y
    slots = devices * capacity

    def fetch(x):
        return pltpu.make_async_copy(base_in.at[:, pl.ds(x, 1)], base.at[:, pl.ds(x, 1)], sems.at[x])

    @pl.loop(0, size_x)
    def _(x):
        fetch(x).start()

    for d in range(devices):
        piece = got[d]
        lanes = slice(d * capacity, (d + 1) * capacity)
        rows[0:8, lanes] = piece[:, 0:capacity]
        rows[8:16, lanes] = piece[:, capacity : 2 * capacity]
    turned = jnp.transpose(rows[8:16, :])
    land_z = turned[:, 2 * nvars + 1 - 8 : 2 * nvars + 2 - 8]
    hot_z[...] = (iota((slots, size_z), 1).astype(jnp.float32) == land_z).astype(jnp.float32).astype(jnp.bfloat16)
    hot_z_low[...] = (iota((slots, size_z), 1).astype(jnp.float32) == land_z).astype(jnp.float32).astype(jnp.float8_e4m3fn)
    land_xy = rows[2 * nvars : 2 * nvars + 1, :]
    hot_xy[...] = ((iota((columns, slots), 0) + 1).astype(jnp.float32) == land_xy).astype(jnp.float32).astype(jnp.bfloat16)
    later[...] = rows[nvars : 2 * nvars, :]

    hits[...] = dot(hot_xy[...], hot_z[...], ((1,), (0,)))
    even_x, even_y = lax.axis_index("gx") % 2 == 0, lax.axis_index("gy") % 2 == 0
    y_low, y_high = zip(*(sides_of("gy", line_inner[v], line_outer[v]) for v in range(nvars)))
    from_low, from_high = mixed_by(table, 1, 0, y_low), mixed_by(table, 1, 1, y_high)
    row_at = iota((size_y, size_z), 0)
    faces = {}

    def keep(c, value):
        grid[c] = value

    land_split(rows, hot_xy, hot_z, hot_z_low, keep, nvars)
    for x in range(size_x):
        fetch(x).wait()
    for x in range(size_x):
        at = slice(x * size_y, (x + 1) * size_y)
        landed = hits[at, :]
        scale = step_tau * jac[x]
        for v in range(nvars):
            change = penalty * (landed * q_now[v, x] - grid[v, at, :])
            change = change - jnp.where(row_at == 0, from_low[v][x : x + 1], 0.0)
            change = change + jnp.where(row_at == size_y - 1, from_high[v][x : x + 1], 0.0)
            new = base[v, x] - scale * change
            state[v, x] = new
            low, high = new[0:1], new[size_y - 1 : size_y]
            y_inner[v * size_x + x : v * size_x + x + 1, :] = jnp.where(even_y, high, low)
            y_outer[v * size_x + x : v * size_x + x + 1, :] = jnp.where(even_y, low, high)
            if x in (0, size_x - 1):
                faces[x, v] = new
    tail = nvars * size_x
    y_inner[tail:, :] = y_outer[tail:, :] = jnp.zeros((8, size_z), jnp.float32)
    for k, x in enumerate((0, size_x - 1)):
        low, high = jac[x][0:1], jac[x][size_y - 1 : size_y]
        y_inner[tail + k : tail + k + 1, :] = jnp.where(even_y, high, low)
        y_outer[tail + k : tail + k + 1, :] = jnp.where(even_y, low, high)
    ends = [y_low[v] for v in range(nvars)] + [y_high[v] for v in range(nvars)]
    for v in range(nvars):
        for k, pair in enumerate(((faces[0, v], faces[size_x - 1, v]), (q_now[v, 0], q_now[v, size_x - 1]))):
            x_inner[k * nvars + v] = jnp.where(even_x, pair[1], pair[0])
            x_outer[k * nvars + v] = jnp.where(even_x, pair[0], pair[1])
    x_inner[2 * nvars] = jnp.where(even_x, jac[size_x - 1], jac[0])
    x_outer[2 * nvars] = jnp.where(even_x, jac[0], jac[size_x - 1])
    x_inner[2 * nvars + 1] = x_outer[2 * nvars + 1] = jnp.zeros((size_y, size_z), jnp.float32)
    for k, line in enumerate(ends):
        low, high = line[0:1], line[size_x - 1 : size_x]
        x_inner[2 * nvars + 1, k : k + 1, :] = jnp.where(even_x, high, low)
        x_outer[2 * nvars + 1, k : k + 1, :] = jnp.where(even_x, low, high)


def late_kernel(rows, hot_xy, hot_z, target):
    def keep(c, value):
        target[c] = value

    land(rows, hot_xy, hot_z, keep, rows.shape[0])


def second_kernel(table, state, weights, q_now, q_prev, jac, target, hits, x_inner, x_outer, y_inner, y_outer, out, planes, sides, edge, buffer, sems, *, size):
    nvars, size_x, size_y, size_z = size
    last = size_x - 1
    x_low, x_high = zip(*(sides_of("gx", x_inner[k], x_outer[k]) for k in range(2 * nvars + 2)))
    own_low = mixed_by(table, 0, 0, x_low[nvars : 2 * nvars])
    own_high = mixed_by(table, 0, 1, x_high[nvars : 2 * nvars])
    ring_low = mixed_by(table, 0, 1, [q_now[v, 0] for v in range(nvars)])
    ring_high = mixed_by(table, 0, 0, [q_now[v, last] for v in range(nvars)])
    around = [[], [], [], []]
    for v in range(nvars):
        edge[0, v] = state[v, 0] + step_tau * jac[0] * own_low[v]
        edge[1, v] = state[v, last] - step_tau * jac[last] * own_high[v]
        around[0].append(x_low[v] - step_tau * x_low[2 * nvars] * ring_low[v])
        around[1].append(x_high[v] + step_tau * x_high[2 * nvars] * ring_high[v])
    row_at = iota((size_x, size_z), 0)
    tail = nvars * size_x
    for side in range(2):
        scale = sides_of("gy", y_inner[tail:, :], y_outer[tail:, :])[side]
        corner = range(side * nvars, (side + 1) * nvars)
        low = mixed_by(table, 0, 0, [x_low[2 * nvars + 1][k : k + 1] for k in corner])
        high = mixed_by(table, 0, 1, [x_high[2 * nvars + 1][k : k + 1] for k in corner])
        for v in range(nvars):
            change = jnp.where(row_at == 0, scale[0:1] * low[v], 0.0) - jnp.where(row_at == last, scale[1:2] * high[v], 0.0)
            face = slice(v * size_x, (v + 1) * size_x)
            around[2 + side].append(sides_of("gy", y_inner[face, :], y_outer[face, :])[side] + step_tau * change)

    def at_plane(v, x):
        return edge[0, v] if x == 0 else edge[1, v] if x == last else state[v, x]

    fill_planes(at_plane, around, planes, sides, size)
    copies = []
    for x in range(size_x):
        at = slice(x * size_y, (x + 1) * size_y)
        flux = flux_at(x, weights, planes, sides, size)
        landed = hits[at, :]
        scale = step_tau * jac[x]
        for v in range(nvars):
            centre = at_plane(v, x)
            physical = (3.0 * centre - 4.0 * q_now[v, x] + q_prev[v, x]) / (2.0 * step_phys)
            coupling = penalty * (landed * centre - target[v, at, :])
            buffer[v, x] = centre - scale * (flux[v] + physical + coupling)
        sent_out(x, size_x, buffer, out, sems, copies)
    for copy in copies:
        copy.wait()


def swapped(inner, outer, axis):
    count_x, count_y = lax.axis_size("gx"), lax.axis_size("gy")
    inner_pairs, outer_pairs = [], []
    for i in range(count_x):
        for j in range(count_y):
            at, count = (i, count_x) if axis == "gx" else (j, count_y)
            for pairs, to in ((inner_pairs, at ^ 1), (outer_pairs, ((at + 1) ^ 1) - 1)):
                x, y = (to, j) if axis == "gx" else (i, to)
                if axis == "gx" and not 0 <= to < count:
                    x, y = i, j ^ 2
                if axis == "gy" and not 0 <= to < count:
                    x, y = i ^ 1, j
                pairs.append((i * count_y + j, x * count_y + y))
    return lax.ppermute(inner, AXES, inner_pairs), lax.ppermute(outer, AXES, outer_pairs)


def sides_of(axis, inner, outer):
    here, last = lax.axis_index(axis), lax.axis_size(axis) - 1
    even = here % 2 == 0
    inside = (here > 0) & (here < last)
    masked = jnp.where(inside, outer, 0.0)
    return jnp.where(even, masked, inner), jnp.where(even, inner, masked)


def params(limit):
    return pltpu.CompilerParams(vmem_limit_bytes=limit)


def body(q_now, q_prev, jacobian, flux_split, donor_base, donor_frac, fringe_dest, receptor_cell, fringe_count):
    size = q_now.shape
    nvars, size_x, size_y, size_z = size
    columns = size_x * size_y
    block = nvars * size_y
    devices = lax.axis_size("gx") * lax.axis_size("gy")
    rows = donor_base.shape[0]
    capacity = 2 * rows // devices
    slots = devices * capacity
    f32, bf16 = jnp.float32, jnp.bfloat16
    hbm = pl.BlockSpec(memory_space=pltpu.HBM)
    vmem = pl.BlockSpec(memory_space=pltpu.VMEM)
    flat = (nvars, columns, size_z)
    shape = jax.ShapeDtypeStruct
    weights_shape = (2, 3 * block, 3 * block + CHANNELS)
    planes = pltpu.VMEM((2, (size_x + 2) * block, size_z), bf16)
    sides = pltpu.VMEM((size_x, CHANNELS, size_z), f32)
    face_y = shape((nvars * size_x + 8, size_z), f32)

    line, line_x = pltpu.VMEM((nvars, size_x, size_z), f32), shape((2 * nvars + 2, size_y, size_z), f32)
    coef = flux_split.reshape(-1)

    def there(x):
        return pltpu.with_memory_space_constraint(x, pltpu.HBM)

    sent, *lines = pl.pallas_call(
        functools.partial(donor_kernel, size=size, devices=devices, capacity=capacity),
        out_shape=[pltpu.HBM((devices, 8, 2 * capacity), f32), line, line],
        in_specs=[pl.BlockSpec(memory_space=pltpu.SMEM)] + [hbm] * 6,
        out_specs=[hbm, vmem, vmem],
        scratch_shapes=[
            pltpu.VMEM((devices, 8, 2 * capacity), f32),
            pltpu.VMEM((2, nvars, columns, size_z), f32),
            pltpu.VMEM((2 * nvars * columns, size_z), bf16),
            pltpu.VMEM((2 * nvars * columns, 2 * size_z), jnp.float8_e4m3fn),
            pltpu.VMEM((size_z, rows), bf16),
            pltpu.VMEM((2 * size_z, rows), jnp.float8_e4m3fn),
            pltpu.VMEM((columns, rows), f32),
            pltpu.VMEM((rows, 8), f32),
            pltpu.VMEM((CHANNELS, rows), f32),
            pltpu.VMEM((1, rows), jnp.int32),
            pltpu.VMEM((3, rows), f32),
            pltpu.VMEM((1, rows), jnp.int32),
            pltpu.VMEM((1, rows), jnp.int32),
            pltpu.SemaphoreType.DMA((5 + 2 * nvars,)),
        ],
        compiler_params=params(DONOR_LIMIT),
        name="donor",
    )(
        fringe_count,
        there(q_prev.reshape(flat)),
        there(q_now.reshape(flat)),
        there(donor_base.reshape(1, rows)),
        there(donor_frac),
        there(fringe_dest.reshape(1, rows)),
        there(receptor_cell.reshape(1, rows)),
    )
    got = lax.all_to_all(sent, AXES, split_axis=0, concat_axis=0, tiled=True)
    lines = swapped(*lines, "gy")
    base, weights, table = pl.pallas_call(
        functools.partial(early_kernel, size=size),
        out_shape=[pltpu.HBM(size, f32), pltpu.HBM(weights_shape, bf16), shape((4 * nvars * nvars, size_z), f32)],
        in_specs=[hbm] + [vmem] * 3,
        out_specs=[hbm, hbm, vmem],
        scratch_shapes=[planes, pltpu.SMEM((6 * nvars * nvars,), f32), pltpu.VMEM(size, f32), pltpu.VMEM(weights_shape, bf16), pltpu.SemaphoreType.DMA((PIECES + 2,))],
        compiler_params=params(20 * MIB),
        name="early",
    )(coef, q_now, q_prev, jacobian)
    state, hits, *faces, later, hot_xy, hot_z = pl.pallas_call(
        functools.partial(first_kernel, size=size, devices=devices, capacity=capacity),
        out_shape=[
            shape(size, f32),
            shape((columns, size_z), f32),
            line_x,
            line_x,
            face_y,
            face_y,
            shape((nvars, slots), f32),
            shape((columns, slots), bf16),
            shape((slots, size_z), bf16),
        ],
        in_specs=[vmem, vmem, hbm] + [vmem] * 4,
        out_specs=[vmem] * 9,
        scratch_shapes=[
            pltpu.VMEM((slots, size_z), jnp.float8_e4m3fn),
            pltpu.VMEM((CHANNELS, slots), f32),
            pltpu.VMEM((nvars, columns, size_z), f32),
            pltpu.VMEM(size, f32),
            pltpu.SemaphoreType.DMA((size_x,)),
        ],
        compiler_params=params(20 * MIB),
        name="first",
    )(table, got, there(base), q_now, jacobian, *lines)
    around = (*swapped(*faces[0:2], "gx"), *swapped(*faces[2:4], "gy"))
    target = pl.pallas_call(
        late_kernel,
        out_shape=shape(flat, f32),
        in_specs=[vmem] * 3,
        out_specs=vmem,
        compiler_params=params(20 * MIB),
        name="late",
    )(later, hot_xy, hot_z)
    return pl.pallas_call(
        functools.partial(second_kernel, size=size),
        out_shape=shape(size, f32),
        in_specs=[vmem] * 12,
        out_specs=hbm,
        scratch_shapes=[planes, sides, pltpu.VMEM((2, nvars, size_y, size_z), f32), pltpu.VMEM(size, f32), pltpu.SemaphoreType.DMA((PIECES,))],
        compiler_params=params(20 * MIB),
        name="second",
    )(table, state, weights, q_now, q_prev, jacobian, target, hits, *around)


def solution(mesh):
    return jax.shard_map(
        body,
        mesh=mesh,
        in_specs=(
            P(None, "gx", "gy", None),
            P(None, "gx", "gy", None),
            P("gx", "gy", None),
            P(),
            P(("gx", "gy")),
            P(None, ("gx", "gy")),
            P(("gx", "gy"), None),
            P(("gx", "gy")),
            P(("gx", "gy")),
        ),
        out_specs=P(None, "gx", "gy", None),
        check_vma=False,
    )
```

```python
import functools

import jax
import jax.numpy as jnp
from jax import lax
from jax.experimental import pallas as pl
from jax.experimental.pallas import tpu as pltpu
from jax.sharding import PartitionSpec as P


step_tau = 0.2
step_phys = 0.5
penalty = 2.0

AXES = ("gx", "gy")
LANES = 256
CHANNELS = 16
MIB = 1 << 20
DONOR_LIMIT = 44 * MIB
PIECES = 8


def iota(shape, dim):
    return lax.broadcasted_iota(jnp.int32, shape, dim)


def dot(a, b, dims):
    return lax.dot_general(a, b, (dims, ((), ())), preferred_element_type=jnp.float32)


def halves(x):
    high = x.astype(jnp.bfloat16)
    return high, (x - high.astype(jnp.float32)).astype(jnp.bfloat16)


def eighth(x, power):
    return (x * 2.0**power).astype(jnp.float8_e4m3fn)


def ranks(dest, devices):
    rows = dest.shape[1]
    blocks = rows // LANES
    hot = (iota((devices, rows), 0) == dest).astype(jnp.float32)
    stacked = jnp.concatenate([hot[:, b * LANES : (b + 1) * LANES] for b in range(blocks)], axis=0)
    before = (iota((LANES, LANES), 0) < iota((LANES, LANES), 1)).astype(jnp.float32)
    local = dot(stacked.astype(jnp.bfloat16), before.astype(jnp.bfloat16), ((1,), (0,)))
    carried = jnp.zeros((devices, 1), jnp.float32)
    pieces = []
    for b in range(blocks):
        part = local[b * devices : (b + 1) * devices]
        own = hot[:, b * LANES : (b + 1) * LANES]
        pieces.append(jnp.sum((part + carried) * own, axis=0, keepdims=True))
        carried = carried + jnp.sum(own, axis=1, keepdims=True)
    return jnp.concatenate(pieces, axis=1)


def donor_kernel(count, q_prev, q_now, base_in, frac_in, dest_in, cell_in, out_there, y_inner, y_outer, out, planes, lhs, lhs_low, spread, spread_low, corner, place, values, base, frac, dest, cell, sems, *, size, devices, capacity):
    nvars, size_x, size_y, size_z = size
    columns = size_x * size_y
    rows = base.shape[1]
    small = [pltpu.make_async_copy(a, b, sems.at[k]) for k, (a, b) in enumerate(((base_in, base), (frac_in, frac), (dest_in, dest), (cell_in, cell)))]
    copies = [pltpu.make_async_copy(ref.at[v], planes.at[k, v], sems.at[5 + k * nvars + v]) for k, ref in enumerate((q_prev, q_now)) for v in range(nvars)]
    for copy in small + copies:
        copy.start()
    for copy in small:
        copy.wait()
    start = base[...].astype(jnp.float32)
    in_y = jnp.floor((start + 0.5) * (1.0 / (size_z - 1)))
    base_z = start - in_y * (size_z - 1)
    base_x = jnp.floor((in_y + 0.5) * (1.0 / (size_y - 1)))
    base_y = in_y - base_x * (size_y - 1)
    frac_x, frac_y, frac_z = frac[0:1, :], frac[1:2, :], frac[2:3, :]

    def weights(first, part, shape):
        at = iota(shape, 0).astype(jnp.float32) - first
        return jnp.where(at == 0.0, 1.0 - part, jnp.where(at == 1.0, part, 0.0))

    along_z = weights(base_z, frac_z, (size_z, rows))
    spread[...] = along_z.astype(jnp.bfloat16)
    rest = along_z - spread[...].astype(jnp.float32)
    spread_low[0:size_z, :] = eighth(rest, 16)
    spread_low[size_z : 2 * size_z, :] = eighth(along_z, 8)
    along_x = weights(base_x, frac_x, (size_x, rows))
    along_y = weights(base_y, frac_y, (size_y, rows))
    for x in range(size_x):
        corner[x * size_y : (x + 1) * size_y, :] = along_x[x : x + 1, :] * along_y
    alive = iota((1, rows), 1) < count[0]
    slot = ranks(dest[...], devices)
    where_to = jnp.where(alive, dest[...].astype(jnp.float32) * capacity + slot, -1.0)
    place[...] = jnp.transpose(jnp.broadcast_to(where_to, (8, rows)))
    landing = cell[...].astype(jnp.float32)
    land_xy = jnp.floor((landing + 0.5) * (1.0 / size_z))
    values[...] = jnp.zeros(values.shape, jnp.float32)
    values[2 * nvars : 2 * nvars + 1, :] = land_xy + 1.0
    values[2 * nvars + 1 : 2 * nvars + 2, :] = landing - land_xy * size_z
    for k in range(2):
        if k == 1:
            for v in range(nvars):
                copies[nvars + v].wait()
            even = lax.axis_index("gy") % 2 == 0
            for v in range(nvars):
                for x in range(size_x):
                    line = planes.at[1, v]
                    low = line[x * size_y : x * size_y + 1, :]
                    high = line[(x + 1) * size_y - 1 : (x + 1) * size_y, :]
                    y_inner[v, x : x + 1, :] = jnp.where(even, high, low)
                    y_outer[v, x : x + 1, :] = jnp.where(even, low, high)
        for v in range(nvars):
            if k == 0:
                copies[v].wait()
            at = pl.ds((k * nvars + v) * columns, columns)
            plane = planes[k, v]
            lhs[at, :] = plane.astype(jnp.bfloat16)
            lhs_low[at, 0:size_z] = eighth(plane, 6)
            lhs_low[at, size_z : 2 * size_z] = eighth(plane - plane.astype(jnp.bfloat16).astype(jnp.float32), 14)
    for n in range(rows // LANES):
        lanes = slice(n * LANES, (n + 1) * LANES)
        for k in range(2):
            at = slice(k * nvars * columns, (k + 1) * nvars * columns)
            part = dot(lhs[at, :], spread[:, lanes], ((1,), (0,)))
            part = part + 2.0**-22 * dot(lhs_low[at, :], spread_low[:, lanes], ((1,), (0,)))
            for v in range(nvars):
                picked = part[v * columns : (v + 1) * columns] * corner[:, lanes]
                values[k * nvars + v : k * nvars + v + 1, lanes] = jnp.sum(picked, axis=0, keepdims=True)
    first = values[...]
    high, rest = first.astype(jnp.bfloat16), None
    rest = first - high.astype(jnp.float32)
    middle = rest.astype(jnp.bfloat16)
    last = (rest - middle.astype(jnp.float32)).astype(jnp.bfloat16)
    three = jnp.concatenate([high, middle, last], axis=0)
    leaving = []
    column = jnp.broadcast_to(place[:, 0:1], (rows, LANES))
    for n in range(devices * capacity // LANES):
        chosen = (column == (iota((rows, LANES), 1) + n * LANES).astype(jnp.float32)).astype(jnp.float32).astype(jnp.bfloat16)
        moved = dot(three, chosen, ((1,), (0,)))
        moved = moved[0:CHANNELS] + moved[CHANNELS : 2 * CHANNELS] + moved[2 * CHANNELS : 3 * CHANNELS]
        for d in range(LANES // capacity):
            piece = moved[:, d * capacity : (d + 1) * capacity]
            to = n * (LANES // capacity) + d
            out[to] = jnp.concatenate([piece[0:8], piece[8:16]], axis=1)
        some = pl.ds(n * (LANES // capacity), LANES // capacity)
        leaving.append(pltpu.make_async_copy(out.at[some], out_there.at[some], sems.at[n]))
        leaving[-1].start()
    for copy in leaving:
        copy.wait()


def mixing_weights(coef, high, low, size):
    nvars, _, size_y, _ = size
    block = nvars * size_y
    width = 3 * block + CHANNELS
    row = iota((size_y, width), 0)
    offset = iota((size_y, width), 1) - row
    lane = iota((size_y, width), 1)

    def at(d, side, a, b):
        return coef[((d * 2 + side) * nvars + a) * nvars + b]

    for a in range(nvars):
        main = jnp.zeros((size_y, width), jnp.float32)
        back = main
        fore = main
        for b in range(nvars):
            first = b * size_y
            same = at(0, 0, a, b) - at(0, 1, a, b) + at(1, 0, a, b) - at(1, 1, a, b) + at(2, 0, a, b) - at(2, 1, a, b)
            main = jnp.where(offset == first, -at(0, 0, a, b), main)
            main = jnp.where(offset == block + first, same, main)
            main = jnp.where((offset == block + first - 1) & (row > 0), -at(1, 0, a, b), main)
            main = jnp.where((offset == block + first + 1) & (row < size_y - 1), at(1, 1, a, b), main)
            main = jnp.where(offset == 2 * block + first, at(0, 1, a, b), main)
            main = jnp.where((lane == 3 * block + b) & (row == 0), -at(1, 0, a, b), main)
            main = jnp.where((lane == 3 * block + nvars + b) & (row == size_y - 1), at(1, 1, a, b), main)
            back = jnp.where(offset == block + first, -at(2, 0, a, b), back)
            fore = jnp.where(offset == block + first, at(2, 1, a, b), fore)
        for k, part in enumerate((main, back, fore)):
            rows = slice(k * block + a * size_y, k * block + (a + 1) * size_y)
            high[rows, :], low[rows, :] = halves(part)


def fill_planes(at_plane, around, planes, sides, size):
    nvars, size_x, size_y, size_z = size
    block = nvars * size_y
    for x in range(size_x + 2):
        for v in range(nvars):
            rows = slice(x * block + v * size_y, x * block + (v + 1) * size_y)
            if 0 < x <= size_x:
                planes[0, rows, :], planes[1, rows, :] = halves(at_plane(v, x - 1))
            elif around is None:
                planes[0, rows, :] = planes[1, rows, :] = jnp.zeros((size_y, size_z), jnp.bfloat16)
            else:
                planes[0, rows, :], planes[1, rows, :] = halves(around[0 if x == 0 else 1][v])
    if around is not None:
        sides[...] = jnp.zeros(sides.shape, jnp.float32)
        for v in range(nvars):
            sides[:, v, :] = around[2][v]
            sides[:, nvars + v, :] = around[3][v]


def flux_at(x, weights, planes, sides, size):
    nvars, _, size_y, size_z = size
    block = nvars * size_y
    if sides is None:
        high = low = jnp.zeros((CHANNELS, size_z), jnp.bfloat16)
    else:
        high, low = halves(sides[x])
    rows = slice(x * block, (x + 3) * block)
    around_high = jnp.concatenate([planes[0, rows, :], high], axis=0)
    around_low = jnp.concatenate([planes[1, rows, :], low], axis=0)
    both = jnp.concatenate([weights[0], weights[1]], axis=0)
    mixed = dot(both, around_high, ((1,), (0,)))
    mixed = mixed[0 : 3 * block] + mixed[3 * block :] + dot(weights[0], around_low, ((1,), (0,)))
    z_at = iota((block, size_z), 1)
    back = jnp.where(z_at == 0, 0.0, pltpu.roll(mixed[block : 2 * block], 1, 1))
    fore = jnp.where(z_at == size_z - 1, 0.0, pltpu.roll(mixed[2 * block :], size_z - 1, 1))
    flux = mixed[0:block] + back + fore
    return [flux[v * size_y : (v + 1) * size_y] for v in range(nvars)]


def sent_out(x, size_x, buffer, out, sems, copies):
    part = size_x // PIECES
    if (x + 1) % part == 0:
        some = pl.ds(x + 1 - part, part)
        copies.append(pltpu.make_async_copy(buffer.at[:, some], out.at[:, some], sems.at[x // part]))
        copies[-1].start()


def early_kernel(coef_in, q_now, q_prev, jac, base, weights_out, table, planes, coef, buffer, weights, sems, *, size):
    nvars, size_x, _, size_z = size
    fetch = pltpu.make_async_copy(coef_in, coef, sems.at[PIECES])
    fetch.start()
    fill_planes(lambda v, x: q_now[v, x], None, planes, None, size)
    fetch.wait()
    for k in range(table.shape[0]):
        table[k : k + 1, :] = jnp.full((1, size_z), coef[k], jnp.float32)
    mixing_weights(coef, weights.at[0], weights.at[1], size)
    copies = [pltpu.make_async_copy(weights, weights_out, sems.at[PIECES + 1])]
    copies[0].start()
    for x in range(size_x):
        flux = flux_at(x, weights, planes, None, size)
        scale = step_tau * jac[x]
        for v in range(nvars):
            centre = q_now[v, x]
            physical = (q_prev[v, x] - centre) / (2.0 * step_phys)
            buffer[v, x] = centre - scale * (flux[v] + physical)
        sent_out(x, size_x, buffer, base, sems, copies)
    for copy in copies:
        copy.wait()


def mixed_by(table, direction, side, lines):
    nvars = len(lines)
    out = []
    for a in range(nvars):
        total = None
        for b in range(nvars):
            k = ((direction * 2 + side) * nvars + a) * nvars + b
            term = table[k : k + 1, :] * lines[b]
            total = term if total is None else total + term
        out.append(total)
    return out


def land(rows, hot_xy, hot_z, store, nvars):
    columns = hot_xy.shape[0]
    for first in range(0, nvars, 2):
        some = range(first, min(first + 2, nvars))
        pieces = []
        for c in some:
            for half in halves(rows[c : c + 1, :]):
                pieces.append(hot_xy[...] * half)
        landed = dot(jnp.concatenate(pieces, axis=0), hot_z[...], ((1,), (0,)))
        for c in some:
            at = 2 * (c - first) * columns
            store(c, landed[at : at + columns] + landed[at + columns : at + 2 * columns])


def land_split(rows, hot_xy, hot_z, hot_z_low, store, nvars):
    columns = hot_xy.shape[0]
    for first in range(0, nvars, 2):
        some = range(first, min(first + 2, nvars))
        high, low = [], []
        for c in some:
            whole = rows[c : c + 1, :]
            part = whole.astype(jnp.bfloat16)
            high.append(hot_xy[...] * part)
            scaled = ((whole - part.astype(jnp.float32)) * 2.0**14).astype(jnp.bfloat16)
            low.append((hot_xy[...] * scaled).astype(jnp.float8_e4m3fn))
        landed = dot(jnp.concatenate(high, axis=0), hot_z[...], ((1,), (0,)))
        landed = landed + 2.0**-14 * dot(jnp.concatenate(low, axis=0), hot_z_low[...], ((1,), (0,)))
        for c in some:
            store(c, landed[(c - first) * columns : (c - first + 1) * columns])


def first_kernel(table, got, base_in, q_now, jac, line_inner, line_outer, state, hits, x_inner, x_outer, y_inner, y_outer, later, hot_xy, hot_z, hot_z_low, rows, grid, base, sems, *, size, devices, capacity):
    nvars, size_x, size_y, size_z = size
    columns = size_x * size_y
    slots = devices * capacity

    def fetch(x):
        return pltpu.make_async_copy(base_in.at[:, pl.ds(x, 1)], base.at[:, pl.ds(x, 1)], sems.at[x])

    @pl.loop(0, size_x)
    def _(x):
        fetch(x).start()

    for d in range(devices):
        piece = got[d]
        lanes = slice(d * capacity, (d + 1) * capacity)
        rows[0:8, lanes] = piece[:, 0:capacity]
        rows[8:16, lanes] = piece[:, capacity : 2 * capacity]
    turned = jnp.transpose(rows[8:16, :])
    land_z = turned[:, 2 * nvars + 1 - 8 : 2 * nvars + 2 - 8]
    hot_z[...] = (iota((slots, size_z), 1).astype(jnp.float32) == land_z).astype(jnp.float32).astype(jnp.bfloat16)
    hot_z_low[...] = (iota((slots, size_z), 1).astype(jnp.float32) == land_z).astype(jnp.float32).astype(jnp.float8_e4m3fn)
    land_xy = rows[2 * nvars : 2 * nvars + 1, :]
    hot_xy[...] = ((iota((columns, slots), 0) + 1).astype(jnp.float32) == land_xy).astype(jnp.float32).astype(jnp.bfloat16)
    later[...] = rows[nvars : 2 * nvars, :]

    hits[...] = dot(hot_xy[...], hot_z[...], ((1,), (0,)))
    even_x, even_y = lax.axis_index("gx") % 2 == 0, lax.axis_index("gy") % 2 == 0
    y_low, y_high = zip(*(sides_of("gy", line_inner[v], line_outer[v]) for v in range(nvars)))
    from_low, from_high = mixed_by(table, 1, 0, y_low), mixed_by(table, 1, 1, y_high)
    row_at = iota((size_y, size_z), 0)
    faces = {}

    def keep(c, value):
        grid[c] = value

    land_split(rows, hot_xy, hot_z, hot_z_low, keep, nvars)
    for x in range(size_x):
        fetch(x).wait()
    for x in range(size_x):
        at = slice(x * size_y, (x + 1) * size_y)
        landed = hits[at, :]
        scale = step_tau * jac[x]
        for v in range(nvars):
            change = penalty * (landed * q_now[v, x] - grid[v, at, :])
            change = change - jnp.where(row_at == 0, from_low[v][x : x + 1], 0.0)
            change = change + jnp.where(row_at == size_y - 1, from_high[v][x : x + 1], 0.0)
            new = base[v, x] - scale * change
            state[v, x] = new
            if x in (0, size_x - 1):
                faces[x, v] = new
    toward = jnp.where(even_y, size_y - 1, 0)
    for v in range(nvars):
        for x in range(size_x):
            y_inner[v * size_x + x : v * size_x + x + 1, :] = state[v, x, pl.ds(toward, 1), :]
            y_outer[v * size_x + x : v * size_x + x + 1, :] = state[v, x, pl.ds(size_y - 1 - toward, 1), :]
    tail = nvars * size_x
    y_inner[tail:, :] = y_outer[tail:, :] = jnp.zeros((8, size_z), jnp.float32)
    for k, x in enumerate((0, size_x - 1)):
        low, high = jac[x][0:1], jac[x][size_y - 1 : size_y]
        y_inner[tail + k : tail + k + 1, :] = jnp.where(even_y, high, low)
        y_outer[tail + k : tail + k + 1, :] = jnp.where(even_y, low, high)
    ends = [y_low[v] for v in range(nvars)] + [y_high[v] for v in range(nvars)]
    for v in range(nvars):
        for k, pair in enumerate(((faces[0, v], faces[size_x - 1, v]), (q_now[v, 0], q_now[v, size_x - 1]))):
            x_inner[k * nvars + v] = jnp.where(even_x, pair[1], pair[0])
            x_outer[k * nvars + v] = jnp.where(even_x, pair[0], pair[1])
    x_inner[2 * nvars] = jnp.where(even_x, jac[size_x - 1], jac[0])
    x_outer[2 * nvars] = jnp.where(even_x, jac[0], jac[size_x - 1])
    x_inner[2 * nvars + 1] = x_outer[2 * nvars + 1] = jnp.zeros((size_y, size_z), jnp.float32)
    for k, line in enumerate(ends):
        low, high = line[0:1], line[size_x - 1 : size_x]
        x_inner[2 * nvars + 1, k : k + 1, :] = jnp.where(even_x, high, low)
        x_outer[2 * nvars + 1, k : k + 1, :] = jnp.where(even_x, low, high)


def late_kernel(rows, hot_xy, hot_z, target):
    def keep(c, value):
        target[c] = value

    land(rows, hot_xy, hot_z, keep, rows.shape[0])


def second_kernel(table, state, weights, q_now, q_prev, jac, target, hits, x_inner, x_outer, y_inner, y_outer, out, planes, sides, edge, buffer, sems, *, size):
    nvars, size_x, size_y, size_z = size
    last = size_x - 1
    x_low, x_high = zip(*(sides_of("gx", x_inner[k], x_outer[k]) for k in range(2 * nvars + 2)))
    own_low = mixed_by(table, 0, 0, x_low[nvars : 2 * nvars])
    own_high = mixed_by(table, 0, 1, x_high[nvars : 2 * nvars])
    ring_low = mixed_by(table, 0, 1, [q_now[v, 0] for v in range(nvars)])
    ring_high = mixed_by(table, 0, 0, [q_now[v, last] for v in range(nvars)])
    around = [[], [], [], []]
    for v in range(nvars):
        edge[0, v] = state[v, 0] + step_tau * jac[0] * own_low[v]
        edge[1, v] = state[v, last] - step_tau * jac[last] * own_high[v]
        around[0].append(x_low[v] - step_tau * x_low[2 * nvars] * ring_low[v])
        around[1].append(x_high[v] + step_tau * x_high[2 * nvars] * ring_high[v])
    row_at = iota((size_x, size_z), 0)
    tail = nvars * size_x
    for side in range(2):
        scale = sides_of("gy", y_inner[tail:, :], y_outer[tail:, :])[side]
        corner = range(side * nvars, (side + 1) * nvars)
        low = mixed_by(table, 0, 0, [x_low[2 * nvars + 1][k : k + 1] for k in corner])
        high = mixed_by(table, 0, 1, [x_high[2 * nvars + 1][k : k + 1] for k in corner])
        for v in range(nvars):
            change = jnp.where(row_at == 0, scale[0:1] * low[v], 0.0) - jnp.where(row_at == last, scale[1:2] * high[v], 0.0)
            face = slice(v * size_x, (v + 1) * size_x)
            around[2 + side].append(sides_of("gy", y_inner[face, :], y_outer[face, :])[side] + step_tau * change)

    def at_plane(v, x):
        return edge[0, v] if x == 0 else edge[1, v] if x == last else state[v, x]

    fill_planes(at_plane, around, planes, sides, size)
    copies = []
    for x in range(size_x):
        at = slice(x * size_y, (x + 1) * size_y)
        flux = flux_at(x, weights, planes, sides, size)
        landed = hits[at, :]
        scale = step_tau * jac[x]
        for v in range(nvars):
            centre = at_plane(v, x)
            physical = (3.0 * centre - 4.0 * q_now[v, x] + q_prev[v, x]) / (2.0 * step_phys)
            coupling = penalty * (landed * centre - target[v, at, :])
            buffer[v, x] = centre - scale * (flux[v] + physical + coupling)
        sent_out(x, size_x, buffer, out, sems, copies)
    for copy in copies:
        copy.wait()


def swapped(inner, outer, axis):
    count_x, count_y = lax.axis_size("gx"), lax.axis_size("gy")
    inner_pairs, outer_pairs = [], []
    for i in range(count_x):
        for j in range(count_y):
            at, count = (i, count_x) if axis == "gx" else (j, count_y)
            for pairs, to in ((inner_pairs, at ^ 1), (outer_pairs, ((at + 1) ^ 1) - 1)):
                x, y = (to, j) if axis == "gx" else (i, to)
                if axis == "gx" and not 0 <= to < count:
                    x, y = i, j ^ 2
                if axis == "gy" and not 0 <= to < count:
                    x, y = i ^ 1, j
                pairs.append((i * count_y + j, x * count_y + y))
    return lax.ppermute(inner, AXES, inner_pairs), lax.ppermute(outer, AXES, outer_pairs)


def sides_of(axis, inner, outer):
    here, last = lax.axis_index(axis), lax.axis_size(axis) - 1
    even = here % 2 == 0
    inside = (here > 0) & (here < last)
    masked = jnp.where(inside, outer, 0.0)
    return jnp.where(even, masked, inner), jnp.where(even, inner, masked)


def params(limit):
    return pltpu.CompilerParams(vmem_limit_bytes=limit)


def body(q_now, q_prev, jacobian, flux_split, donor_base, donor_frac, fringe_dest, receptor_cell, fringe_count):
    size = q_now.shape
    nvars, size_x, size_y, size_z = size
    columns = size_x * size_y
    block = nvars * size_y
    devices = lax.axis_size("gx") * lax.axis_size("gy")
    rows = donor_base.shape[0]
    capacity = 2 * rows // devices
    slots = devices * capacity
    f32, bf16 = jnp.float32, jnp.bfloat16
    hbm = pl.BlockSpec(memory_space=pltpu.HBM)
    vmem = pl.BlockSpec(memory_space=pltpu.VMEM)
    flat = (nvars, columns, size_z)
    shape = jax.ShapeDtypeStruct
    weights_shape = (2, 3 * block, 3 * block + CHANNELS)
    planes = pltpu.VMEM((2, (size_x + 2) * block, size_z), bf16)
    sides = pltpu.VMEM((size_x, CHANNELS, size_z), f32)
    face_y = shape((nvars * size_x + 8, size_z), f32)

    line, line_x = pltpu.VMEM((nvars, size_x, size_z), f32), shape((2 * nvars + 2, size_y, size_z), f32)
    coef = flux_split.reshape(-1)

    def there(x):
        return pltpu.with_memory_space_constraint(x, pltpu.HBM)

    sent, *lines = pl.pallas_call(
        functools.partial(donor_kernel, size=size, devices=devices, capacity=capacity),
        out_shape=[pltpu.HBM((devices, 8, 2 * capacity), f32), line, line],
        in_specs=[pl.BlockSpec(memory_space=pltpu.SMEM)] + [hbm] * 6,
        out_specs=[hbm, vmem, vmem],
        scratch_shapes=[
            pltpu.VMEM((devices, 8, 2 * capacity), f32),
            pltpu.VMEM((2, nvars, columns, size_z), f32),
            pltpu.VMEM((2 * nvars * columns, size_z), bf16),
            pltpu.VMEM((2 * nvars * columns, 2 * size_z), jnp.float8_e4m3fn),
            pltpu.VMEM((size_z, rows), bf16),
            pltpu.VMEM((2 * size_z, rows), jnp.float8_e4m3fn),
            pltpu.VMEM((columns, rows), f32),
            pltpu.VMEM((rows, 8), f32),
            pltpu.VMEM((CHANNELS, rows), f32),
            pltpu.VMEM((1, rows), jnp.int32),
            pltpu.VMEM((3, rows), f32),
            pltpu.VMEM((1, rows), jnp.int32),
            pltpu.VMEM((1, rows), jnp.int32),
            pltpu.SemaphoreType.DMA((5 + 2 * nvars,)),
        ],
        compiler_params=params(DONOR_LIMIT),
        name="donor",
    )(
        fringe_count,
        there(q_prev.reshape(flat)),
        there(q_now.reshape(flat)),
        there(donor_base.reshape(1, rows)),
        there(donor_frac),
        there(fringe_dest.reshape(1, rows)),
        there(receptor_cell.reshape(1, rows)),
    )
    got = lax.all_to_all(sent, AXES, split_axis=0, concat_axis=0, tiled=True)
    lines = swapped(*lines, "gy")
    base, weights, table = pl.pallas_call(
        functools.partial(early_kernel, size=size),
        out_shape=[pltpu.HBM(size, f32), pltpu.HBM(weights_shape, bf16), shape((4 * nvars * nvars, size_z), f32)],
        in_specs=[hbm] + [vmem] * 3,
        out_specs=[hbm, hbm, vmem],
        scratch_shapes=[planes, pltpu.SMEM((6 * nvars * nvars,), f32), pltpu.VMEM(size, f32), pltpu.VMEM(weights_shape, bf16), pltpu.SemaphoreType.DMA((PIECES + 2,))],
        compiler_params=params(20 * MIB),
        name="early",
    )(coef, q_now, q_prev, jacobian)
    state, hits, *faces, later, hot_xy, hot_z = pl.pallas_call(
        functools.partial(first_kernel, size=size, devices=devices, capacity=capacity),
        out_shape=[
            shape(size, f32),
            shape((columns, size_z), f32),
            line_x,
            line_x,
            face_y,
            face_y,
            shape((nvars, slots), f32),
            shape((columns, slots), bf16),
            shape((slots, size_z), bf16),
        ],
        in_specs=[vmem, vmem, hbm] + [vmem] * 4,
        out_specs=[vmem] * 9,
        scratch_shapes=[
            pltpu.VMEM((slots, size_z), jnp.float8_e4m3fn),
            pltpu.VMEM((CHANNELS, slots), f32),
            pltpu.VMEM((nvars, columns, size_z), f32),
            pltpu.VMEM(size, f32),
            pltpu.SemaphoreType.DMA((size_x,)),
        ],
        compiler_params=params(20 * MIB),
        name="first",
    )(table, got, there(base), q_now, jacobian, *lines)
    around = (*swapped(*faces[0:2], "gx"), *swapped(*faces[2:4], "gy"))
    target = pl.pallas_call(
        late_kernel,
        out_shape=shape(flat, f32),
        in_specs=[vmem] * 3,
        out_specs=vmem,
        compiler_params=params(20 * MIB),
        name="late",
    )(later, hot_xy, hot_z)
    return pl.pallas_call(
        functools.partial(second_kernel, size=size),
        out_shape=shape(size, f32),
        in_specs=[vmem] * 12,
        out_specs=hbm,
        scratch_shapes=[planes, sides, pltpu.VMEM((2, nvars, size_y, size_z), f32), pltpu.VMEM(size, f32), pltpu.SemaphoreType.DMA((PIECES,))],
        compiler_params=params(20 * MIB),
        name="second",
    )(table, state, weights, q_now, q_prev, jacobian, target, hits, *around)


def solution(mesh):
    return jax.shard_map(
        body,
        mesh=mesh,
        in_specs=(
            P(None, "gx", "gy", None),
            P(None, "gx", "gy", None),
            P("gx", "gy", None),
            P(),
            P(("gx", "gy")),
            P(None, ("gx", "gy")),
            P(("gx", "gy"), None),
            P(("gx", "gy")),
            P(("gx", "gy")),
        ),
        out_specs=P(None, "gx", "gy", None),
        check_vma=False,
    )
```
